256 devices in a mesh: pop: 2 (over z), dp: 2 (over core), tensor: 64 (over y, x).
Axes of the slice: x: 8, y: 8, z: 2, core: 2. Of those that a mesh axis runs over, the one named last changes fastest.
The devices are a block of a 8x8x16 slice.
Arguments:
- tokens: bfloat16 [1024, 16384], P(('pop', 'dp'), 'tensor'), parts along dimension 0, may hold values from -6 to 6
- weight: bfloat16 [16384, 26624], P('dp', 'tensor'), may hold values from -0.046875 to 0.046875
- adapter_in: bfloat16 [8, 16384, 64], P(('pop', 'dp'), 'tensor'), parts along dimension 0, may hold values from -0.046875 to 0.046875
- adapter_out: bfloat16 [8, 64, 26624], P(('pop', 'dp'), None, 'tensor'), parts along dimension 0, may hold values from -0.375 to 0.375
- cotangent: bfloat16 [1024, 26624], P(('pop', 'dp'), 'tensor'), parts along dimension 0, may hold values from -0.59765625 to 0.59765625
- member_blocks: int32 [8], P('pop'), parts along dimension 0, may hold values from 0 to 3, as said below
- block_live: int32 [8], P(('pop', 'dp')), parts along dimension 0, may hold values from 1 to 128, as said below
Outputs:
- hidden: bfloat16 [1024, 26624], P(('pop', 'dp'), 'tensor'), parts along dimension 0
- input_gradient: bfloat16 [1024, 16384], P(('pop', 'dp'), 'tensor'), parts along dimension 0
- down_factor_gradient: float32 [8, 16384, 64], P(('pop', 'dp'), 'tensor'), parts along dimension 0
- up_factor_gradient: float32 [8, 64, 26624], P(('pop', 'dp'), None, 'tensor'), parts along dimension 0
The draws below stay inside these ranges and needn't reach their ends.
There are 2 independent parts, one for each index of `pop`. The reference program is written for one: setup_inputs(seed, part) draws one part's arguments, and reference() takes and returns one part's arrays. A program takes and returns all parts, laid end to end along the dimension named above; an argument that names none is the same for every part. Nothing has to cross between parts.
Inputs may be any that keep to these rules, and one draw needn't show every extreme that they name: `member_blocks`: the number of 128-token blocks of each member; the counts sum to 4 and the blocks come in order of member. `block_live`: the live tokens stand at the start of each block; every block but the last one of its member is full.
All inputs are finite; a program needn't handle non-finite values.
Results may differ from the reference program's by a relative error of at most 0.003.
Values may be sent and summed in bfloat16 or wider, within the bound.
A program may use at most 128 MiB of HBM per device.

```python
import jax
import jax.numpy as jnp
from jax import lax

D = 16384
FFW = 26624
MEMBERS = 4
RANK = 64
BLOCK = 128
TOKENS = 512
NBLK = 4


def member_layout(key):
    salted = jax.random.fold_in(key, 31)
    first_key, second_key, third_key = jax.random.split(salted, 3)
    biggest = NBLK // 2 + 1
    leader = jax.random.randint(third_key, (), 0, MEMBERS).astype(jnp.int32)
    others = jax.random.randint(first_key, (NBLK - biggest,), 0, MEMBERS - 1).astype(jnp.int32)
    others = (others + (others >= leader).astype(jnp.int32)).astype(jnp.int32)
    leading = jnp.zeros((biggest,), dtype=jnp.int32) + leader
    members = jnp.sort(jnp.concatenate([leading, others])).astype(jnp.int32)
    return (members, second_key)


def draw_member_blocks(key, part):
    members, second_key = member_layout(key)
    hits = (members[:, None] == jnp.arange(MEMBERS, dtype=jnp.int32)[None, :]).astype(jnp.int32)
    return jnp.sum(hits, axis=0).astype(jnp.int32)


def draw_block_live(key, part):
    members, second_key = member_layout(key)
    closing = jnp.concatenate([members[1:] != members[:-1], jnp.ones((1,), dtype=jnp.bool_)])
    partial_fill = jax.random.randint(second_key, (NBLK,), 1, BLOCK + 1)
    return jnp.where(closing, partial_fill, BLOCK).astype(jnp.int32)


def level_of(own_key, extent, cuts, low, largest):
    def one(position, shards_of):
        heights = jax.random.uniform(jax.random.fold_in(jax.random.fold_in(own_key, 6), position), (shards_of,), jnp.float32, low / len(cuts), largest / len(cuts))
        return jnp.repeat(jnp.exp(heights), extent[position] // shards_of).reshape((-1,) + (1,) * (len(extent) - position - 1))

    factor_of = one(*cuts[0])
    for cut in cuts[1:]:
        factor_of = factor_of * one(*cut)
    return factor_of


def gaussian(own_key, extent, deviation, bound, pieces=(), held_as=jnp.bfloat16):
    array = jax.random.normal(own_key, extent, jnp.float32) * deviation
    if len(pieces) > 0:
        array = level_of(own_key, extent, pieces, -0.22, 0.18) * array
    return jnp.clip(array, min=-bound, max=bound).astype(held_as)


def setup_inputs(seed: int = 0, part: int = 0) -> dict:
    streams_of = jax.random.split(jax.random.key(seed), 8)
    part_splits = jax.random.split(jax.random.fold_in(streams_of[7], part), 8)
    tokens = gaussian(part_splits[0], (TOKENS, D), 1.0, 6.0, ((0, 2), (1, 64)))
    weight = gaussian(streams_of[1], (D, FFW), D ** -0.5, 0.046875, ((0, 2), (1, 64)))
    adapter_in = gaussian(part_splits[2], (MEMBERS, D, RANK), D ** -0.5, 0.046875, ((0, 2), (1, 64)))
    adapter_out = gaussian(part_splits[3], (MEMBERS, RANK, FFW), (4 * RANK) ** -0.5, 0.375, ((0, 2), (2, 64)))
    cotangent = gaussian(part_splits[4], (TOKENS, FFW), 0.1, 0.59765625, ((0, 2), (1, 64)))
    member_blocks = draw_member_blocks(jax.random.fold_in(jax.random.fold_in(streams_of[7], part), 71), part)
    block_live = draw_block_live(jax.random.fold_in(jax.random.fold_in(streams_of[7], part), 71), part)
    return {"tokens": tokens, "weight": weight, "adapter_in": adapter_in, "adapter_out": adapter_out, "cotangent": cotangent, "member_blocks": member_blocks, "block_live": block_live}


adapter_scale = 0.5


def reference(tokens, weight, adapter_in, adapter_out, cotangent, member_blocks, block_live):
    ends = jnp.cumsum(member_blocks).astype(jnp.int32)
    blocks = jnp.arange(NBLK, dtype=jnp.int32)
    members = jnp.sum((ends[None, :] <= blocks[:, None]).astype(jnp.int32), axis=1).astype(jnp.int32)
    member_lookup = (members[:, None] == jnp.arange(MEMBERS, dtype=jnp.int32)[None, :]).astype(jnp.float32)
    offsets = jnp.arange(BLOCK, dtype=jnp.int32)
    active_member_mask = (offsets[None, :] < block_live[:, None]).astype(jnp.bfloat16).reshape(TOKENS, 1)
    chosen_in = jnp.take(adapter_in, members, axis=0).astype(jnp.float32)
    chosen_out = jnp.take(adapter_out, members, axis=0).astype(jnp.float32)
    token_blocks = tokens.reshape(NBLK, BLOCK, D).astype(jnp.float32)
    low_in = jnp.einsum("btk,bkr->btr", token_blocks, chosen_in).astype(jnp.bfloat16)
    frozen_projection = jnp.dot(tokens, weight, preferred_element_type=jnp.float32)
    raised_hidden = jnp.einsum("btr,brf->btf", low_in.astype(jnp.float32), chosen_out).reshape(TOKENS, FFW)
    hidden = (active_member_mask.astype(jnp.float32) * (frozen_projection + adapter_scale * raised_hidden)).astype(jnp.bfloat16)
    masked = cotangent * active_member_mask
    grad_blocks = masked.reshape(NBLK, BLOCK, FFW).astype(jnp.float32)
    low_back = jnp.einsum("btf,brf->btr", grad_blocks, chosen_out).astype(jnp.bfloat16)
    projected_output = lax.dot_general(masked, weight, (((1,), (1,)), ((), ())), preferred_element_type=jnp.float32)
    reduced_hidden = jnp.einsum("btr,bkr->btk", low_back.astype(jnp.float32), chosen_in).reshape(TOKENS, D)
    input_gradient = (projected_output + adapter_scale * reduced_hidden).astype(jnp.bfloat16)
    down_outer_product = jnp.einsum("btk,btr->bkr", token_blocks, low_back.astype(jnp.float32))
    up_outer_product = jnp.einsum("btr,btf->brf", low_in.astype(jnp.float32), grad_blocks)
    down_factor_gradient = adapter_scale * jnp.einsum("gw,gsd->wsd", member_lookup, down_outer_product, precision=lax.Precision.HIGHEST)
    up_factor_gradient = adapter_scale * jnp.einsum("jg,juy->guy", member_lookup, up_outer_product, precision=lax.Precision.HIGHEST)
    return hidden, input_gradient, down_factor_gradient, up_factor_gradient
```

```python
import functools
import math

import jax
import jax.numpy as jnp
from jax import lax
from jax.experimental import pallas as pl
from jax.experimental.pallas import tpu as pltpu
from jax.sharding import Mesh
from jax.sharding import PartitionSpec as P

BLOCK = 128
SCALE = 0.5
MESH = pl.DeviceIdType.MESH
ROW, COL, CORE = "tensor_0", "tensor_1", "dp"
F32, BF16 = jnp.float32, jnp.bfloat16

NN = (((1,), (0,)), ((), ()))
NT = (((1,), (1,)), ((), ()))
TN = (((0,), (0,)), ((), ()))


def dot(a, b, dims):
    return lax.dot_general(a, b, dims, preferred_element_type=F32)


LANES, SUBLANES = 128, 8
UNIT = 2.0**21
TOP = 32760.0


def halves(v):
    return [v[:, k : k + LANES] for k in range(0, v.shape[1], LANES)]


def encode(v):
    groups = [h.reshape(-1, SUBLANES, LANES) for h in halves(v)]
    largest = functools.reduce(jnp.maximum, [jnp.max(jnp.abs(q), axis=0) for q in groups])
    scale = (largest * UNIT).astype(jnp.int32) + 1
    by = (TOP * UNIT) / scale.astype(F32)
    out = []
    for q in groups:
        code = (q * by[None]).astype(jnp.int32)
        mid = code.shape[0] // 2
        pair = (code[:mid] << 16) | (code[mid:] & 0xFFFF)
        out.append(pair.reshape(-1, LANES))
    return jnp.concatenate([*out, scale], axis=0)


def decode(code):
    scale = code[-SUBLANES:].astype(F32) * (1.0 / (TOP * UNIT))
    body = code[:-SUBLANES]
    mid = body.shape[0] // 2
    out = []
    for k in range(2):
        pair = body[k * mid : (k + 1) * mid].reshape(-1, SUBLANES, LANES)
        both = jnp.concatenate([pair >> 16, (pair << 16) >> 16], axis=0)
        out.append((both.astype(F32) * scale[None]).reshape(-1, LANES))
    return jnp.concatenate(out, axis=1)


def kernel(
    n,
    mb,
    bl,
    tok_hbm,
    w_hbm,
    ain_hbm,
    aout_hbm,
    cot,
    hidden,
    igrad,
    dgrad,
    ugrad,
    g,
    w,
    p,
    rb,
    r2,
    masked,
    acc,
    adt,
    ain,
    aout,
    cin,
    cout,
    part,
    xbuf,
    ybuf,
    low,
    usend,
    dsend,
    urecv,
    drecv,
    ag1_s,
    ag1_r,
    ag2_s,
    ag2_r,
    rs1_s,
    rs1_r,
    rs2_s,
    rs2_r,
    own_sem,
    w_sem,
    wx_s,
    wx_r,
    ad_sem,
    adx_s,
    adx_r,
    xs,
    xr,
    ys,
    yr,
    zs,
    zr,
    gx_s,
    gx_r,
):
    half = n // 2
    ticks = n + half
    early, middle, late = n // 4, n // 2, 3 * n // 4
    y, x, d = lax.axis_index(ROW), lax.axis_index(COL), lax.axis_index(CORE)
    mate = {CORE: 1 - d}
    me = y * n + x
    chunks = n * n
    members = ain.shape[0]
    owned = members // 2
    own_chunks = w_hbm.shape[0]
    pieces = w_sem.shape[0]
    piece = own_chunks // pieces
    rank = ain.shape[2]
    minor_axis, major_axis = (COL, ROW), (ROW, COL)
    minor_at, major_at = (x, y), (y, x)

    def chunk(c, major, minor):
        return major * n + minor if c == 0 else minor * n + major

    def wrap(v):
        return lax.rem(v + 2 * n, n)

    def remote(src, dst, ss, rs, to):
        return pltpu.make_async_remote_copy(
            src_ref=src, dst_ref=dst, send_sem=ss, recv_sem=rs, device_id=to, device_id_type=MESH
        )

    def landed(dst, sem):
        pltpu.make_async_copy(dst, dst, sem).wait()

    for c in range(2):
        pltpu.make_async_copy(tok_hbm.at[c], g.at[c, me], own_sem.at[c]).start()
    barrier = pltpu.get_barrier_semaphore()
    for k in range(1, n):
        pl.semaphore_signal(barrier, inc=1, device_id={COL: wrap(x + k)}, device_id_type=MESH)
        pl.semaphore_signal(barrier, inc=1, device_id={ROW: wrap(y + k)}, device_id_type=MESH)
    pl.semaphore_signal(barrier, inc=1, device_id=mate, device_id_type=MESH)

    def ad_local(k):
        hbm, vm = ((ain_hbm, ain), (aout_hbm, aout))[k]
        return pltpu.make_async_copy(hbm, vm.at[pl.ds(d * owned, owned)], ad_sem.at[k])

    def ad_remote(k):
        hbm, vm = ((ain_hbm, ain), (aout_hbm, aout))[k]
        return remote(hbm, vm.at[pl.ds(d * owned, owned)], adx_s.at[k], adx_r.at[k], mate)

    def w_local(q):
        src = w_hbm.at[pl.ds(q * piece, piece)]
        return pltpu.make_async_copy(src, w.at[pl.ds(d * own_chunks + q * piece, piece)], w_sem.at[q])

    def w_remote(q):
        src = w_hbm.at[pl.ds(q * piece, piece)]
        return remote(src, w.at[pl.ds(d * own_chunks + q * piece, piece)], wx_s.at[q], wx_r.at[q], mate)

    for k in range(2):
        ad_local(k).start()
    for q in range(pieces):
        w_local(q).start()
    for c in range(2):
        landed(g.at[c, me], own_sem.at[c])
    pl.semaphore_wait(barrier, 2 * (n - 1) + 1)

    def minor_offset(j):
        back = lax.div(j + 1, 2)
        return jnp.where(lax.rem(j, 2) == 1, -back, lax.div(j, 2))

    def ag1_copy(c, j, right):
        src = chunk(c, major_at[c], wrap(minor_at[c] + minor_offset(j)))
        lands = jnp.where(j == 0, 1 if right else 2, j + 2)
        to = {minor_axis[c]: wrap(minor_at[c] + (1 if right else -1))}
        return remote(g.at[c, src], g.at[c, src], ag1_s.at[c, lands], ag1_r.at[c, lands], to)

    def ag1_step(j):
        for c in range(2):
            src = chunk(c, major_at[c], wrap(minor_at[c] + minor_offset(j)))

            @pl.when(j >= 1)
            def _(c=c, src=src):
                landed(g.at[c, src], ag1_r.at[c, j])

            @pl.when(jnp.logical_or(j == 0, jnp.logical_and(lax.rem(j, 2) == 1, j + 2 < n)))
            def _(c=c):
                ag1_copy(c, j, True).start()

            @pl.when(jnp.logical_and(lax.rem(j, 2) == 0, j + 2 < n))
            def _(c=c):
                ag1_copy(c, j, False).start()

    def ag2_copy(c, e, j, s):
        way = 1 - 2 * e
        t = chunk(c, wrap(major_at[c] - way * s), wrap(minor_at[c] + minor_offset(j)))
        to = {major_axis[c]: wrap(major_at[c] + way)}
        return remote(g.at[c, t], g.at[c, t], ag2_s.at[c, e, j, s], ag2_r.at[c, e, j, s], to)

    def ag2_landed(c, e, j, s):
        t = chunk(c, wrap(major_at[c] - (1 - 2 * e) * s), wrap(minor_at[c] + minor_offset(j)))
        landed(g.at[c, t], ag2_r.at[c, e, j, s - 1])

    def is_long(e, j):
        return lax.rem(j, 2) == e

    def live_stream(j):
        return jnp.logical_and(j >= 0, j < n)

    def ag_tick(tick):
        @pl.when(tick < n)
        def _():
            ag1_step(tick)

        for s in range(half + 1):
            j = tick - s

            @pl.when(live_stream(j))
            def _(j=j, s=s):
                for c in range(2):
                    for e in range(2):
                        if s < half:
                            if s > 0:
                                ag2_landed(c, e, j, s)
                            if s < half - 1:
                                ag2_copy(c, e, j, s).start()
                            else:

                                @pl.when(is_long(e, j))
                                def _(c=c, e=e):
                                    ag2_copy(c, e, j, s).start()
                        else:

                            @pl.when(is_long(e, j))
                            def _(c=c, e=e):
                                ag2_landed(c, e, j, s)

    def dest_offset(i):
        ahead = lax.div(n - i, 2)
        back = lax.div(n - 1 - i, 2)
        return jnp.where(lax.rem(i, 2) == 0, ahead, -back)

    def hops(e, i):
        return jnp.where(is_long(e, i), half, half - 1)

    def rs1_chunk(c, e, i, s):
        far = (1 - 2 * e) * (hops(e, i) - s)
        return chunk(c, wrap(major_at[c] + far), wrap(minor_at[c] + dest_offset(i)))

    def rs1_copy(c, e, i, s):
        t = rs1_chunk(c, e, i, s)
        to = {major_axis[c]: wrap(major_at[c] + 1 - 2 * e)}
        return remote(p.at[c, t], rb.at[c, e, i, s], rs1_s.at[c, e, i, s], rs1_r.at[c, e, i, s], to)

    def rs1_add_send(c, e, i, s):
        t = rs1_chunk(c, e, i, s)
        p[c, t] = encode(decode(p[c, t]) + decode(rb[c, e, i, s - 1]))
        rs1_copy(c, e, i, s).start()

    def rs2_copy(c, i, right):
        t = chunk(c, major_at[c], wrap(minor_at[c] + dest_offset(i)))
        to = {minor_axis[c]: wrap(minor_at[c] + (1 if right else -1))}
        return remote(p.at[c, t], r2.at[c, i], rs2_s.at[c, i], rs2_r.at[c, i], to)

    def rs1_done(c, i):
        t = chunk(c, major_at[c], wrap(minor_at[c] + dest_offset(i)))
        total = decode(p[c, t])
        for e in range(2):
            total = total + decode(rb[c, e, i, hops(e, i) - 1])
        return t, total

    def rs2_step(i):
        for c in range(2):

            @pl.when(i < 2)
            def _(c=c):
                t, total = rs1_done(c, i)
                p[c, t] = encode(total)

            @pl.when(jnp.logical_and(i >= 2, i < n - 1))
            def _(c=c):
                landed(r2.at[c, i - 2], rs2_r.at[c, i - 2])
                t, total = rs1_done(c, i)
                p[c, t] = encode(total + decode(r2[c, i - 2]))

            @pl.when(jnp.logical_and(i < n - 1, lax.rem(i, 2) == 0))
            def _(c=c):
                rs2_copy(c, i, True).start()

            @pl.when(jnp.logical_and(i < n - 1, lax.rem(i, 2) == 1))
            def _(c=c):
                rs2_copy(c, i, False).start()

            @pl.when(i == n - 1)
            def _(c=c):
                t, total = rs1_done(c, i)
                total = total + adt[c]
                for k in (n - 3, n - 2):
                    landed(r2.at[c, k], rs2_r.at[c, k])
                    total = total + decode(r2[c, k])
                igrad[c] = total.astype(BF16)

    def rs_tick(tick):
        for s in range(half + 1):
            i = tick - s

            @pl.when(live_stream(i))
            def _(i=i, s=s):
                for c in range(2):
                    for e in range(2):
                        if s == 0:
                            rs1_copy(c, e, i, s).start()
                        elif s < half - 1:
                            landed(rb.at[c, e, i, s - 1], rs1_r.at[c, e, i, s - 1])
                            rs1_add_send(c, e, i, s)
                        elif s == half - 1:
                            landed(rb.at[c, e, i, s - 1], rs1_r.at[c, e, i, s - 1])

                            @pl.when(is_long(e, i))
                            def _(c=c, e=e):
                                rs1_add_send(c, e, i, s)
                        else:

                            @pl.when(is_long(e, i))
                            def _(c=c, e=e):
                                landed(rb.at[c, e, i, s - 1], rs1_r.at[c, e, i, s - 1])

                if s == half:
                    rs2_step(i)

    def member_of(b):
        end, count = jnp.int32(0), jnp.int32(0)
        for m in range(members):
            end = end + mb[m]
            count = count + jnp.where(end <= d * 2 + b, 1, 0)
        return count

    def weight_of(b, m):
        return jnp.where(member_of(b) == m, F32(1.0), F32(0.0))

    def live_rows(b):
        at = lax.broadcasted_iota(jnp.int32, (BLOCK, cot.shape[2]), 0)
        return jnp.where(at < bl[b], F32(1.0), F32(0.0))

    def rows(b):
        return pl.ds(b * BLOCK, BLOCK)

    def mask_step():
        for b in range(2):
            masked[rows(b)] = (cot[b].astype(F32) * live_rows(b)).astype(BF16)

    def low_rank_start():
        for k in range(2):
            ad_local(k).wait()
            ad_remote(k).wait_recv()
        for b in range(2):
            a, o = weight_of(b, 0) * ain[0].astype(F32), weight_of(b, 0) * aout[0].astype(F32)
            for m in range(1, members):
                a = a + weight_of(b, m) * ain[m].astype(F32)
                o = o + weight_of(b, m) * aout[m].astype(F32)
            cin[b], cout[b] = a.astype(BF16), o.astype(BF16)
        tall = part.shape[1]
        for b in range(2):
            into = dot(g[b, me], cin[b], NN)
            back = dot(masked[rows(b)], cout[b], NT)
            both = jnp.concatenate([into, back], axis=1)
            each = BLOCK // tall
            part[pl.ds(b * each, each)] = both.reshape(each, tall, 2 * rank)
        xbuf[x] = part[x]

    def x_copy(k):
        to = wrap(x + k)
        return remote(part.at[to], xbuf.at[x], xs.at[k], xr.at[k], {COL: to})

    def y_copy(k):
        return remote(ybuf.at[y], ybuf.at[y], ys.at[k], yr.at[k], {ROW: wrap(y + k)})

    def z_copy(k):
        return remote(low.at[x], low.at[x], zs.at[k], zr.at[k], {COL: wrap(x + k)})

    def total_of(ref):
        total = ref[0]
        for k in range(1, n):
            total = total + ref[k]
        return total

    def x_done():
        for k in range(1, n):
            landed(xbuf.at[wrap(x - k)], xr.at[k])
        ybuf[y] = total_of(xbuf)

    def y_done():
        for k in range(1, n):
            landed(ybuf.at[wrap(y - k)], yr.at[k])
        low[x] = total_of(ybuf).astype(BF16)

    def low_of(b):
        each = n // 2
        both = low[pl.ds(b * each, each)].reshape(BLOCK, 2 * rank)
        return both[:, :rank], both[:, rank:]

    def g_copy(k):
        src, dst = ((usend, urecv), (dsend, drecv))[k]
        return remote(src, dst, gx_s.at[k], gx_r.at[k], mate)

    def z_done():
        for k in range(1, n):
            landed(low.at[wrap(x - k)], zr.at[k])
        ups, downs = [], []
        for b in range(2):
            into, back = low_of(b)
            ups.append(SCALE * dot(into, masked[rows(b)], TN))
            downs.append(SCALE * dot(g[b, me], back, TN))
        for q in range(owned):
            theirs, mine = (1 - d) * owned + q, d * owned + q
            usend[q] = weight_of(0, theirs) * ups[0] + weight_of(1, theirs) * ups[1]
            dsend[q] = weight_of(0, theirs) * downs[0] + weight_of(1, theirs) * downs[1]
            ugrad[q] = weight_of(0, mine) * ups[0] + weight_of(1, mine) * ups[1]
            dgrad[q] = weight_of(0, mine) * downs[0] + weight_of(1, mine) * downs[1]

    def terms_step():
        for b in range(2):
            into, back = low_of(b)
            acc[rows(b)] = SCALE * dot(into, cout[b], NN)
            adt[b] = SCALE * dot(back, cin[b], NT)

    def grads_done():
        for k in range(2):
            g_copy(k).wait_recv()
        for q in range(owned):
            ugrad[q] = ugrad[q] + urecv[q]
            dgrad[q] = dgrad[q] + drecv[q]

    def back_chunk(k):
        t = lax.rem(d * own_chunks + k, chunks)
        out = dot(masked[...], w[t], NT)
        for b in range(2):
            p[b, t] = encode(out[b * BLOCK : (b + 1) * BLOCK])

    def front_chunk(t):
        rows_in = jnp.concatenate([g[0, t], g[1, t]], axis=0)
        acc[...] += dot(rows_in, w[t], NN)

    def hidden_step():
        for b in range(2):
            hidden[b] = (acc[rows(b)] * live_rows(b)).astype(BF16)

    def some(body, first, last):
        lax.fori_loop(first, last, lambda k, z: (body(k), z)[1], 0)

    rs_from = n
    last = rs_from + ticks - 1
    back_from, back_ticks = early, rs_from - early
    back_each = -(-chunks // back_ticks)
    front_from, front_ticks = ticks, last - 1 - ticks
    front_each = -(-chunks // front_ticks)

    def every_tick(tick, carry):
        @pl.when(tick < ticks)
        def _():
            ag_tick(tick)

        @pl.when(tick >= rs_from)
        def _():
            rs_tick(tick - rs_from)

        @pl.when(tick == 0)
        def _():
            for k in range(2):
                ad_remote(k).start()
            for q in range(pieces):
                w_remote(q).start()
            mask_step()
            low_rank_start()
            for k in range(1, n):
                x_copy(k).start()

        @pl.when(tick == early)
        def _():
            x_done()
            for k in range(1, n):
                y_copy(k).start()
            for q in range(pieces):
                w_local(q).wait()

        @pl.when(tick == middle)
        def _():
            y_done()
            for k in range(1, n):
                z_copy(k).start()
            for q in range(pieces):
                theirs = w.at[pl.ds((1 - d) * own_chunks + q * piece, piece)]
                landed(theirs, wx_r.at[q])

        @pl.when(tick == late)
        def _():
            z_done()
            for k in range(2):
                g_copy(k).start()
            terms_step()

        @pl.when(tick == rs_from + 1)
        def _():
            grads_done()

        @pl.when(jnp.logical_and(tick >= back_from, tick < back_from + back_ticks))
        def _():
            first = (tick - back_from) * back_each
            some(back_chunk, first, jnp.minimum(first + back_each, chunks))

        @pl.when(jnp.logical_and(tick >= front_from, tick < front_from + front_ticks))
        def _():
            first = (tick - front_from) * front_each
            some(front_chunk, first, jnp.minimum(first + front_each, chunks))

        @pl.when(tick == front_from + front_ticks)
        def _():
            hidden_step()

        return carry

    lax.fori_loop(0, last + 1, every_tick, 0)

    for k in range(2):
        ad_remote(k).wait_send()
        g_copy(k).wait_send()
    for q in range(pieces):
        w_remote(q).wait_send()
    for k in range(1, n):
        x_copy(k).wait_send()
        y_copy(k).wait_send()
        z_copy(k).wait_send()

    def sent(src, sem):
        pltpu.make_async_copy(src, src, sem).wait()

    def drain(j, carry):
        @pl.when(j >= 1)
        def _():
            for c in range(2):
                sent(g.at[c, 0], ag1_s.at[c, j])

        @pl.when(j < n - 1)
        def _():
            for c in range(2):
                sent(p.at[c, 0], rs2_s.at[c, j])

        for c in range(2):
            for e in range(2):
                for s in range(half - 1):
                    sent(g.at[c, 0], ag2_s.at[c, e, j, s])
                    sent(p.at[c, 0], rs1_s.at[c, e, j, s])

                @pl.when(is_long(e, j))
                def _(c=c, e=e):
                    sent(g.at[c, 0], ag2_s.at[c, e, j, half - 1])
                    sent(p.at[c, 0], rs1_s.at[c, e, j, half - 1])

        return carry

    lax.fori_loop(0, n, drain, 0)


def local(n, tokens, weight, adapter_in, adapter_out, cotangent, member_blocks, block_live):
    token_rows, width = tokens.shape
    depth, hidden_width = weight.shape
    blocks = token_rows // BLOCK
    owned, _, rank = adapter_in.shape
    members = 2 * owned
    half = n // 2
    tall = token_rows // n
    chunks = n * n
    vmem, anywhere, smem = (
        pl.BlockSpec(memory_space=s) for s in (pltpu.VMEM, pl.ANY, pltpu.SMEM)
    )
    pieces = 4
    coded = BLOCK * width // (2 * LANES) + SUBLANES
    dma = lambda *shape: pltpu.SemaphoreType.DMA(shape)
    both_ways = (2, 2, n, half)
    out = pl.pallas_call(
        functools.partial(kernel, n),
        out_shape=(
            jax.ShapeDtypeStruct((blocks, BLOCK, hidden_width), BF16),
            jax.ShapeDtypeStruct((blocks, BLOCK, width), BF16),
            jax.ShapeDtypeStruct((owned, width, rank), F32),
            jax.ShapeDtypeStruct((owned, rank, hidden_width), F32),
        ),
        in_specs=[smem, smem, anywhere, anywhere, anywhere, anywhere, vmem],
        out_specs=(vmem,) * 4,
        scratch_shapes=[
            pltpu.VMEM((blocks, chunks, BLOCK, width), BF16),
            pltpu.VMEM((chunks, width, hidden_width), BF16),
            pltpu.VMEM((blocks, chunks, coded, LANES), jnp.int32),
            pltpu.VMEM((*both_ways, coded, LANES), jnp.int32),
            pltpu.VMEM((2, n - 1, coded, LANES), jnp.int32),
            pltpu.VMEM((token_rows, hidden_width), BF16),
            pltpu.VMEM((token_rows, hidden_width), F32),
            pltpu.VMEM((blocks, BLOCK, width), F32),
            pltpu.VMEM((members, width, rank), BF16),
            pltpu.VMEM((members, rank, hidden_width), BF16),
            pltpu.VMEM((blocks, width, rank), BF16),
            pltpu.VMEM((blocks, rank, hidden_width), BF16),
            pltpu.VMEM((n, tall, 2 * rank), F32),
            pltpu.VMEM((n, tall, 2 * rank), F32),
            pltpu.VMEM((n, tall, 2 * rank), F32),
            pltpu.VMEM((n, tall, 2 * rank), BF16),
            pltpu.VMEM((owned, rank, hidden_width), F32),
            pltpu.VMEM((owned, width, rank), F32),
            pltpu.VMEM((owned, rank, hidden_width), F32),
            pltpu.VMEM((owned, width, rank), F32),
            dma(2, n),
            dma(2, n),
            dma(*both_ways),
            dma(*both_ways),
            dma(*both_ways),
            dma(*both_ways),
            dma(2, n),
            dma(2, n),
            dma(2),
            dma(pieces),
            dma(pieces),
            dma(pieces),
            dma(2),
            dma(2),
            dma(2),
            dma(n),
            dma(n),
            dma(n),
            dma(n),
            dma(n),
            dma(n),
            dma(2),
            dma(2),
        ],
        compiler_params=pltpu.CompilerParams(
            collective_id=0, has_side_effects=True, vmem_limit_bytes=62 * 2**20
        ),
        name="step",
    )(
        member_blocks,
        block_live,
        tokens.reshape(blocks, BLOCK, width),
        weight.reshape(depth // width, width, hidden_width),
        adapter_in,
        adapter_out,
        cotangent.reshape(blocks, BLOCK, hidden_width),
    )
    return (
        out[0].reshape(token_rows, hidden_width),
        out[1].reshape(token_rows, width),
        out[2],
        out[3],
    )


def solution(mesh):
    n = math.isqrt(mesh.shape["tensor"])
    tensor = (ROW, COL)
    finer = Mesh(
        mesh.devices.reshape(mesh.shape["pop"], mesh.shape["dp"], n, n), ("pop", CORE, ROW, COL)
    )
    return jax.shard_map(
        functools.partial(local, n),
        mesh=finer,
        in_specs=(
            P(("pop", "dp"), tensor),
            P("dp", tensor),
            P(("pop", "dp"), tensor, None),
            P(("pop", "dp"), None, tensor),
            P(("pop", "dp"), tensor),
            P("pop"),
            P(("pop", "dp")),
        ),
        out_specs=(
            P(("pop", "dp"), tensor),
            P(("pop", "dp"), tensor),
            P(("pop", "dp"), tensor, None),
            P(("pop", "dp"), None, tensor),
        ),
        check_vma=False,
    )
```

```python
import functools
import math

import jax
import jax.numpy as jnp
from jax import lax
from jax.experimental import pallas as pl
from jax.experimental.pallas import tpu as pltpu
from jax.sharding import Mesh
from jax.sharding import PartitionSpec as P

BLOCK = 128
SCALE = 0.5
MESH = pl.DeviceIdType.MESH
ROW, COL, CORE = "tensor_0", "tensor_1", "dp"
F32, BF16 = jnp.float32, jnp.bfloat16

NN = (((1,), (0,)), ((), ()))
NT = (((1,), (1,)), ((), ()))
TN = (((0,), (0,)), ((), ()))


def dot(a, b, dims):
    return lax.dot_general(a, b, dims, preferred_element_type=F32)


LANES, SUBLANES = 128, 8
UNIT = 2.0**21
TOP = 32760.0


def halves(v):
    return [v[:, k : k + LANES] for k in range(0, v.shape[1], LANES)]


def encode(v):
    groups = [h.reshape(-1, SUBLANES, LANES) for h in halves(v)]
    largest = functools.reduce(jnp.maximum, [jnp.max(jnp.abs(q), axis=0) for q in groups])
    scale = (largest * UNIT).astype(jnp.int32) + 1
    by = (TOP * UNIT) / scale.astype(F32)
    out = []
    for q in groups:
        code = (q * by[None]).astype(jnp.int32)
        mid = code.shape[0] // 2
        pair = (code[:mid] << 16) | (code[mid:] & 0xFFFF)
        out.append(pair.reshape(-1, LANES))
    return jnp.concatenate([*out, scale], axis=0)


def decode(code):
    scale = code[-SUBLANES:].astype(F32) * (1.0 / (TOP * UNIT))
    body = code[:-SUBLANES]
    mid = body.shape[0] // 2
    out = []
    for k in range(2):
        pair = body[k * mid : (k + 1) * mid].reshape(-1, SUBLANES, LANES)
        both = jnp.concatenate([pair >> 16, (pair << 16) >> 16], axis=0)
        out.append((both.astype(F32) * scale[None]).reshape(-1, LANES))
    return jnp.concatenate(out, axis=1)


def kernel(
    n,
    mb,
    bl,
    tok_hbm,
    w_hbm,
    ain_hbm,
    aout_hbm,
    cot,
    hidden,
    igrad,
    dgrad,
    ugrad,
    g,
    w,
    p,
    rb,
    r2,
    masked,
    acc,
    adt,
    ain,
    aout,
    cin,
    cout,
    part,
    xbuf,
    ybuf,
    low,
    usend,
    dsend,
    urecv,
    drecv,
    ag1_s,
    ag1_r,
    ag2_s,
    ag2_r,
    rs1_s,
    rs1_r,
    rs2_s,
    rs2_r,
    own_sem,
    w_sem,
    wx_s,
    wx_r,
    ad_sem,
    adx_s,
    adx_r,
    xs,
    xr,
    ys,
    yr,
    zs,
    zr,
    gx_s,
    gx_r,
):
    half = n // 2
    ticks = n + half
    early, middle, late = n // 4, n // 2, 3 * n // 4
    y, x, d = lax.axis_index(ROW), lax.axis_index(COL), lax.axis_index(CORE)
    mate = {CORE: 1 - d}
    me = y * n + x
    chunks = n * n
    members = ain.shape[0]
    owned = members // 2
    width = g.shape[3]
    own_depth = w_hbm.shape[1]
    own_chunks = own_depth // width
    pieces = w_sem.shape[0]
    piece = own_depth // pieces
    rank = ain.shape[1]
    minor_axis, major_axis = (COL, ROW), (ROW, COL)
    minor_at, major_at = (x, y), (y, x)

    def chunk(c, major, minor):
        return major * n + minor if c == 0 else minor * n + major

    def wrap(v):
        return lax.rem(v + 2 * n, n)

    def remote(src, dst, ss, rs, to):
        return pltpu.make_async_remote_copy(
            src_ref=src, dst_ref=dst, send_sem=ss, recv_sem=rs, device_id=to, device_id_type=MESH
        )

    def landed(dst, sem):
        pltpu.make_async_copy(dst, dst, sem).wait()

    for c in range(2):
        pltpu.make_async_copy(tok_hbm.at[c], g.at[c, me], own_sem.at[c]).start()
    barrier = pltpu.get_barrier_semaphore()
    for k in range(1, n):
        pl.semaphore_signal(barrier, inc=1, device_id={COL: wrap(x + k)}, device_id_type=MESH)
        pl.semaphore_signal(barrier, inc=1, device_id={ROW: wrap(y + k)}, device_id_type=MESH)
    pl.semaphore_signal(barrier, inc=1, device_id=mate, device_id_type=MESH)

    def ad_local(k):
        hbm, vm = ((ain_hbm, ain), (aout_hbm, aout))[k]
        return pltpu.make_async_copy(hbm, vm.at[pl.ds(d * owned, owned)], ad_sem.at[k])

    def ad_remote(k):
        hbm, vm = ((ain_hbm, ain), (aout_hbm, aout))[k]
        return remote(hbm, vm.at[pl.ds(d * owned, owned)], adx_s.at[k], adx_r.at[k], mate)

    def w_piece(core, q):
        return w.at[:, pl.ds(pl.multiple_of(core * own_depth + q * piece, LANES), piece)]

    def w_local(q):
        src = w_hbm.at[:, pl.ds(q * piece, piece)]
        return pltpu.make_async_copy(src, w_piece(d, q), w_sem.at[q])

    def w_remote(q):
        src = w_hbm.at[:, pl.ds(q * piece, piece)]
        return remote(src, w_piece(d, q), wx_s.at[q], wx_r.at[q], mate)

    def w_chunk(t):
        return w[:, pl.ds(pl.multiple_of(t * width, LANES), width)]

    for k in range(2):
        ad_local(k).start()
    for q in range(pieces):
        w_local(q).start()
    for c in range(2):
        landed(g.at[c, me], own_sem.at[c])
    pl.semaphore_wait(barrier, 2 * (n - 1) + 1)

    def minor_offset(j):
        back = lax.div(j + 1, 2)
        return jnp.where(lax.rem(j, 2) == 1, -back, lax.div(j, 2))

    def ag1_copy(c, j, right):
        src = chunk(c, major_at[c], wrap(minor_at[c] + minor_offset(j)))
        lands = jnp.where(j == 0, 1 if right else 2, j + 2)
        to = {minor_axis[c]: wrap(minor_at[c] + (1 if right else -1))}
        return remote(g.at[c, src], g.at[c, src], ag1_s.at[c, lands], ag1_r.at[c, lands], to)

    def ag1_step(j):
        for c in range(2):
            src = chunk(c, major_at[c], wrap(minor_at[c] + minor_offset(j)))

            @pl.when(j >= 1)
            def _(c=c, src=src):
                landed(g.at[c, src], ag1_r.at[c, j])

            @pl.when(jnp.logical_or(j == 0, jnp.logical_and(lax.rem(j, 2) == 1, j + 2 < n)))
            def _(c=c):
                ag1_copy(c, j, True).start()

            @pl.when(jnp.logical_and(lax.rem(j, 2) == 0, j + 2 < n))
            def _(c=c):
                ag1_copy(c, j, False).start()

    def ag2_copy(c, e, j, s):
        way = 1 - 2 * e
        t = chunk(c, wrap(major_at[c] - way * s), wrap(minor_at[c] + minor_offset(j)))
        to = {major_axis[c]: wrap(major_at[c] + way)}
        return remote(g.at[c, t], g.at[c, t], ag2_s.at[c, e, j, s], ag2_r.at[c, e, j, s], to)

    def ag2_landed(c, e, j, s):
        t = chunk(c, wrap(major_at[c] - (1 - 2 * e) * s), wrap(minor_at[c] + minor_offset(j)))
        landed(g.at[c, t], ag2_r.at[c, e, j, s - 1])

    def is_long(e, j):
        return lax.rem(j, 2) == e

    def live_stream(j):
        return jnp.logical_and(j >= 0, j < n)

    def ag_tick(tick):
        @pl.when(tick < n)
        def _():
            ag1_step(tick)

        for s in range(half + 1):
            j = tick - s

            @pl.when(live_stream(j))
            def _(j=j, s=s):
                for c in range(2):
                    for e in range(2):
                        if s < half:
                            if s > 0:
                                ag2_landed(c, e, j, s)
                            if s < half - 1:
                                ag2_copy(c, e, j, s).start()
                            else:

                                @pl.when(is_long(e, j))
                                def _(c=c, e=e):
                                    ag2_copy(c, e, j, s).start()
                        else:

                            @pl.when(is_long(e, j))
                            def _(c=c, e=e):
                                ag2_landed(c, e, j, s)

    def dest_offset(i):
        ahead = lax.div(n - i, 2)
        back = lax.div(n - 1 - i, 2)
        return jnp.where(lax.rem(i, 2) == 0, ahead, -back)

    def hops(e, i):
        return jnp.where(is_long(e, i), half, half - 1)

    def rs1_chunk(c, e, i, s):
        far = (1 - 2 * e) * (hops(e, i) - s)
        return chunk(c, wrap(major_at[c] + far), wrap(minor_at[c] + dest_offset(i)))

    def rs1_copy(c, e, i, s):
        t = rs1_chunk(c, e, i, s)
        to = {major_axis[c]: wrap(major_at[c] + 1 - 2 * e)}
        return remote(p.at[c, t], rb.at[c, e, i, s], rs1_s.at[c, e, i, s], rs1_r.at[c, e, i, s], to)

    def rs1_add_send(c, e, i, s):
        t = rs1_chunk(c, e, i, s)
        p[c, t] = encode(decode(p[c, t]) + decode(rb[c, e, i, s - 1]))
        rs1_copy(c, e, i, s).start()

    def rs2_copy(c, i, right):
        t = chunk(c, major_at[c], wrap(minor_at[c] + dest_offset(i)))
        to = {minor_axis[c]: wrap(minor_at[c] + (1 if right else -1))}
        return remote(p.at[c, t], r2.at[c, i], rs2_s.at[c, i], rs2_r.at[c, i], to)

    def rs1_done(c, i):
        t = chunk(c, major_at[c], wrap(minor_at[c] + dest_offset(i)))
        total = decode(p[c, t])
        for e in range(2):
            total = total + decode(rb[c, e, i, hops(e, i) - 1])
        return t, total

    def rs2_step(i):
        for c in range(2):

            @pl.when(i < 2)
            def _(c=c):
                t, total = rs1_done(c, i)
                p[c, t] = encode(total)

            @pl.when(jnp.logical_and(i >= 2, i < n - 1))
            def _(c=c):
                landed(r2.at[c, i - 2], rs2_r.at[c, i - 2])
                t, total = rs1_done(c, i)
                p[c, t] = encode(total + decode(r2[c, i - 2]))

            @pl.when(jnp.logical_and(i < n - 1, lax.rem(i, 2) == 0))
            def _(c=c):
                rs2_copy(c, i, True).start()

            @pl.when(jnp.logical_and(i < n - 1, lax.rem(i, 2) == 1))
            def _(c=c):
                rs2_copy(c, i, False).start()

            @pl.when(i == n - 1)
            def _(c=c):
                t, total = rs1_done(c, i)
                total = total + adt[c]
                for k in (n - 3, n - 2):
                    landed(r2.at[c, k], rs2_r.at[c, k])
                    total = total + decode(r2[c, k])
                igrad[c] = total.astype(BF16)

    def rs_tick(tick):
        for s in range(half + 1):
            i = tick - s

            @pl.when(live_stream(i))
            def _(i=i, s=s):
                for c in range(2):
                    for e in range(2):
                        if s == 0:
                            rs1_copy(c, e, i, s).start()
                        elif s < half - 1:
                            landed(rb.at[c, e, i, s - 1], rs1_r.at[c, e, i, s - 1])
                            rs1_add_send(c, e, i, s)
                        elif s == half - 1:
                            landed(rb.at[c, e, i, s - 1], rs1_r.at[c, e, i, s - 1])

                            @pl.when(is_long(e, i))
                            def _(c=c, e=e):
                                rs1_add_send(c, e, i, s)
                        else:

                            @pl.when(is_long(e, i))
                            def _(c=c, e=e):
                                landed(rb.at[c, e, i, s - 1], rs1_r.at[c, e, i, s - 1])

                if s == half:
                    rs2_step(i)

    def member_of(b):
        end, count = jnp.int32(0), jnp.int32(0)
        for m in range(members):
            end = end + mb[m]
            count = count + jnp.where(end <= d * 2 + b, 1, 0)
        return count

    def weight_of(b, m):
        return jnp.where(member_of(b) == m, F32(1.0), F32(0.0))

    def live(b, shape, dim):
        at = lax.broadcasted_iota(jnp.int32, shape, dim)
        return jnp.where(at < bl[b], F32(1.0), F32(0.0))

    def rows(b):
        return pl.ds(b * BLOCK, BLOCK)

    def mask_step():
        for b in range(2):
            across = jnp.transpose(cot[:, b * BLOCK : (b + 1) * BLOCK].astype(F32))
            masked[rows(b)] = (across * live(b, across.shape, 0)).astype(BF16)

    def low_rank_start():
        for k in range(2):
            ad_local(k).wait()
            ad_remote(k).wait_recv()
        for b in range(2):
            a, o = weight_of(b, 0) * ain[0].astype(F32), weight_of(b, 0) * aout[0].astype(F32)
            for m in range(1, members):
                a = a + weight_of(b, m) * ain[m].astype(F32)
                o = o + weight_of(b, m) * aout[m].astype(F32)
            cin[b], cout[b] = a.astype(BF16), o.astype(BF16)
        tall = part.shape[1]
        for b in range(2):
            into = dot(g[b, me], cin[b], NT)
            back = dot(masked[rows(b)], cout[b], NT)
            both = jnp.concatenate([into, back], axis=1)
            each = BLOCK // tall
            part[pl.ds(b * each, each)] = both.reshape(each, tall, 2 * rank)
        xbuf[x] = part[x]

    def x_copy(k):
        to = wrap(x + k)
        return remote(part.at[to], xbuf.at[x], xs.at[k], xr.at[k], {COL: to})

    def y_copy(k):
        return remote(ybuf.at[y], ybuf.at[y], ys.at[k], yr.at[k], {ROW: wrap(y + k)})

    def z_copy(k):
        return remote(low.at[x], low.at[x], zs.at[k], zr.at[k], {COL: wrap(x + k)})

    def total_of(ref):
        total = ref[0]
        for k in range(1, n):
            total = total + ref[k]
        return total

    def x_done():
        for k in range(1, n):
            landed(xbuf.at[wrap(x - k)], xr.at[k])
        ybuf[y] = total_of(xbuf)

    def y_done():
        for k in range(1, n):
            landed(ybuf.at[wrap(y - k)], yr.at[k])
        low[x] = total_of(ybuf).astype(BF16)

    def low_of(b):
        each = n // 2
        both = low[pl.ds(b * each, each)].reshape(BLOCK, 2 * rank)
        return both[:, :rank], both[:, rank:]

    def g_copy(k):
        src, dst = ((usend, urecv), (dsend, drecv))[k]
        return remote(src, dst, gx_s.at[k], gx_r.at[k], mate)

    def z_done():
        for k in range(1, n):
            landed(low.at[wrap(x - k)], zr.at[k])
        ups, downs = [], []
        for b in range(2):
            into, back = low_of(b)
            ups.append(SCALE * dot(into, masked[rows(b)], TN))
            downs.append(SCALE * dot(back, g[b, me], TN))
        for q in range(owned):
            theirs, mine = (1 - d) * owned + q, d * owned + q
            usend[q] = weight_of(0, theirs) * ups[0] + weight_of(1, theirs) * ups[1]
            dsend[q] = weight_of(0, theirs) * downs[0] + weight_of(1, theirs) * downs[1]
            ugrad[q] = weight_of(0, mine) * ups[0] + weight_of(1, mine) * ups[1]
            dgrad[q] = weight_of(0, mine) * downs[0] + weight_of(1, mine) * downs[1]

    def terms_step():
        for b in range(2):
            into, back = low_of(b)
            turned = jnp.transpose(into.astype(F32)).astype(BF16)
            acc[:, b * BLOCK : (b + 1) * BLOCK] = SCALE * dot(cout[b], turned, TN)
            adt[b] = SCALE * dot(back, cin[b], NN)

    def grads_done():
        for k in range(2):
            g_copy(k).wait_recv()
        for q in range(owned):
            ugrad[q] = ugrad[q] + urecv[q]
            dgrad[q] = dgrad[q] + drecv[q]

    def back_chunk(k):
        t = lax.rem(d * own_chunks + k, chunks)
        out = dot(masked[...], w_chunk(t), NN)
        for b in range(2):
            p[b, t] = encode(out[b * BLOCK : (b + 1) * BLOCK])

    def front_chunk(t):
        rows_in = jnp.concatenate([g[0, t], g[1, t]], axis=0)
        acc[...] += dot(w_chunk(t), rows_in, NT)

    def hidden_step():
        for b in range(2):
            cols = acc[:, b * BLOCK : (b + 1) * BLOCK]
            hidden[:, b * BLOCK : (b + 1) * BLOCK] = (cols * live(b, cols.shape, 1)).astype(BF16)

    def some(body, first, last):
        lax.fori_loop(first, last, lambda k, z: (body(k), z)[1], 0)

    rs_from = n
    last = rs_from + ticks - 1
    back_from, back_ticks = early, rs_from - early
    back_each = -(-chunks // back_ticks)
    front_from, front_ticks = ticks, last - 1 - ticks
    front_each = -(-chunks // front_ticks)

    def every_tick(tick, carry):
        @pl.when(tick < ticks)
        def _():
            ag_tick(tick)

        @pl.when(tick >= rs_from)
        def _():
            rs_tick(tick - rs_from)

        @pl.when(tick == 0)
        def _():
            for k in range(2):
                ad_remote(k).start()
            for q in range(pieces):
                w_remote(q).start()
            mask_step()
            low_rank_start()
            for k in range(1, n):
                x_copy(k).start()

        @pl.when(tick == early)
        def _():
            x_done()
            for k in range(1, n):
                y_copy(k).start()
            for q in range(pieces):
                w_local(q).wait()

        @pl.when(tick == middle)
        def _():
            y_done()
            for k in range(1, n):
                z_copy(k).start()
            for q in range(pieces):
                landed(w_piece(1 - d, q), wx_r.at[q])

        @pl.when(tick == late)
        def _():
            z_done()
            for k in range(2):
                g_copy(k).start()
            terms_step()

        @pl.when(tick == rs_from + 1)
        def _():
            grads_done()

        @pl.when(jnp.logical_and(tick >= back_from, tick < back_from + back_ticks))
        def _():
            first = (tick - back_from) * back_each
            some(back_chunk, first, jnp.minimum(first + back_each, chunks))

        @pl.when(jnp.logical_and(tick >= front_from, tick < front_from + front_ticks))
        def _():
            first = (tick - front_from) * front_each
            some(front_chunk, first, jnp.minimum(first + front_each, chunks))

        @pl.when(tick == front_from + front_ticks)
        def _():
            hidden_step()

        return carry

    lax.fori_loop(0, last + 1, every_tick, 0)

    for k in range(2):
        ad_remote(k).wait_send()
        g_copy(k).wait_send()
    for q in range(pieces):
        w_remote(q).wait_send()
    for k in range(1, n):
        x_copy(k).wait_send()
        y_copy(k).wait_send()
        z_copy(k).wait_send()

    def sent(src, sem):
        pltpu.make_async_copy(src, src, sem).wait()

    def drain(j, carry):
        @pl.when(j >= 1)
        def _():
            for c in range(2):
                sent(g.at[c, 0], ag1_s.at[c, j])

        @pl.when(j < n - 1)
        def _():
            for c in range(2):
                sent(p.at[c, 0], rs2_s.at[c, j])

        for c in range(2):
            for e in range(2):
                for s in range(half - 1):
                    sent(g.at[c, 0], ag2_s.at[c, e, j, s])
                    sent(p.at[c, 0], rs1_s.at[c, e, j, s])

                @pl.when(is_long(e, j))
                def _(c=c, e=e):
                    sent(g.at[c, 0], ag2_s.at[c, e, j, half - 1])
                    sent(p.at[c, 0], rs1_s.at[c, e, j, half - 1])

        return carry

    lax.fori_loop(0, n, drain, 0)


def hand_over(*refs):
    for src, dst in zip(refs[:4], refs[4:]):
        dst[...] = src[...]


def local(n, tokens, weight, adapter_in, adapter_out, cotangent, member_blocks, block_live):
    token_rows, width = tokens.shape
    hidden_width = weight.shape[1]
    blocks = token_rows // BLOCK
    owned, _, rank = adapter_in.shape
    members = 2 * owned
    half = n // 2
    tall = token_rows // n
    chunks = n * n
    vmem, anywhere, smem = (
        pl.BlockSpec(memory_space=s) for s in (pltpu.VMEM, pl.ANY, pltpu.SMEM)
    )
    pieces = 4
    coded = BLOCK * width // (2 * LANES) + SUBLANES
    dma = lambda *shape: pltpu.SemaphoreType.DMA(shape)
    both_ways = (2, 2, n, half)
    out = pl.pallas_call(
        functools.partial(kernel, n),
        out_shape=(
            jax.ShapeDtypeStruct((hidden_width, token_rows), BF16),
            jax.ShapeDtypeStruct((blocks, BLOCK, width), BF16),
            jax.ShapeDtypeStruct((owned, rank, width), F32),
            jax.ShapeDtypeStruct((owned, rank, hidden_width), F32),
        ),
        in_specs=[smem, smem, anywhere, anywhere, anywhere, anywhere, vmem],
        out_specs=(vmem,) * 4,
        scratch_shapes=[
            pltpu.VMEM((blocks, chunks, BLOCK, width), BF16),
            pltpu.VMEM((hidden_width, chunks * width), BF16),
            pltpu.VMEM((blocks, chunks, coded, LANES), jnp.int32),
            pltpu.VMEM((*both_ways, coded, LANES), jnp.int32),
            pltpu.VMEM((2, n - 1, coded, LANES), jnp.int32),
            pltpu.VMEM((token_rows, hidden_width), BF16),
            pltpu.VMEM((hidden_width, token_rows), F32),
            pltpu.VMEM((blocks, BLOCK, width), F32),
            pltpu.VMEM((members, rank, width), BF16),
            pltpu.VMEM((members, rank, hidden_width), BF16),
            pltpu.VMEM((blocks, rank, width), BF16),
            pltpu.VMEM((blocks, rank, hidden_width), BF16),
            pltpu.VMEM((n, tall, 2 * rank), F32),
            pltpu.VMEM((n, tall, 2 * rank), F32),
            pltpu.VMEM((n, tall, 2 * rank), F32),
            pltpu.VMEM((n, tall, 2 * rank), BF16),
            pltpu.VMEM((owned, rank, hidden_width), F32),
            pltpu.VMEM((owned, rank, width), F32),
            pltpu.VMEM((owned, rank, hidden_width), F32),
            pltpu.VMEM((owned, rank, width), F32),
            dma(2, n),
            dma(2, n),
            dma(*both_ways),
            dma(*both_ways),
            dma(*both_ways),
            dma(*both_ways),
            dma(2, n),
            dma(2, n),
            dma(2),
            dma(pieces),
            dma(pieces),
            dma(pieces),
            dma(2),
            dma(2),
            dma(2),
            dma(n),
            dma(n),
            dma(n),
            dma(n),
            dma(n),
            dma(n),
            dma(2),
            dma(2),
        ],
        compiler_params=pltpu.CompilerParams(
            collective_id=0, has_side_effects=True, vmem_limit_bytes=62 * 2**20
        ),
        name="step",
    )(
        member_blocks,
        block_live,
        tokens.reshape(blocks, BLOCK, width),
        weight.T,
        jnp.swapaxes(adapter_in, 1, 2),
        adapter_out,
        cotangent.T,
    )
    out = pl.pallas_call(
        hand_over,
        out_shape=tuple(jax.ShapeDtypeStruct(o.shape, o.dtype) for o in out),
        in_specs=[vmem] * 4,
        out_specs=(vmem,) * 4,
        name="hand_over",
    )(*out)
    return (
        out[0].T,
        out[1].reshape(token_rows, width),
        jnp.swapaxes(out[2], 1, 2),
        out[3],
    )


def solution(mesh):
    n = math.isqrt(mesh.shape["tensor"])
    tensor = (ROW, COL)
    finer = Mesh(
        mesh.devices.reshape(mesh.shape["pop"], mesh.shape["dp"], n, n), ("pop", CORE, ROW, COL)
    )
    return jax.shard_map(
        functools.partial(local, n),
        mesh=finer,
        in_specs=(
            P(("pop", "dp"), tensor),
            P("dp", tensor),
            P(("pop", "dp"), tensor, None),
            P(("pop", "dp"), None, tensor),
            P(("pop", "dp"), tensor),
            P("pop"),
            P(("pop", "dp")),
        ),
        out_specs=(
            P(("pop", "dp"), tensor),
            P(("pop", "dp"), tensor),
            P(("pop", "dp"), tensor, None),
            P(("pop", "dp"), None, tensor),
        ),
        check_vma=False,
    )
```

```python
import functools
import math

import jax
import jax.numpy as jnp
from jax import lax
from jax.experimental import pallas as pl
from jax.experimental.pallas import tpu as pltpu
from jax.sharding import Mesh
from jax.sharding import PartitionSpec as P

BLOCK = 128
SCALE = 0.5
MESH = pl.DeviceIdType.MESH
ROW, COL, CORE = "tensor_0", "tensor_1", "dp"
F32, BF16 = jnp.float32, jnp.bfloat16

NN = (((1,), (0,)), ((), ()))
NT = (((1,), (1,)), ((), ()))
TN = (((0,), (0,)), ((), ()))


def dot(a, b, dims):
    return lax.dot_general(a, b, dims, preferred_element_type=F32)


LANES = 128
UNIT = 2.0**21
TOP = 32760.0


def halves(v):
    return [v[:, k : k + LANES] for k in range(0, v.shape[1], LANES)]


def put(ref, at, v):
    parts = halves(v)
    largest = jnp.max(functools.reduce(jnp.maximum, [jnp.abs(q) for q in parts]), axis=0, keepdims=True)
    scale = (largest * UNIT).astype(jnp.int32) + 1
    by = (TOP * UNIT) / scale.astype(F32)
    mid = v.shape[0] // 2
    for k, q in enumerate(parts):
        code = (q * by).astype(jnp.int32)
        ref[(*at, slice(k * mid, (k + 1) * mid))] = (code[:mid] << 16) | (code[mid:] & 0xFFFF)
    ref[(*at, slice(2 * mid, 2 * mid + 1))] = scale


def get(ref, at):
    mid = (ref.shape[-2] - 1) // 2
    scale = ref[(*at, slice(2 * mid, 2 * mid + 1))].astype(F32) * (1.0 / (TOP * UNIT))
    out = []
    for k in range(2):
        pair = ref[(*at, slice(k * mid, (k + 1) * mid))]
        both = jnp.concatenate([pair >> 16, (pair << 16) >> 16], axis=0)
        out.append(both.astype(F32) * scale)
    return jnp.concatenate(out, axis=1)


def kernel(
    n,
    mb_hbm,
    bl_hbm,
    tok_hbm,
    w_hbm,
    ain_hbm,
    aout_hbm,
    cot_hbm,
    hidden_hbm,
    igrad_hbm,
    dgrad_hbm,
    ugrad_hbm,
    mb,
    bl,
    cot,
    hidden,
    igrad,
    dgrad,
    ugrad,
    g,
    w,
    p,
    rb,
    r2,
    masked,
    acc,
    adt,
    ain,
    aout,
    cin,
    cout,
    part,
    xbuf,
    ybuf,
    low,
    usend,
    dsend,
    urecv,
    drecv,
    ag1_s,
    ag1_r,
    ag2_s,
    ag2_r,
    rs1_s,
    rs1_r,
    rs2_s,
    rs2_r,
    own_sem,
    w_sem,
    wx_s,
    wx_r,
    ad_sem,
    adx_s,
    adx_r,
    xs,
    xr,
    ys,
    yr,
    zs,
    zr,
    gx_s,
    gx_r,
    in_sem,
    out_sem,
    here,
):
    half = n // 2
    ticks = n + half
    early, middle = n // 4, n // 2
    low_from = early
    low_to = low_from + 3 * half
    y, x, d = lax.axis_index(ROW), lax.axis_index(COL), lax.axis_index(CORE)
    mate = {CORE: 1 - d}
    me = y * n + x
    chunks = n * n
    members = ain.shape[0]
    owned = members // 2
    width = g.shape[3]
    own_depth = w_hbm.shape[1]
    own_chunks = own_depth // width
    pieces = w_sem.shape[0]
    piece = own_depth // pieces
    rank = ain.shape[1]
    minor_axis, major_axis = (COL, ROW), (ROW, COL)
    minor_at, major_at = (x, y), (y, x)

    def chunk(c, major, minor):
        return major * n + minor if c == 0 else minor * n + major

    def wrap(v):
        return lax.rem(v + 2 * n, n)

    def remote(src, dst, ss, rs, to):
        return pltpu.make_async_remote_copy(
            src_ref=src, dst_ref=dst, send_sem=ss, recv_sem=rs, device_id=to, device_id_type=MESH
        )

    def landed(dst, sem):
        pltpu.make_async_copy(dst, dst, sem).wait()

    barrier = pltpu.get_barrier_semaphore()
    for step in (1, n - 1):
        pl.semaphore_signal(barrier, inc=1, device_id={COL: wrap(x + step)}, device_id_type=MESH)
        pl.semaphore_signal(barrier, inc=1, device_id={ROW: wrap(y + step)}, device_id_type=MESH)

    @pl.when(d == 1)
    def _():
        pl.semaphore_signal(barrier, inc=1, device_id=mate, device_id_type=MESH)

    for c in range(2):
        pltpu.make_async_copy(tok_hbm.at[c], g.at[c, me], own_sem.at[c]).start()
    taken = ((mb_hbm, mb), (bl_hbm, bl), (cot_hbm, cot))
    given = ((hidden, hidden_hbm), (igrad, igrad_hbm), (dgrad, dgrad_hbm), (ugrad, ugrad_hbm))

    def take(k):
        return pltpu.make_async_copy(*taken[k], in_sem.at[k])

    def give(k):
        return pltpu.make_async_copy(*given[k], out_sem.at[k])

    for k in range(3):
        take(k).start()

    def ad_local(k):
        hbm, vm = ((ain_hbm, ain), (aout_hbm, aout))[k]
        return pltpu.make_async_copy(hbm, vm.at[pl.ds(d * owned, owned)], ad_sem.at[k])

    def ad_remote(k):
        hbm, vm = ((ain_hbm, ain), (aout_hbm, aout))[k]
        return remote(hbm, vm.at[pl.ds(d * owned, owned)], adx_s.at[k], adx_r.at[k], mate)

    def w_piece(core, q):
        return w.at[:, pl.ds(pl.multiple_of(core * own_depth + q * piece, LANES), piece)]

    def w_local(q):
        src = w_hbm.at[:, pl.ds(q * piece, piece)]
        return pltpu.make_async_copy(src, w_piece(d, q), w_sem.at[q])

    def w_remote(q):
        src = w_hbm.at[:, pl.ds(q * piece, piece)]
        return remote(src, w_piece(d, q), wx_s.at[q], wx_r.at[q], mate)

    def w_chunk(t):
        return w[:, pl.ds(pl.multiple_of(t * width, LANES), width)]

    for k in range(2):
        ad_local(k).start()
    for q in range(pieces):
        w_local(q).start()
    for c in range(2):
        landed(g.at[c, me], own_sem.at[c])
    pl.semaphore_wait(barrier, 4 + 1 - d)

    @pl.when(d == 0)
    def _():
        pl.semaphore_signal(here, inc=1, device_id=mate, device_id_type=MESH)


    def minor_offset(j):
        back = lax.div(j + 1, 2)
        return jnp.where(lax.rem(j, 2) == 1, -back, lax.div(j, 2))

    def ag1_copy(c, j, right):
        src = chunk(c, major_at[c], wrap(minor_at[c] + minor_offset(j)))
        lands = jnp.where(j == 0, 1 if right else 2, j + 2)
        to = {minor_axis[c]: wrap(minor_at[c] + (1 if right else -1))}
        return remote(g.at[c, src], g.at[c, src], ag1_s.at[c, lands], ag1_r.at[c, lands], to)

    def ag1_step(j):
        for c in range(2):
            src = chunk(c, major_at[c], wrap(minor_at[c] + minor_offset(j)))

            @pl.when(j >= 1)
            def _(c=c, src=src):
                landed(g.at[c, src], ag1_r.at[c, j])

            @pl.when(jnp.logical_or(j == 0, jnp.logical_and(lax.rem(j, 2) == 1, j + 2 < n)))
            def _(c=c):
                ag1_copy(c, j, True).start()

            @pl.when(jnp.logical_and(lax.rem(j, 2) == 0, j + 2 < n))
            def _(c=c):
                ag1_copy(c, j, False).start()

    def ag2_copy(c, e, j, s):
        way = 1 - 2 * e
        t = chunk(c, wrap(major_at[c] - way * s), wrap(minor_at[c] + minor_offset(j)))
        to = {major_axis[c]: wrap(major_at[c] + way)}
        return remote(g.at[c, t], g.at[c, t], ag2_s.at[c, e, j, s], ag2_r.at[c, e, j, s], to)

    def ag2_landed(c, e, j, s):
        t = chunk(c, wrap(major_at[c] - (1 - 2 * e) * s), wrap(minor_at[c] + minor_offset(j)))
        landed(g.at[c, t], ag2_r.at[c, e, j, s - 1])

    def is_long(e, j):
        return lax.rem(j, 2) == e

    def live_stream(j):
        return jnp.logical_and(j >= 0, j < n)

    def ag_tick(tick):
        @pl.when(tick < n)
        def _():
            ag1_step(tick)

        for s in range(half + 1):
            j = tick - s

            @pl.when(live_stream(j))
            def _(j=j, s=s):
                for c in range(2):
                    for e in range(2):
                        if s < half:
                            if s > 0:
                                ag2_landed(c, e, j, s)
                            if s < half - 1:
                                ag2_copy(c, e, j, s).start()
                            else:

                                @pl.when(is_long(e, j))
                                def _(c=c, e=e):
                                    ag2_copy(c, e, j, s).start()
                        else:

                            @pl.when(is_long(e, j))
                            def _(c=c, e=e):
                                ag2_landed(c, e, j, s)

    def dest_offset(i):
        ahead = lax.div(n - i, 2)
        back = lax.div(n - 1 - i, 2)
        return jnp.where(lax.rem(i, 2) == 0, ahead, -back)

    def hops(e, i):
        return jnp.where(is_long(e, i), half, half - 1)

    def rs1_chunk(c, e, i, s):
        far = (1 - 2 * e) * (hops(e, i) - s)
        return chunk(c, wrap(major_at[c] + far), wrap(minor_at[c] + dest_offset(i)))

    def rs1_copy(c, e, i, s):
        t = rs1_chunk(c, e, i, s)
        to = {major_axis[c]: wrap(major_at[c] + 1 - 2 * e)}
        return remote(p.at[c, t], rb.at[c, e, i, s], rs1_s.at[c, e, i, s], rs1_r.at[c, e, i, s], to)

    def rs1_add_send(c, e, i, s):
        t = rs1_chunk(c, e, i, s)
        put(p, (c, t), get(p, (c, t)) + get(rb, (c, e, i, s - 1)))
        rs1_copy(c, e, i, s).start()

    def rs2_copy(c, i, right):
        t = chunk(c, major_at[c], wrap(minor_at[c] + dest_offset(i)))
        to = {minor_axis[c]: wrap(minor_at[c] + (1 if right else -1))}
        return remote(p.at[c, t], r2.at[c, i], rs2_s.at[c, i], rs2_r.at[c, i], to)

    def rs1_done(c, i):
        t = chunk(c, major_at[c], wrap(minor_at[c] + dest_offset(i)))
        total = get(p, (c, t))
        for e in range(2):
            total = total + get(rb, (c, e, i, hops(e, i) - 1))
        return t, total

    def rs2_step(i):
        for c in range(2):

            @pl.when(i < 2)
            def _(c=c):
                t, total = rs1_done(c, i)
                put(p, (c, t), total)

            @pl.when(jnp.logical_and(i >= 2, i < n - 1))
            def _(c=c):
                landed(r2.at[c, i - 2], rs2_r.at[c, i - 2])
                t, total = rs1_done(c, i)
                put(p, (c, t), total + get(r2, (c, i - 2)))

            @pl.when(jnp.logical_and(i < n - 1, lax.rem(i, 2) == 0))
            def _(c=c):
                rs2_copy(c, i, True).start()

            @pl.when(jnp.logical_and(i < n - 1, lax.rem(i, 2) == 1))
            def _(c=c):
                rs2_copy(c, i, False).start()

            @pl.when(i == n - 1)
            def _(c=c):
                t, total = rs1_done(c, i)
                total = total + adt[c]
                for k in (n - 3, n - 2):
                    landed(r2.at[c, k], rs2_r.at[c, k])
                    total = total + get(r2, (c, k))
                igrad[c] = total.astype(BF16)

    def rs_tick(tick):
        for s in range(half + 1):
            i = tick - s

            @pl.when(live_stream(i))
            def _(i=i, s=s):
                for c in range(2):
                    for e in range(2):
                        if s == 0:
                            rs1_copy(c, e, i, s).start()
                        elif s < half - 1:
                            landed(rb.at[c, e, i, s - 1], rs1_r.at[c, e, i, s - 1])
                            rs1_add_send(c, e, i, s)
                        elif s == half - 1:
                            landed(rb.at[c, e, i, s - 1], rs1_r.at[c, e, i, s - 1])

                            @pl.when(is_long(e, i))
                            def _(c=c, e=e):
                                rs1_add_send(c, e, i, s)
                        else:

                            @pl.when(is_long(e, i))
                            def _(c=c, e=e):
                                landed(rb.at[c, e, i, s - 1], rs1_r.at[c, e, i, s - 1])

                if s == half:
                    rs2_step(i)

    def member_of(b):
        end, count = jnp.int32(0), jnp.int32(0)
        for m in range(members):
            end = end + mb[m]
            count = count + jnp.where(end <= d * 2 + b, 1, 0)
        return count

    def weight_of(b, m):
        return jnp.where(member_of(b) == m, F32(1.0), F32(0.0))

    def live(b, shape, dim):
        at = lax.broadcasted_iota(jnp.int32, shape, dim)
        return jnp.where(at < bl[b], F32(1.0), F32(0.0))

    def rows(b):
        return pl.ds(b * BLOCK, BLOCK)

    def mask_step():
        for b in range(2):
            across = jnp.transpose(cot[:, b * BLOCK : (b + 1) * BLOCK].astype(F32))
            masked[rows(b)] = (across * live(b, across.shape, 0)).astype(BF16)

    def low_rank_start():
        for k in range(2):
            ad_local(k).wait()
            ad_remote(k).wait_recv()
        for b in range(2):
            a, o = weight_of(b, 0) * ain[0].astype(F32), weight_of(b, 0) * aout[0].astype(F32)
            for m in range(1, members):
                a = a + weight_of(b, m) * ain[m].astype(F32)
                o = o + weight_of(b, m) * aout[m].astype(F32)
            cin[b], cout[b] = a.astype(BF16), o.astype(BF16)
        tall = part.shape[1]
        for b in range(2):
            into = dot(g[b, me], cin[b], NT)
            back = dot(masked[rows(b)], cout[b], NT)
            both = jnp.concatenate([into, back], axis=1)
            each = BLOCK // tall
            part[pl.ds(b * each, each)] = both.reshape(each, tall, 2 * rank)

    def x_copy(e, s):
        way = 1 - 2 * e
        piece = wrap(x + way * (half - e - s))
        to = {COL: wrap(x + way)}
        return remote(part.at[piece], xbuf.at[e, s], xs.at[e, s], xr.at[e, s], to)

    def x_step(s):
        for e in range(2):
            if 1 <= s <= half - e:
                piece = wrap(x + (1 - 2 * e) * (half - e - s))
                landed(xbuf.at[e, s - 1], xr.at[e, s - 1])
                part[piece] = part[piece] + xbuf[e, s - 1]
            if s < half - e:
                x_copy(e, s).start()

    def round_copy(buf, at, axis, ss, rs, e, s):
        src = wrap(at - (1 - 2 * e) * s)
        to = {axis: wrap(at + 1 - 2 * e)}
        return remote(buf.at[src], buf.at[src], ss.at[e, s], rs.at[e, s], to)

    def round_step(ring, s):
        buf, at, axis, ss, rs = ring
        for e in range(2):
            if 1 <= s <= half - e:
                landed(buf.at[wrap(at - (1 - 2 * e) * s)], rs.at[e, s - 1])
            if s < half - e:
                round_copy(*ring, e, s).start()

    y_ring, z_ring = (ybuf, y, ROW, ys, yr), (low, x, COL, zs, zr)

    def total_of(ref):
        total = ref[0]
        for k in range(1, n):
            total = total + ref[k]
        return total

    def low_step(k):
        if k <= half:
            x_step(k)
        if k == half:
            ybuf[y] = part[x]
        if half <= k <= 2 * half:
            round_step(y_ring, k - half)
        if k == 2 * half:
            low[x] = total_of(ybuf).astype(BF16)
        if 2 * half <= k:
            round_step(z_ring, k - 2 * half)

    def low_of(b):
        each = n // 2
        both = low[pl.ds(b * each, each)].reshape(BLOCK, 2 * rank)
        return both[:, :rank], both[:, rank:]

    def g_copy(k):
        src, dst = ((usend, urecv), (dsend, drecv))[k]
        return remote(src, dst, gx_s.at[k], gx_r.at[k], mate)

    def grads_start():
        ups, downs = [], []
        for b in range(2):
            into, back = low_of(b)
            ups.append(SCALE * dot(into, masked[rows(b)], TN))
            downs.append(SCALE * dot(back, g[b, me], TN))
        for q in range(owned):
            theirs, mine = (1 - d) * owned + q, d * owned + q
            usend[q] = weight_of(0, theirs) * ups[0] + weight_of(1, theirs) * ups[1]
            dsend[q] = weight_of(0, theirs) * downs[0] + weight_of(1, theirs) * downs[1]
            ugrad[q] = weight_of(0, mine) * ups[0] + weight_of(1, mine) * ups[1]
            dgrad[q] = weight_of(0, mine) * downs[0] + weight_of(1, mine) * downs[1]

    def terms_step():
        for b in range(2):
            into, back = low_of(b)
            turned = jnp.transpose(into.astype(F32)).astype(BF16)
            acc[:, b * BLOCK : (b + 1) * BLOCK] += SCALE * dot(cout[b], turned, TN)
            adt[b] = SCALE * dot(back, cin[b], NN)

    def grads_done():
        for k in range(2):
            g_copy(k).wait_recv()
        for q in range(owned):
            ugrad[q] = ugrad[q] + urecv[q]
            dgrad[q] = dgrad[q] + drecv[q]
        give(2).start()
        give(3).start()

    def back_chunk(k):
        t = lax.rem(d * own_chunks + k, chunks)
        out = dot(masked[...], w_chunk(t), NN)
        for b in range(2):
            put(p, (b, t), out[b * BLOCK : (b + 1) * BLOCK])

    def front_chunk(t):
        rows_in = jnp.concatenate([g[0, t], g[1, t]], axis=0)
        acc[...] += dot(w_chunk(t), rows_in, NT)

    def hidden_step():
        for b in range(2):
            cols = acc[:, b * BLOCK : (b + 1) * BLOCK]
            hidden[:, b * BLOCK : (b + 1) * BLOCK] = (cols * live(b, cols.shape, 1)).astype(BF16)
        give(0).start()

    def some(body, first, last):
        lax.fori_loop(first, last, lambda k, z: (body(k), z)[1], 0)

    rs_from = n
    last = rs_from + ticks - 1
    back_from, back_ticks = early, rs_from - early
    back_each = -(-chunks // back_ticks)
    front_from, front_ticks = ticks, half + 1
    front_each = -(-chunks // front_ticks)

    def every_tick(tick, carry):
        @pl.when(tick < ticks)
        def _():
            ag_tick(tick)

        @pl.when(tick >= rs_from)
        def _():
            rs_tick(tick - rs_from)

        @pl.when(tick == early - 1)
        def _():
            @pl.when(d == 1)
            def _():
                pl.semaphore_wait(here, 1)

            for k in range(2):
                ad_remote(k).start()
            for q in range(pieces):
                w_remote(q).start()
            for k in range(3):
                take(k).wait()
            mask_step()
            acc[...] = jnp.zeros_like(acc)

        @pl.when(tick == low_from)
        def _():
            low_rank_start()
            for q in range(pieces):
                w_local(q).wait()

        for k in range(3 * half + 1):

            @pl.when(tick == low_from + k)
            def _(k=k):
                low_step(k)

        @pl.when(tick == middle)
        def _():
            for q in range(pieces):
                landed(w_piece(1 - d, q), wx_r.at[q])

        @pl.when(tick == low_to)
        def _():
            grads_start()
            for k in range(2):
                g_copy(k).start()
            terms_step()

        @pl.when(tick == low_to + 1)
        def _():
            grads_done()

        @pl.when(jnp.logical_and(tick >= back_from, tick < back_from + back_ticks))
        def _():
            first = (tick - back_from) * back_each
            some(back_chunk, first, jnp.minimum(first + back_each, chunks))

        @pl.when(jnp.logical_and(tick >= front_from, tick < front_from + front_ticks))
        def _():
            first = (tick - front_from) * front_each
            some(front_chunk, first, jnp.minimum(first + front_each, chunks))

        @pl.when(tick == front_from + front_ticks)
        def _():
            hidden_step()

        return carry

    lax.fori_loop(0, last + 1, every_tick, 0)

    give(1).start()

    for k in range(2):
        ad_remote(k).wait_send()
        g_copy(k).wait_send()
    for q in range(pieces):
        w_remote(q).wait_send()
    for e in range(2):
        for s in range(half - e):
            x_copy(e, s).wait_send()
            round_copy(*y_ring, e, s).wait_send()
            round_copy(*z_ring, e, s).wait_send()

    def sent(src, sem):
        pltpu.make_async_copy(src, src, sem).wait()

    def drain(j, carry):
        @pl.when(j >= 1)
        def _():
            for c in range(2):
                sent(g.at[c, 0], ag1_s.at[c, j])

        @pl.when(j < n - 1)
        def _():
            for c in range(2):
                sent(p.at[c, 0], rs2_s.at[c, j])

        for c in range(2):
            for e in range(2):
                for s in range(half - 1):
                    sent(g.at[c, 0], ag2_s.at[c, e, j, s])
                    sent(p.at[c, 0], rs1_s.at[c, e, j, s])

                @pl.when(is_long(e, j))
                def _(c=c, e=e):
                    sent(g.at[c, 0], ag2_s.at[c, e, j, half - 1])
                    sent(p.at[c, 0], rs1_s.at[c, e, j, half - 1])

        return carry

    lax.fori_loop(0, n, drain, 0)
    for k in range(4):
        give(k).wait()


def hand_over(*refs):
    for src, dst in zip(refs[:4], refs[4:]):
        dst[...] = src[...]


def local(n, tokens, weight, adapter_in, adapter_out, cotangent, member_blocks, block_live):
    token_rows, width = tokens.shape
    hidden_width = weight.shape[1]
    blocks = token_rows // BLOCK
    owned, _, rank = adapter_in.shape
    members = 2 * owned
    half = n // 2
    tall = token_rows // n
    chunks = n * n
    vmem, anywhere = (pl.BlockSpec(memory_space=s) for s in (pltpu.VMEM, pl.ANY))
    pieces = 4
    coded = BLOCK * width // (2 * LANES) + 1
    dma = lambda *shape: pltpu.SemaphoreType.DMA(shape)
    both_ways = (2, 2, n, half)
    out = pl.pallas_call(
        functools.partial(kernel, n),
        out_shape=(
            jax.ShapeDtypeStruct((hidden_width, token_rows), BF16),
            jax.ShapeDtypeStruct((blocks, BLOCK, width), BF16),
            jax.ShapeDtypeStruct((owned, rank, width), F32),
            jax.ShapeDtypeStruct((owned, rank, hidden_width), F32),
        ),
        in_specs=[anywhere] * 7,
        out_specs=(anywhere,) * 4,
        scratch_shapes=[
            pltpu.SMEM(member_blocks.shape, jnp.int32),
            pltpu.SMEM(block_live.shape, jnp.int32),
            pltpu.VMEM((hidden_width, token_rows), BF16),
            pltpu.VMEM((hidden_width, token_rows), BF16),
            pltpu.VMEM((blocks, BLOCK, width), BF16),
            pltpu.VMEM((owned, rank, width), F32),
            pltpu.VMEM((owned, rank, hidden_width), F32),
            pltpu.VMEM((blocks, chunks, BLOCK, width), BF16),
            pltpu.VMEM((hidden_width, chunks * width), BF16),
            pltpu.VMEM((blocks, chunks, coded, LANES), jnp.int32),
            pltpu.VMEM((*both_ways, coded, LANES), jnp.int32),
            pltpu.VMEM((2, n - 1, coded, LANES), jnp.int32),
            pltpu.VMEM((token_rows, hidden_width), BF16),
            pltpu.VMEM((hidden_width, token_rows), F32),
            pltpu.VMEM((blocks, BLOCK, width), F32),
            pltpu.VMEM((members, rank, width), BF16),
            pltpu.VMEM((members, rank, hidden_width), BF16),
            pltpu.VMEM((blocks, rank, width), BF16),
            pltpu.VMEM((blocks, rank, hidden_width), BF16),
            pltpu.VMEM((n, tall, 2 * rank), F32),
            pltpu.VMEM((2, half, tall, 2 * rank), F32),
            pltpu.VMEM((n, tall, 2 * rank), F32),
            pltpu.VMEM((n, tall, 2 * rank), BF16),
            pltpu.VMEM((owned, rank, hidden_width), F32),
            pltpu.VMEM((owned, rank, width), F32),
            pltpu.VMEM((owned, rank, hidden_width), F32),
            pltpu.VMEM((owned, rank, width), F32),
            dma(2, n),
            dma(2, n),
            dma(*both_ways),
            dma(*both_ways),
            dma(*both_ways),
            dma(*both_ways),
            dma(2, n),
            dma(2, n),
            dma(2),
            dma(pieces),
            dma(pieces),
            dma(pieces),
            dma(2),
            dma(2),
            dma(2),
            dma(2, half),
            dma(2, half),
            dma(2, half),
            dma(2, half),
            dma(2, half),
            dma(2, half),
            dma(2),
            dma(2),
            dma(3),
            dma(4),
            pltpu.SemaphoreType.REGULAR,
        ],
        compiler_params=pltpu.CompilerParams(
            collective_id=0, has_side_effects=True, vmem_limit_bytes=62 * 2**20
        ),
        name="step",
    )(
        member_blocks,
        block_live,
        tokens.reshape(blocks, BLOCK, width),
        weight.T,
        jnp.swapaxes(adapter_in, 1, 2),
        adapter_out,
        cotangent.T,
    )
    out = pl.pallas_call(
        hand_over,
        out_shape=tuple(jax.ShapeDtypeStruct(o.shape, o.dtype) for o in out),
        in_specs=[vmem] * 4,
        out_specs=(vmem,) * 4,
        name="hand_over",
    )(*out)
    return (
        out[0].T,
        out[1].reshape(token_rows, width),
        jnp.swapaxes(out[2], 1, 2),
        out[3],
    )


def solution(mesh):
    n = math.isqrt(mesh.shape["tensor"])
    tensor = (ROW, COL)
    finer = Mesh(
        mesh.devices.reshape(mesh.shape["pop"], mesh.shape["dp"], n, n), ("pop", CORE, ROW, COL)
    )
    return jax.shard_map(
        functools.partial(local, n),
        mesh=finer,
        in_specs=(
            P(("pop", "dp"), tensor),
            P("dp", tensor),
            P(("pop", "dp"), tensor, None),
            P(("pop", "dp"), None, tensor),
            P(("pop", "dp"), tensor),
            P("pop"),
            P(("pop", "dp")),
        ),
        out_specs=(
            P(("pop", "dp"), tensor),
            P(("pop", "dp"), tensor),
            P(("pop", "dp"), tensor, None),
            P(("pop", "dp"), None, tensor),
        ),
        check_vma=False,
    )
```

```python
import functools
import math

import jax
import jax.numpy as jnp
from jax import lax
from jax.experimental import pallas as pl
from jax.experimental.pallas import tpu as pltpu
from jax.sharding import Mesh
from jax.sharding import PartitionSpec as P

BLOCK = 128
SCALE = 0.5
MESH = pl.DeviceIdType.MESH
ROW, COL, CORE = "tensor_0", "tensor_1", "dp"
F32, BF16 = jnp.float32, jnp.bfloat16

NN = (((1,), (0,)), ((), ()))
NT = (((1,), (1,)), ((), ()))
TN = (((0,), (0,)), ((), ()))


def dot(a, b, dims):
    return lax.dot_general(a, b, dims, preferred_element_type=F32)


LANES = 128
UNIT = 2.0**21
TOP = 32760.0


def halves(v):
    return [v[:, k : k + LANES] for k in range(0, v.shape[1], LANES)]


def put(ref, at, v):
    parts = halves(v)
    largest = jnp.max(functools.reduce(jnp.maximum, [jnp.abs(q) for q in parts]), axis=0, keepdims=True)
    scale = (largest * UNIT).astype(jnp.int32) + 1
    by = (TOP * UNIT) / scale.astype(F32)
    mid = v.shape[0] // 2
    for k, q in enumerate(parts):
        code = (q * by).astype(jnp.int32)
        ref[(*at, slice(k * mid, (k + 1) * mid))] = (code[:mid] << 16) | (code[mid:] & 0xFFFF)
    ref[(*at, slice(2 * mid, 2 * mid + 1))] = scale


def get(ref, at):
    mid = (ref.shape[-2] - 1) // 2
    scale = ref[(*at, slice(2 * mid, 2 * mid + 1))].astype(F32) * (1.0 / (TOP * UNIT))
    out = []
    for k in range(2):
        pair = ref[(*at, slice(k * mid, (k + 1) * mid))]
        both = jnp.concatenate([pair >> 16, (pair << 16) >> 16], axis=0)
        out.append(both.astype(F32) * scale)
    return jnp.concatenate(out, axis=1)


def kernel(
    n,
    mb_hbm,
    bl_hbm,
    tok_hbm,
    w_hbm,
    ain_hbm,
    aout_hbm,
    cot_hbm,
    hidden_hbm,
    igrad_hbm,
    dgrad_hbm,
    ugrad_hbm,
    mb,
    bl,
    cot,
    hidden,
    igrad,
    dgrad,
    ugrad,
    g,
    w,
    p,
    rb,
    r2,
    masked,
    acc,
    adt,
    ain,
    aout,
    cin,
    cout,
    part,
    xbuf,
    ybuf,
    low,
    usend,
    dsend,
    urecv,
    drecv,
    ag_s,
    rs_s,
    flow_r,
    turn_r,
    own_sem,
    w_sem,
    wx_s,
    wx_r,
    ad_sem,
    adx_s,
    adx_r,
    low_s,
    xz_r,
    y_r,
    gx_s,
    gx_r,
    in_sem,
    out_sem,
    here,
):
    half = n // 2
    ticks = n - 1 + half
    cycle, shift = (5, 3) if n >= 8 else (2 * n, n)
    early, middle = n // 4, n // 2
    low_from = early
    low_to = low_from + 3 * half
    y, x, d = lax.axis_index(ROW), lax.axis_index(COL), lax.axis_index(CORE)
    mate = {CORE: 1 - d}
    me = y * n + x
    chunks = n * n
    members = ain.shape[0]
    owned = members // 2
    width = g.shape[3]
    own_depth = w_hbm.shape[1]
    own_chunks = own_depth // width
    rank = ain.shape[1]
    minor_axis, major_axis = (COL, ROW), (ROW, COL)
    minor_at, major_at = (x, y), (y, x)

    def chunk(c, major, minor):
        return major * n + minor if c == 0 else minor * n + major

    def wrap(v):
        return lax.rem(v + 2 * n, n)

    def remote(src, dst, ss, rs, to):
        return pltpu.make_async_remote_copy(
            src_ref=src, dst_ref=dst, send_sem=ss, recv_sem=rs, device_id=to, device_id_type=MESH
        )

    def landed(dst, sem):
        pltpu.make_async_copy(dst, dst, sem).wait()

    barrier = pltpu.get_barrier_semaphore()
    for step in (1, n - 1):
        pl.semaphore_signal(barrier, inc=1, device_id={COL: wrap(x + step)}, device_id_type=MESH)
        pl.semaphore_signal(barrier, inc=1, device_id={ROW: wrap(y + step)}, device_id_type=MESH)

    @pl.when(d == 1)
    def _():
        pl.semaphore_signal(barrier, inc=1, device_id=mate, device_id_type=MESH)

    own = pltpu.make_async_copy(tok_hbm, g.at[:, me], own_sem)
    own.start()
    taken = ((mb_hbm, mb), (bl_hbm, bl), (cot_hbm, cot))
    given = ((hidden, hidden_hbm), (igrad, igrad_hbm), (dgrad, dgrad_hbm), (ugrad, ugrad_hbm))

    def take(k):
        return pltpu.make_async_copy(*taken[k], in_sem.at[k])

    def give(k):
        return pltpu.make_async_copy(*given[k], out_sem.at[k])

    for k in range(3):
        take(k).start()

    def ad_local(k):
        hbm, vm = ((ain_hbm, ain), (aout_hbm, aout))[k]
        return pltpu.make_async_copy(hbm, vm.at[pl.ds(d * owned, owned)], ad_sem.at[k])

    def ad_remote(k):
        hbm, vm = ((ain_hbm, ain), (aout_hbm, aout))[k]
        return remote(hbm, vm.at[pl.ds(d * owned, owned)], adx_s.at[k], adx_r.at[k], mate)

    def w_half(core):
        return w.at[:, pl.ds(pl.multiple_of(core * own_depth, LANES), own_depth)]

    w_local = pltpu.make_async_copy(w_hbm, w_half(d), w_sem)
    w_remote = remote(w_hbm, w_half(d), wx_s, wx_r, mate)

    def w_chunk(t):
        return w[:, pl.ds(pl.multiple_of(t * width, LANES), width)]

    for k in range(2):
        ad_local(k).start()
    w_local.start()
    own.wait()
    pl.semaphore_wait(barrier, 4 + 1 - d)

    @pl.when(d == 0)
    def _():
        pl.semaphore_signal(here, inc=1, device_id=mate, device_id_type=MESH)


    def minor_offset(j):
        back = lax.div(j + 1, 2)
        return jnp.where(lax.rem(j, 2) == 1, -back, lax.div(j, 2))

    def ag1_copy(c, j, right):
        src = chunk(c, major_at[c], wrap(minor_at[c] + minor_offset(j)))
        lands = jnp.where(j == 0, 1 if right else 2, j + 2)
        to = {minor_axis[c]: wrap(minor_at[c] + (1 if right else -1))}
        return remote(g.at[c, src], g.at[c, src], ag_s.at[c], turn_r.at[c, lands], to)

    def ag1_step(j):
        for c in range(2):
            src = chunk(c, major_at[c], wrap(minor_at[c] + minor_offset(j)))

            @pl.when(j >= 1)
            def _(c=c, src=src):
                landed(g.at[c, src], turn_r.at[c, j])

            @pl.when(jnp.logical_or(j == 0, jnp.logical_and(lax.rem(j, 2) == 1, j + 2 < n)))
            def _(c=c):
                ag1_copy(c, j, True).start()

            @pl.when(jnp.logical_and(lax.rem(j, 2) == 0, j + 2 < n))
            def _(c=c):
                ag1_copy(c, j, False).start()

    def ag2_copy(c, e, j, s):
        way = 1 - 2 * e
        t = chunk(c, wrap(major_at[c] - way * s), wrap(minor_at[c] + minor_offset(j)))
        to = {major_axis[c]: wrap(major_at[c] + way)}
        return remote(g.at[c, t], g.at[c, t], ag_s.at[c], flow_r.at[c, e, lax.rem(j, cycle), s], to)

    def ag2_landed(c, e, j, s):
        t = chunk(c, wrap(major_at[c] - (1 - 2 * e) * s), wrap(minor_at[c] + minor_offset(j)))
        landed(g.at[c, t], flow_r.at[c, e, lax.rem(j, cycle), s - 1])

    def is_long(e, j):
        return lax.rem(j, 2) == e

    def streams(at, first, body):
        j = at + jnp.where(at > first, 1, 0)

        @pl.when(jnp.logical_and(at >= 0, at < n - 1))
        def _():
            lax.fori_loop(j, j + 1 + jnp.where(at == first, 1, 0), lambda k, z: (body(k), z)[1], 0)

    def ag_tick(tick):
        streams(tick, 1, ag1_step)
        for s in range(half + 1):

            def hop(j, s=s):
                for c in range(2):
                    for e in range(2):
                        if s < half:
                            if s > 0:
                                ag2_landed(c, e, j, s)
                            if s < half - 1:
                                ag2_copy(c, e, j, s).start()
                            else:

                                @pl.when(is_long(e, j))
                                def _(c=c, e=e):
                                    ag2_copy(c, e, j, s).start()
                        else:

                            @pl.when(is_long(e, j))
                            def _(c=c, e=e):
                                ag2_landed(c, e, j, s)

            streams(tick - s, 1, hop)

    def dest_offset(i):
        ahead = lax.div(n - i, 2)
        back = lax.div(n - 1 - i, 2)
        return jnp.where(lax.rem(i, 2) == 0, ahead, -back)

    def hops(e, i):
        return jnp.where(is_long(e, i), half, half - 1)

    def rs1_chunk(c, e, i, s):
        far = (1 - 2 * e) * (hops(e, i) - s)
        return chunk(c, wrap(major_at[c] + far), wrap(minor_at[c] + dest_offset(i)))

    def rs1_sem(c, e, i, s):
        return flow_r.at[c, e, lax.rem(i + shift, cycle), s]

    def rs1_landed(c, e, i, s):
        landed(rb.at[c, e, i, s], rs1_sem(c, e, i, s))

    def rs1_copy(c, e, i, s):
        t = rs1_chunk(c, e, i, s)
        to = {major_axis[c]: wrap(major_at[c] + 1 - 2 * e)}
        return remote(p.at[c, t], rb.at[c, e, i, s], rs_s.at[c], rs1_sem(c, e, i, s), to)

    def rs1_add_send(c, e, i, s):
        t = rs1_chunk(c, e, i, s)
        put(p, (c, t), get(p, (c, t)) + get(rb, (c, e, i, s - 1)))
        rs1_copy(c, e, i, s).start()

    def rs2_copy(c, i, right):
        t = chunk(c, major_at[c], wrap(minor_at[c] + dest_offset(i)))
        to = {minor_axis[c]: wrap(minor_at[c] + (1 if right else -1))}
        return remote(p.at[c, t], r2.at[c, i], rs_s.at[c], turn_r.at[c, i], to)

    def rs1_done(c, i):
        t = chunk(c, major_at[c], wrap(minor_at[c] + dest_offset(i)))
        total = get(p, (c, t))
        for e in range(2):
            total = total + get(rb, (c, e, i, hops(e, i) - 1))
        return t, total

    def rs2_step(i):
        for c in range(2):

            @pl.when(i < 2)
            def _(c=c):
                t, total = rs1_done(c, i)
                put(p, (c, t), total)

            @pl.when(jnp.logical_and(i >= 2, i < n - 1))
            def _(c=c):
                landed(r2.at[c, i - 2], turn_r.at[c, i - 2])
                t, total = rs1_done(c, i)
                put(p, (c, t), total + get(r2, (c, i - 2)))

            @pl.when(jnp.logical_and(i < n - 1, lax.rem(i, 2) == 0))
            def _(c=c):
                rs2_copy(c, i, True).start()

            @pl.when(jnp.logical_and(i < n - 1, lax.rem(i, 2) == 1))
            def _(c=c):
                rs2_copy(c, i, False).start()

            @pl.when(i == n - 1)
            def _(c=c):
                t, total = rs1_done(c, i)
                total = total + adt[c]
                for k in (n - 3, n - 2):
                    landed(r2.at[c, k], turn_r.at[c, k])
                    total = total + get(r2, (c, k))
                igrad[c] = total.astype(BF16)

    def rs_tick(tick):
        for s in range(half + 1):

            def hop(i, s=s):
                for c in range(2):
                    for e in range(2):
                        if s == 0:
                            rs1_copy(c, e, i, s).start()
                        elif s < half - 1:
                            rs1_landed(c, e, i, s - 1)
                            rs1_add_send(c, e, i, s)
                        elif s == half - 1:
                            rs1_landed(c, e, i, s - 1)

                            @pl.when(is_long(e, i))
                            def _(c=c, e=e):
                                rs1_add_send(c, e, i, s)
                        else:

                            @pl.when(is_long(e, i))
                            def _(c=c, e=e):
                                rs1_landed(c, e, i, s - 1)

                if s == half:
                    rs2_step(i)

            streams(tick - s, n - 3, hop)

    def member_of(b):
        end, count = jnp.int32(0), jnp.int32(0)
        for m in range(members):
            end = end + mb[m]
            count = count + jnp.where(end <= d * 2 + b, 1, 0)
        return count

    def weight_of(b, m):
        return jnp.where(member_of(b) == m, F32(1.0), F32(0.0))

    def live(b, shape, dim):
        at = lax.broadcasted_iota(jnp.int32, shape, dim)
        return jnp.where(at < bl[b], F32(1.0), F32(0.0))

    def rows(b):
        return pl.ds(b * BLOCK, BLOCK)

    def mask_step():
        for b in range(2):
            across = jnp.transpose(cot[:, b * BLOCK : (b + 1) * BLOCK].astype(F32))
            masked[rows(b)] = (across * live(b, across.shape, 0)).astype(BF16)

    def low_rank_start():
        for k in range(2):
            ad_local(k).wait()
            ad_remote(k).wait_recv()
        for b in range(2):
            a, o = weight_of(b, 0) * ain[0].astype(F32), weight_of(b, 0) * aout[0].astype(F32)
            for m in range(1, members):
                a = a + weight_of(b, m) * ain[m].astype(F32)
                o = o + weight_of(b, m) * aout[m].astype(F32)
            cin[b], cout[b] = a.astype(BF16), o.astype(BF16)
        tall = part.shape[1]
        for b in range(2):
            into = dot(g[b, me], cin[b], NT)
            back = dot(masked[rows(b)], cout[b], NT)
            both = jnp.concatenate([into, back], axis=1)
            each = BLOCK // tall
            part[pl.ds(b * each, each)] = both.reshape(each, tall, 2 * rank)

    def x_copy(e, s):
        way = 1 - 2 * e
        piece = wrap(x + way * (half - e - s))
        to = {COL: wrap(x + way)}
        return remote(part.at[piece], xbuf.at[e, s], low_s.at[0], xz_r.at[e, s], to)

    def x_step(s):
        for e in range(2):
            if 1 <= s <= half - e:
                piece = wrap(x + (1 - 2 * e) * (half - e - s))
                landed(xbuf.at[e, s - 1], xz_r.at[e, s - 1])
                part[piece] = part[piece] + xbuf[e, s - 1]
            if s < half - e:
                x_copy(e, s).start()

    def round_copy(buf, at, axis, ss, rs, e, s):
        src = wrap(at - (1 - 2 * e) * s)
        to = {axis: wrap(at + 1 - 2 * e)}
        return remote(buf.at[src], buf.at[src], ss, rs.at[e, s], to)

    def round_step(ring, s):
        buf, at, axis, ss, rs = ring
        for e in range(2):
            if 1 <= s <= half - e:
                landed(buf.at[wrap(at - (1 - 2 * e) * s)], rs.at[e, s - 1])
            if s < half - e:
                round_copy(*ring, e, s).start()

    y_ring, z_ring = (ybuf, y, ROW, low_s.at[1], y_r), (low, x, COL, low_s.at[2], xz_r)

    def total_of(ref):
        total = ref[0]
        for k in range(1, n):
            total = total + ref[k]
        return total

    def low_step(k):
        if k <= half:
            x_step(k)
        if k == half:
            ybuf[y] = part[x]
        if half <= k <= 2 * half:
            round_step(y_ring, k - half)
        if k == 2 * half:
            low[x] = total_of(ybuf).astype(BF16)
        if 2 * half <= k:
            round_step(z_ring, k - 2 * half)

    def low_of(b):
        each = n // 2
        both = low[pl.ds(b * each, each)].reshape(BLOCK, 2 * rank)
        return both[:, :rank], both[:, rank:]

    def g_copy(k):
        src, dst = ((usend, urecv), (dsend, drecv))[k]
        return remote(src, dst, gx_s.at[k], gx_r.at[k], mate)

    def grads_start():
        ups, downs = [], []
        for b in range(2):
            into, back = low_of(b)
            ups.append(SCALE * dot(into, masked[rows(b)], TN))
            downs.append(SCALE * dot(back, g[b, me], TN))
        for q in range(owned):
            theirs, mine = (1 - d) * owned + q, d * owned + q
            usend[q] = weight_of(0, theirs) * ups[0] + weight_of(1, theirs) * ups[1]
            dsend[q] = weight_of(0, theirs) * downs[0] + weight_of(1, theirs) * downs[1]
            ugrad[q] = weight_of(0, mine) * ups[0] + weight_of(1, mine) * ups[1]
            dgrad[q] = weight_of(0, mine) * downs[0] + weight_of(1, mine) * downs[1]

    def terms_step():
        for b in range(2):
            into, back = low_of(b)
            turned = jnp.transpose(into.astype(F32)).astype(BF16)
            acc[:, b * BLOCK : (b + 1) * BLOCK] += SCALE * dot(cout[b], turned, TN)
            adt[b] = SCALE * dot(back, cin[b], NN)

    def grads_done():
        for k in range(2):
            g_copy(k).wait_recv()
        for q in range(owned):
            ugrad[q] = ugrad[q] + urecv[q]
            dgrad[q] = dgrad[q] + drecv[q]
        give(2).start()
        give(3).start()

    def back_chunk(k):
        t = lax.rem(d * own_chunks + k, chunks)
        out = dot(masked[...], w_chunk(t), NN)
        for b in range(2):
            put(p, (b, t), out[b * BLOCK : (b + 1) * BLOCK])

    def front_chunk(t):
        rows_in = jnp.concatenate([g[0, t], g[1, t]], axis=0)
        acc[...] += dot(w_chunk(t), rows_in, NT)

    def hidden_step():
        for b in range(2):
            cols = acc[:, b * BLOCK : (b + 1) * BLOCK]
            hidden[:, b * BLOCK : (b + 1) * BLOCK] = (cols * live(b, cols.shape, 1)).astype(BF16)
        give(0).start()

    def some(body, first, last):
        lax.fori_loop(first, last, lambda k, z: (body(k), z)[1], 0)

    rs_from = n - 1 if n >= 8 else n + 1
    last = max(rs_from + ticks - 1, low_to + 2)
    back_from, back_ticks = early, rs_from - early
    back_each = -(-chunks // back_ticks)
    front_from, front_ticks = ticks, half + 1
    front_each = -(-chunks // front_ticks)

    def every_tick(tick, carry):
        @pl.when(tick < ticks)
        def _():
            ag_tick(tick)

        @pl.when(tick >= rs_from)
        def _():
            rs_tick(tick - rs_from)

        @pl.when(tick == early - 1)
        def _():
            @pl.when(d == 1)
            def _():
                pl.semaphore_wait(here, 1)

            for k in range(2):
                ad_remote(k).start()
            w_remote.start()
            for k in range(3):
                take(k).wait()
            mask_step()
            acc[...] = jnp.zeros_like(acc)

        @pl.when(tick == low_from)
        def _():
            low_rank_start()
            w_local.wait()

        for k in range(3 * half + 1):

            @pl.when(tick == low_from + k)
            def _(k=k):
                low_step(k)

        @pl.when(tick == middle)
        def _():
            landed(w_half(1 - d), wx_r)

        @pl.when(tick == low_to)
        def _():
            grads_start()
            for k in range(2):
                g_copy(k).start()
            terms_step()

        @pl.when(tick == low_to + 2)
        def _():
            grads_done()

        @pl.when(jnp.logical_and(tick >= back_from, tick < back_from + back_ticks))
        def _():
            first = (tick - back_from) * back_each
            some(back_chunk, first, jnp.minimum(first + back_each, chunks))

        @pl.when(jnp.logical_and(tick >= front_from, tick < front_from + front_ticks))
        def _():
            first = (tick - front_from) * front_each
            some(front_chunk, first, jnp.minimum(first + front_each, chunks))

        @pl.when(tick == front_from + front_ticks)
        def _():
            hidden_step()

        return carry

    lax.fori_loop(0, last + 1, every_tick, 0)

    give(1).start()

    for k in range(2):
        ad_remote(k).wait_send()
        g_copy(k).wait_send()
    w_remote.wait_send()

    def sent(src, sem):
        pltpu.make_async_copy(src, src, sem).wait()

    for k, buf in enumerate((part, ybuf, low)):
        sent(buf.at[pl.ds(0, n - 1)], low_s.at[k])
    for c in range(2):
        sent(g.at[c, pl.ds(0, chunks - 1)], ag_s.at[c])
        sent(p.at[c, pl.ds(0, chunks - 1)], rs_s.at[c])
    for k in range(4):
        give(k).wait()


def hand_over(*refs):
    for src, dst in zip(refs[:4], refs[4:]):
        dst[...] = src[...]


def local(n, tokens, weight, adapter_in, adapter_out, cotangent, member_blocks, block_live):
    token_rows, width = tokens.shape
    hidden_width = weight.shape[1]
    blocks = token_rows // BLOCK
    owned, _, rank = adapter_in.shape
    members = 2 * owned
    half = n // 2
    tall = token_rows // n
    chunks = n * n
    vmem, anywhere = (pl.BlockSpec(memory_space=s) for s in (pltpu.VMEM, pl.ANY))
    coded = BLOCK * width // (2 * LANES) + 1
    dma = lambda *shape: pltpu.SemaphoreType.DMA(shape)
    both_ways = (2, 2, n, half)
    out = pl.pallas_call(
        functools.partial(kernel, n),
        out_shape=(
            jax.ShapeDtypeStruct((hidden_width, token_rows), BF16),
            jax.ShapeDtypeStruct((blocks, BLOCK, width), BF16),
            jax.ShapeDtypeStruct((owned, rank, width), F32),
            jax.ShapeDtypeStruct((owned, rank, hidden_width), F32),
        ),
        in_specs=[anywhere] * 7,
        out_specs=(anywhere,) * 4,
        scratch_shapes=[
            pltpu.SMEM(member_blocks.shape, jnp.int32),
            pltpu.SMEM(block_live.shape, jnp.int32),
            pltpu.VMEM((hidden_width, token_rows), BF16),
            pltpu.VMEM((hidden_width, token_rows), BF16),
            pltpu.VMEM((blocks, BLOCK, width), BF16),
            pltpu.VMEM((owned, rank, width), F32),
            pltpu.VMEM((owned, rank, hidden_width), F32),
            pltpu.VMEM((blocks, chunks, BLOCK, width), BF16),
            pltpu.VMEM((hidden_width, chunks * width), BF16),
            pltpu.VMEM((blocks, chunks, coded, LANES), jnp.int32),
            pltpu.VMEM((*both_ways, coded, LANES), jnp.int32),
            pltpu.VMEM((2, n - 1, coded, LANES), jnp.int32),
            pltpu.VMEM((token_rows, hidden_width), BF16),
            pltpu.VMEM((hidden_width, token_rows), F32),
            pltpu.VMEM((blocks, BLOCK, width), F32),
            pltpu.VMEM((members, rank, width), BF16),
            pltpu.VMEM((members, rank, hidden_width), BF16),
            pltpu.VMEM((blocks, rank, width), BF16),
            pltpu.VMEM((blocks, rank, hidden_width), BF16),
            pltpu.VMEM((n, tall, 2 * rank), F32),
            pltpu.VMEM((2, half, tall, 2 * rank), F32),
            pltpu.VMEM((n, tall, 2 * rank), F32),
            pltpu.VMEM((n, tall, 2 * rank), BF16),
            pltpu.VMEM((owned, rank, hidden_width), F32),
            pltpu.VMEM((owned, rank, width), F32),
            pltpu.VMEM((owned, rank, hidden_width), F32),
            pltpu.VMEM((owned, rank, width), F32),
            dma(2),
            dma(2),
            dma(2, 2, 5 if n >= 8 else 2 * n, half),
            dma(2, n),
            pltpu.SemaphoreType.DMA,
            pltpu.SemaphoreType.DMA,
            pltpu.SemaphoreType.DMA,
            pltpu.SemaphoreType.DMA,
            dma(2),
            dma(2),
            dma(2),
            dma(3),
            dma(2, half),
            dma(2, half),
            dma(2),
            dma(2),
            dma(3),
            dma(4),
            pltpu.SemaphoreType.REGULAR,
        ],
        compiler_params=pltpu.CompilerParams(
            collective_id=0, has_side_effects=True, vmem_limit_bytes=62 * 2**20
        ),
        name="step",
    )(
        member_blocks,
        block_live,
        tokens.reshape(blocks, BLOCK, width),
        weight.T,
        jnp.swapaxes(adapter_in, 1, 2),
        adapter_out,
        cotangent.T,
    )
    out = pl.pallas_call(
        hand_over,
        out_shape=tuple(jax.ShapeDtypeStruct(o.shape, o.dtype) for o in out),
        in_specs=[vmem] * 4,
        out_specs=(vmem,) * 4,
        name="hand_over",
    )(*out)
    return (
        out[0].T,
        out[1].reshape(token_rows, width),
        jnp.swapaxes(out[2], 1, 2),
        out[3],
    )


def solution(mesh):
    n = math.isqrt(mesh.shape["tensor"])
    tensor = (ROW, COL)
    finer = Mesh(
        mesh.devices.reshape(mesh.shape["pop"], mesh.shape["dp"], n, n), ("pop", CORE, ROW, COL)
    )
    return jax.shard_map(
        functools.partial(local, n),
        mesh=finer,
        in_specs=(
            P(("pop", "dp"), tensor),
            P("dp", tensor),
            P(("pop", "dp"), tensor, None),
            P(("pop", "dp"), None, tensor),
            P(("pop", "dp"), tensor),
            P("pop"),
            P(("pop", "dp")),
        ),
        out_specs=(
            P(("pop", "dp"), tensor),
            P(("pop", "dp"), tensor),
            P(("pop", "dp"), tensor, None),
            P(("pop", "dp"), None, tensor),
        ),
        check_vma=False,
    )
```

```python
import functools
import math

import jax
import jax.numpy as jnp
from jax import lax
from jax.experimental import pallas as pl
from jax.experimental.pallas import tpu as pltpu
from jax.sharding import Mesh
from jax.sharding import PartitionSpec as P

BLOCK = 128
SCALE = 0.5
MESH = pl.DeviceIdType.MESH
ROW, COL, CORE = "tensor_0", "tensor_1", "dp"
F32, BF16 = jnp.float32, jnp.bfloat16

NN = (((1,), (0,)), ((), ()))
NT = (((1,), (1,)), ((), ()))
TN = (((0,), (0,)), ((), ()))


def dot(a, b, dims):
    return lax.dot_general(a, b, dims, preferred_element_type=F32)


LANES = 128
UNIT = 2.0**21
TOP = 32760.0


def halves(v):
    return [v[:, k : k + LANES] for k in range(0, v.shape[1], LANES)]


def put(ref, at, v):
    parts = halves(v)
    largest = jnp.max(functools.reduce(jnp.maximum, [jnp.abs(q) for q in parts]), axis=0, keepdims=True)
    scale = (largest * UNIT).astype(jnp.int32) + 1
    by = (TOP * UNIT) / scale.astype(F32)
    mid = v.shape[0] // 2
    for k, q in enumerate(parts):
        code = (q * by).astype(jnp.int32)
        ref[(*at, slice(k * mid, (k + 1) * mid))] = (code[:mid] << 16) | (code[mid:] & 0xFFFF)
    ref[(*at, slice(2 * mid, 2 * mid + 1))] = scale


def get(ref, at):
    mid = (ref.shape[-2] - 1) // 2
    scale = ref[(*at, slice(2 * mid, 2 * mid + 1))].astype(F32) * (1.0 / (TOP * UNIT))
    out = []
    for k in range(2):
        pair = ref[(*at, slice(k * mid, (k + 1) * mid))]
        both = jnp.concatenate([pair >> 16, (pair << 16) >> 16], axis=0)
        out.append(both.astype(F32) * scale)
    return jnp.concatenate(out, axis=1)


def kernel(
    n,
    mb_hbm,
    bl_hbm,
    tok_hbm,
    w_hbm,
    ain_hbm,
    aout_hbm,
    cot_hbm,
    hidden,
    igrad,
    dgrad,
    ugrad,
    mb,
    bl,
    cot,
    g,
    w,
    p,
    rb,
    r2,
    masked,
    acc,
    adt,
    ain,
    aout,
    cin,
    cout,
    part,
    xbuf,
    ybuf,
    low,
    usend,
    dsend,
    urecv,
    drecv,
    ag_s,
    rs_s,
    flow_r,
    turn_r,
    own_sem,
    w_sem,
    wx_s,
    wx_r,
    ad_sem,
    adx_s,
    adx_r,
    low_s,
    xz_r,
    y_r,
    gx_s,
    gx_r,
    in_sem,
    here,
):
    half = n // 2
    ticks = n - 1 + half
    cycle, shift = (5, 3) if n >= 8 else (2 * n, n)
    early, middle = n // 4, n // 2
    low_from = early
    low_to = low_from + 3 * half
    y, x, d = lax.axis_index(ROW), lax.axis_index(COL), lax.axis_index(CORE)
    mate = {CORE: 1 - d}
    me = y * n + x
    chunks = n * n
    group = 4
    members = ain.shape[0]
    owned = members // 2
    width = g.shape[3]
    own_depth = w_hbm.shape[1]
    own_chunks = own_depth // width
    rank = ain.shape[1]
    minor_axis, major_axis = (COL, ROW), (ROW, COL)
    minor_at, major_at = (x, y), (y, x)

    def chunk(c, major, minor):
        return major * n + minor if c == 0 else minor * n + major

    def wrap(v):
        return lax.rem(v + 2 * n, n)

    def remote(src, dst, ss, rs, to):
        return pltpu.make_async_remote_copy(
            src_ref=src, dst_ref=dst, send_sem=ss, recv_sem=rs, device_id=to, device_id_type=MESH
        )

    def landed(dst, sem):
        pltpu.make_async_copy(dst, dst, sem).wait()

    barrier = pltpu.get_barrier_semaphore()
    for step in (1, n - 1):
        pl.semaphore_signal(barrier, inc=1, device_id={COL: wrap(x + step)}, device_id_type=MESH)
        pl.semaphore_signal(barrier, inc=1, device_id={ROW: wrap(y + step)}, device_id_type=MESH)

    @pl.when(d == 1)
    def _():
        pl.semaphore_signal(barrier, inc=1, device_id=mate, device_id_type=MESH)

    own = pltpu.make_async_copy(tok_hbm, g.at[:, me], own_sem)
    own.start()
    taken = ((mb_hbm, mb), (bl_hbm, bl), (cot_hbm, cot))

    def take(k):
        return pltpu.make_async_copy(*taken[k], in_sem.at[k])

    for k in range(3):
        take(k).start()

    def ad_local(k):
        hbm, vm = ((ain_hbm, ain), (aout_hbm, aout))[k]
        return pltpu.make_async_copy(hbm, vm.at[pl.ds(d * owned, owned)], ad_sem.at[k])

    def ad_remote(k):
        hbm, vm = ((ain_hbm, ain), (aout_hbm, aout))[k]
        return remote(hbm, vm.at[pl.ds(d * owned, owned)], adx_s.at[k], adx_r.at[k], mate)

    def w_half(core):
        return w.at[:, pl.ds(pl.multiple_of(core * own_depth, LANES), own_depth)]

    w_local = pltpu.make_async_copy(w_hbm, w_half(d), w_sem)
    w_remote = remote(w_hbm, w_half(d), wx_s, wx_r, mate)

    def w_chunk(t):
        return w[:, pl.ds(pl.multiple_of(t * width, LANES), width)]

    for k in range(2):
        ad_local(k).start()
    w_local.start()
    own.wait()
    pl.semaphore_wait(barrier, 4 + 1 - d)

    @pl.when(d == 0)
    def _():
        pl.semaphore_signal(here, inc=1, device_id=mate, device_id_type=MESH)


    def minor_offset(j):
        back = lax.div(j + 1, 2)
        return jnp.where(lax.rem(j, 2) == 1, -back, lax.div(j, 2))

    def ag1_copy(c, j, right):
        src = chunk(c, major_at[c], wrap(minor_at[c] + minor_offset(j)))
        lands = jnp.where(j == 0, 1 if right else 2, j + 2)
        to = {minor_axis[c]: wrap(minor_at[c] + (1 if right else -1))}
        return remote(g.at[c, src], g.at[c, src], ag_s.at[c], turn_r.at[c, lands], to)

    def ag1_step(j):
        for c in range(2):
            src = chunk(c, major_at[c], wrap(minor_at[c] + minor_offset(j)))

            @pl.when(j >= 1)
            def _(c=c, src=src):
                landed(g.at[c, src], turn_r.at[c, j])

            @pl.when(jnp.logical_or(j == 0, jnp.logical_and(lax.rem(j, 2) == 1, j + 2 < n)))
            def _(c=c):
                ag1_copy(c, j, True).start()

            @pl.when(jnp.logical_and(lax.rem(j, 2) == 0, j + 2 < n))
            def _(c=c):
                ag1_copy(c, j, False).start()

    def ag2_copy(c, e, j, s):
        way = 1 - 2 * e
        t = chunk(c, wrap(major_at[c] - way * s), wrap(minor_at[c] + minor_offset(j)))
        to = {major_axis[c]: wrap(major_at[c] + way)}
        return remote(g.at[c, t], g.at[c, t], ag_s.at[c], flow_r.at[c, e, lax.rem(j, cycle), s], to)

    def ag2_landed(c, e, j, s):
        t = chunk(c, wrap(major_at[c] - (1 - 2 * e) * s), wrap(minor_at[c] + minor_offset(j)))
        landed(g.at[c, t], flow_r.at[c, e, lax.rem(j, cycle), s - 1])

    def is_long(e, j):
        return lax.rem(j, 2) == e

    def streams(at, first, body):
        j = at + jnp.where(at > first, 1, 0)

        @pl.when(jnp.logical_and(at >= 0, at < n - 1))
        def _():
            lax.fori_loop(j, j + 1 + jnp.where(at == first, 1, 0), lambda k, z: (body(k), z)[1], 0)

    def ag_tick(tick):
        streams(tick, 1, ag1_step)
        for s in range(half + 1):

            def hop(j, s=s):
                for c in range(2):
                    for e in range(2):
                        if s < half:
                            if s > 0:
                                ag2_landed(c, e, j, s)
                            if s < half - 1:
                                ag2_copy(c, e, j, s).start()
                            else:

                                @pl.when(is_long(e, j))
                                def _(c=c, e=e):
                                    ag2_copy(c, e, j, s).start()
                        else:

                            @pl.when(is_long(e, j))
                            def _(c=c, e=e):
                                ag2_landed(c, e, j, s)

            streams(tick - s, 1, hop)

    def dest_offset(i):
        ahead = lax.div(n - i, 2)
        back = lax.div(n - 1 - i, 2)
        return jnp.where(lax.rem(i, 2) == 0, ahead, -back)

    def hops(e, i):
        return jnp.where(is_long(e, i), half, half - 1)

    def rs1_chunk(c, e, i, s):
        far = (1 - 2 * e) * (hops(e, i) - s)
        return chunk(c, wrap(major_at[c] + far), wrap(minor_at[c] + dest_offset(i)))

    def rs1_sem(c, e, i, s):
        return flow_r.at[c, e, lax.rem(i + shift, cycle), s]

    def rs1_landed(c, e, i, s):
        landed(rb.at[c, e, i, s], rs1_sem(c, e, i, s))

    def rs1_copy(c, e, i, s):
        t = rs1_chunk(c, e, i, s)
        to = {major_axis[c]: wrap(major_at[c] + 1 - 2 * e)}
        return remote(p.at[c, t], rb.at[c, e, i, s], rs_s.at[c], rs1_sem(c, e, i, s), to)

    def rs1_add_send(c, e, i, s):
        t = rs1_chunk(c, e, i, s)
        put(p, (c, t), get(p, (c, t)) + get(rb, (c, e, i, s - 1)))
        rs1_copy(c, e, i, s).start()

    def rs2_copy(c, i, right):
        t = chunk(c, major_at[c], wrap(minor_at[c] + dest_offset(i)))
        to = {minor_axis[c]: wrap(minor_at[c] + (1 if right else -1))}
        return remote(p.at[c, t], r2.at[c, i], rs_s.at[c], turn_r.at[c, i], to)

    def rs1_done(c, i):
        t = chunk(c, major_at[c], wrap(minor_at[c] + dest_offset(i)))
        total = get(p, (c, t))
        for e in range(2):
            total = total + get(rb, (c, e, i, hops(e, i) - 1))
        return t, total

    def rs2_step(i):
        for c in range(2):

            @pl.when(i < 2)
            def _(c=c):
                t, total = rs1_done(c, i)
                put(p, (c, t), total)

            @pl.when(jnp.logical_and(i >= 2, i < n - 1))
            def _(c=c):
                landed(r2.at[c, i - 2], turn_r.at[c, i - 2])
                t, total = rs1_done(c, i)
                put(p, (c, t), total + get(r2, (c, i - 2)))

            @pl.when(jnp.logical_and(i < n - 1, lax.rem(i, 2) == 0))
            def _(c=c):
                rs2_copy(c, i, True).start()

            @pl.when(jnp.logical_and(i < n - 1, lax.rem(i, 2) == 1))
            def _(c=c):
                rs2_copy(c, i, False).start()

            @pl.when(i == n - 1)
            def _(c=c):
                t, total = rs1_done(c, i)
                total = total + adt[c]
                for k in (n - 3, n - 2):
                    landed(r2.at[c, k], turn_r.at[c, k])
                    total = total + get(r2, (c, k))
                igrad[c] = total.astype(BF16)

    def rs_tick(tick):
        for s in range(half + 1):

            def hop(i, s=s):
                for c in range(2):
                    for e in range(2):
                        if s == 0:
                            rs1_copy(c, e, i, s).start()
                        elif s < half - 1:
                            rs1_landed(c, e, i, s - 1)
                            rs1_add_send(c, e, i, s)
                        elif s == half - 1:
                            rs1_landed(c, e, i, s - 1)

                            @pl.when(is_long(e, i))
                            def _(c=c, e=e):
                                rs1_add_send(c, e, i, s)
                        else:

                            @pl.when(is_long(e, i))
                            def _(c=c, e=e):
                                rs1_landed(c, e, i, s - 1)

                if s == half:
                    rs2_step(i)

            streams(tick - s, n - 3, hop)

    def member_of(b):
        end, count = jnp.int32(0), jnp.int32(0)
        for m in range(members):
            end = end + mb[m]
            count = count + jnp.where(end <= d * 2 + b, 1, 0)
        return count

    def weight_of(b, m):
        return jnp.where(member_of(b) == m, F32(1.0), F32(0.0))

    def live(b, shape, dim):
        at = lax.broadcasted_iota(jnp.int32, shape, dim)
        return jnp.where(at < bl[b], F32(1.0), F32(0.0))

    def rows(b):
        return pl.ds(b * BLOCK, BLOCK)

    def mask_step():
        for b in range(2):
            across = jnp.transpose(cot[:, b * BLOCK : (b + 1) * BLOCK].astype(F32))
            masked[rows(b)] = (across * live(b, across.shape, 0)).astype(BF16)

    def low_rank_start():
        for k in range(2):
            ad_local(k).wait()
            ad_remote(k).wait_recv()
        for b in range(2):
            a, o = weight_of(b, 0) * ain[0].astype(F32), weight_of(b, 0) * aout[0].astype(F32)
            for m in range(1, members):
                a = a + weight_of(b, m) * ain[m].astype(F32)
                o = o + weight_of(b, m) * aout[m].astype(F32)
            cin[b], cout[b] = a.astype(BF16), o.astype(BF16)
        tall = part.shape[1]
        for b in range(2):
            into = dot(g[b, me], cin[b], NT)
            back = dot(masked[rows(b)], cout[b], NT)
            both = jnp.concatenate([into, back], axis=1)
            each = BLOCK // tall
            part[pl.ds(b * each, each)] = both.reshape(each, tall, 2 * rank)

    def x_copy(e, s):
        way = 1 - 2 * e
        piece = wrap(x + way * (half - e - s))
        to = {COL: wrap(x + way)}
        return remote(part.at[piece], xbuf.at[e, s], low_s.at[0], xz_r.at[e, s], to)

    def x_step(s):
        for e in range(2):
            if 1 <= s <= half - e:
                piece = wrap(x + (1 - 2 * e) * (half - e - s))
                landed(xbuf.at[e, s - 1], xz_r.at[e, s - 1])
                part[piece] = part[piece] + xbuf[e, s - 1]
            if s < half - e:
                x_copy(e, s).start()

    def round_copy(buf, at, axis, ss, rs, e, s):
        src = wrap(at - (1 - 2 * e) * s)
        to = {axis: wrap(at + 1 - 2 * e)}
        return remote(buf.at[src], buf.at[src], ss, rs.at[e, s], to)

    def round_step(ring, s):
        buf, at, axis, ss, rs = ring
        for e in range(2):
            if 1 <= s <= half - e:
                landed(buf.at[wrap(at - (1 - 2 * e) * s)], rs.at[e, s - 1])
            if s < half - e:
                round_copy(*ring, e, s).start()

    y_ring, z_ring = (ybuf, y, ROW, low_s.at[1], y_r), (low, x, COL, low_s.at[2], xz_r)

    def total_of(ref):
        total = ref[0]
        for k in range(1, n):
            total = total + ref[k]
        return total

    def low_step(k):
        if k <= half:
            x_step(k)
        if k == half:
            ybuf[y] = part[x]
        if half <= k <= 2 * half:
            round_step(y_ring, k - half)
        if k == 2 * half:
            low[x] = total_of(ybuf).astype(BF16)
        if 2 * half <= k:
            round_step(z_ring, k - 2 * half)

    def low_of(b):
        each = n // 2
        both = low[pl.ds(b * each, each)].reshape(BLOCK, 2 * rank)
        return both[:, :rank], both[:, rank:]

    def g_copy(k):
        src, dst = ((usend, urecv), (dsend, drecv))[k]
        return remote(src, dst, gx_s.at[k], gx_r.at[k], mate)

    def grads_start():
        ups, downs = [], []
        for b in range(2):
            into, back = low_of(b)
            ups.append(SCALE * dot(into, masked[rows(b)], TN))
            downs.append(SCALE * dot(back, g[b, me], TN))
        for q in range(owned):
            theirs, mine = (1 - d) * owned + q, d * owned + q
            usend[q] = weight_of(0, theirs) * ups[0] + weight_of(1, theirs) * ups[1]
            dsend[q] = weight_of(0, theirs) * downs[0] + weight_of(1, theirs) * downs[1]
            ugrad[q] = weight_of(0, mine) * ups[0] + weight_of(1, mine) * ups[1]
            dgrad[q] = weight_of(0, mine) * downs[0] + weight_of(1, mine) * downs[1]

    def terms_step():
        for b in range(2):
            into, back = low_of(b)
            turned = jnp.transpose(into.astype(F32)).astype(BF16)
            acc[:, b * BLOCK : (b + 1) * BLOCK] += SCALE * dot(cout[b], turned, TN)
            adt[b] = SCALE * dot(back, cin[b], NN)

    def grads_done():
        for k in range(2):
            g_copy(k).wait_recv()
        for q in range(owned):
            ugrad[q] = ugrad[q] + urecv[q]
            dgrad[q] = dgrad[q] + drecv[q]

    def back_chunk(k):
        t = lax.rem(d * own_chunks + k, chunks)
        out = dot(masked[...], w_chunk(t), NN)
        for b in range(2):
            put(p, (b, t), out[b * BLOCK : (b + 1) * BLOCK])

    def front_group(k):
        first = k * group
        rows_in = jnp.concatenate(
            [jnp.concatenate([g[0, first + i], g[1, first + i]], axis=0) for i in range(group)], axis=1
        )
        at = pl.multiple_of(first * width, LANES)
        acc[...] += dot(w[:, pl.ds(at, group * width)], rows_in, NT)

    def hidden_step():
        for b in range(2):
            cols = acc[:, b * BLOCK : (b + 1) * BLOCK]
            hidden[:, b * BLOCK : (b + 1) * BLOCK] = (cols * live(b, cols.shape, 1)).astype(BF16)

    def some(body, first, last):
        lax.fori_loop(first, last, lambda k, z: (body(k), z)[1], 0)

    rs_from = n - 1 if n >= 8 else n + 1
    last = max(rs_from + ticks - 1, low_to + 2)
    back_from, back_ticks = early, rs_from - early
    back_each = -(-chunks // back_ticks)
    front_from, front_ticks = ticks, 3
    front_each = -(-(chunks // group) // front_ticks)

    def every_tick(tick, carry):
        @pl.when(tick < ticks)
        def _():
            ag_tick(tick)

        @pl.when(tick >= rs_from)
        def _():
            rs_tick(tick - rs_from)

        @pl.when(tick == early - 1)
        def _():
            @pl.when(d == 1)
            def _():
                pl.semaphore_wait(here, 1)

            for k in range(2):
                ad_remote(k).start()
            w_remote.start()
            for k in range(3):
                take(k).wait()
            mask_step()
            acc[...] = jnp.zeros_like(acc)

        @pl.when(tick == low_from)
        def _():
            low_rank_start()
            w_local.wait()

        for k in range(3 * half + 1):

            @pl.when(tick == low_from + k)
            def _(k=k):
                low_step(k)

        @pl.when(tick == middle)
        def _():
            landed(w_half(1 - d), wx_r)

        @pl.when(tick == low_to)
        def _():
            grads_start()
            for k in range(2):
                g_copy(k).start()
            terms_step()

        @pl.when(tick == low_to + 2)
        def _():
            grads_done()

        @pl.when(jnp.logical_and(tick >= back_from, tick < back_from + back_ticks))
        def _():
            first = (tick - back_from) * back_each
            some(back_chunk, first, jnp.minimum(first + back_each, chunks))

        @pl.when(jnp.logical_and(tick >= front_from, tick < front_from + front_ticks))
        def _():
            first = (tick - front_from) * front_each
            some(front_group, first, jnp.minimum(first + front_each, chunks // group))

        @pl.when(tick == front_from + front_ticks)
        def _():
            hidden_step()

        return carry

    lax.fori_loop(0, last + 1, every_tick, 0)


    for k in range(2):
        ad_remote(k).wait_send()
        g_copy(k).wait_send()
    w_remote.wait_send()

    def sent(src, sem):
        pltpu.make_async_copy(src, src, sem).wait()

    for k, buf in enumerate((part, ybuf, low)):
        sent(buf.at[pl.ds(0, n - 1)], low_s.at[k])
    for c in range(2):
        sent(g.at[c, pl.ds(0, chunks - 1)], ag_s.at[c])
        sent(p.at[c, pl.ds(0, chunks - 1)], rs_s.at[c])


def hand_over(*refs):
    copies = [pltpu.make_async_copy(refs[k], refs[4 + k], refs[8].at[k]) for k in range(4)]
    for copy in copies:
        copy.start()
    for copy in copies:
        copy.wait()


def local(n, tokens, weight, adapter_in, adapter_out, cotangent, member_blocks, block_live):
    token_rows, width = tokens.shape
    hidden_width = weight.shape[1]
    blocks = token_rows // BLOCK
    owned, _, rank = adapter_in.shape
    members = 2 * owned
    half = n // 2
    tall = token_rows // n
    chunks = n * n
    vmem, hbm = (pl.BlockSpec(memory_space=s) for s in (pltpu.VMEM, pltpu.HBM))
    coded = BLOCK * width // (2 * LANES) + 1
    dma = lambda *shape: pltpu.SemaphoreType.DMA(shape)
    both_ways = (2, 2, n, half)
    out = pl.pallas_call(
        functools.partial(kernel, n),
        out_shape=(
            jax.ShapeDtypeStruct((hidden_width, token_rows), BF16),
            jax.ShapeDtypeStruct((blocks, BLOCK, width), BF16),
            jax.ShapeDtypeStruct((owned, rank, width), F32),
            jax.ShapeDtypeStruct((owned, rank, hidden_width), F32),
        ),
        in_specs=[hbm] * 7,
        out_specs=(vmem,) * 4,
        scratch_shapes=[
            pltpu.SMEM(member_blocks.shape, jnp.int32),
            pltpu.SMEM(block_live.shape, jnp.int32),
            pltpu.VMEM((hidden_width, token_rows), BF16),
            pltpu.VMEM((blocks, chunks, BLOCK, width), BF16),
            pltpu.VMEM((hidden_width, chunks * width), BF16),
            pltpu.VMEM((blocks, chunks, coded, LANES), jnp.int32),
            pltpu.VMEM((*both_ways, coded, LANES), jnp.int32),
            pltpu.VMEM((2, n - 1, coded, LANES), jnp.int32),
            pltpu.VMEM((token_rows, hidden_width), BF16),
            pltpu.VMEM((hidden_width, token_rows), F32),
            pltpu.VMEM((blocks, BLOCK, width), F32),
            pltpu.VMEM((members, rank, width), BF16),
            pltpu.VMEM((members, rank, hidden_width), BF16),
            pltpu.VMEM((blocks, rank, width), BF16),
            pltpu.VMEM((blocks, rank, hidden_width), BF16),
            pltpu.VMEM((n, tall, 2 * rank), F32),
            pltpu.VMEM((2, half, tall, 2 * rank), F32),
            pltpu.VMEM((n, tall, 2 * rank), F32),
            pltpu.VMEM((n, tall, 2 * rank), BF16),
            pltpu.VMEM((owned, rank, hidden_width), F32),
            pltpu.VMEM((owned, rank, width), F32),
            pltpu.VMEM((owned, rank, hidden_width), F32),
            pltpu.VMEM((owned, rank, width), F32),
            dma(2),
            dma(2),
            dma(2, 2, 5 if n >= 8 else 2 * n, half),
            dma(2, n),
            pltpu.SemaphoreType.DMA,
            pltpu.SemaphoreType.DMA,
            pltpu.SemaphoreType.DMA,
            pltpu.SemaphoreType.DMA,
            dma(2),
            dma(2),
            dma(2),
            dma(3),
            dma(2, half),
            dma(2, half),
            dma(2),
            dma(2),
            dma(3),
            pltpu.SemaphoreType.REGULAR,
        ],
        compiler_params=pltpu.CompilerParams(
            collective_id=0, has_side_effects=True, vmem_limit_bytes=47 * 2**20
        ),
        name="step",
    )(
        *(
            pltpu.with_memory_space_constraint(v, pltpu.HBM)
            for v in (
                member_blocks,
                block_live,
                tokens.reshape(blocks, BLOCK, width),
                weight.T,
                jnp.swapaxes(adapter_in, 1, 2),
                adapter_out,
                cotangent.T,
            )
        )
    )
    out = pl.pallas_call(
        hand_over,
        out_shape=tuple(jax.ShapeDtypeStruct(o.shape, o.dtype) for o in out),
        in_specs=[vmem] * 4,
        out_specs=(hbm,) * 4,
        scratch_shapes=[dma(4)],
        compiler_params=pltpu.CompilerParams(vmem_limit_bytes=4 * 2**20),
        name="hand_over",
    )(*out)
    return (
        out[0].T,
        out[1].reshape(token_rows, width),
        jnp.swapaxes(out[2], 1, 2),
        out[3],
    )


def solution(mesh):
    n = math.isqrt(mesh.shape["tensor"])
    tensor = (ROW, COL)
    finer = Mesh(
        mesh.devices.reshape(mesh.shape["pop"], mesh.shape["dp"], n, n), ("pop", CORE, ROW, COL)
    )
    return jax.shard_map(
        functools.partial(local, n),
        mesh=finer,
        in_specs=(
            P(("pop", "dp"), tensor),
            P("dp", tensor),
            P(("pop", "dp"), tensor, None),
            P(("pop", "dp"), None, tensor),
            P(("pop", "dp"), tensor),
            P("pop"),
            P(("pop", "dp")),
        ),
        out_specs=(
            P(("pop", "dp"), tensor),
            P(("pop", "dp"), tensor),
            P(("pop", "dp"), tensor, None),
            P(("pop", "dp"), None, tensor),
        ),
        check_vma=False,
    )
```

```python
import functools
import math

import jax
import jax.numpy as jnp
from jax import lax
from jax.experimental import pallas as pl
from jax.experimental.pallas import tpu as pltpu
from jax.sharding import Mesh
from jax.sharding import PartitionSpec as P

BLOCK = 128
SCALE = 0.5
MESH = pl.DeviceIdType.MESH
ROW, COL, CORE = "tensor_0", "tensor_1", "dp"
F32, BF16 = jnp.float32, jnp.bfloat16

NN = (((1,), (0,)), ((), ()))
NT = (((1,), (1,)), ((), ()))
TN = (((0,), (0,)), ((), ()))


def dot(a, b, dims):
    return lax.dot_general(a, b, dims, preferred_element_type=F32)


LANES = 128
UNIT = 2.0**21
TOP = 32760.0


def halves(v):
    return [v[:, k : k + LANES] for k in range(0, v.shape[1], LANES)]


def put(ref, at, v):
    parts = halves(v)
    largest = jnp.max(functools.reduce(jnp.maximum, [jnp.abs(q) for q in parts]), axis=0, keepdims=True)
    scale = (largest * UNIT).astype(jnp.int32) + 1
    by = (TOP * UNIT) / scale.astype(F32)
    mid = v.shape[0] // 2
    for k, q in enumerate(parts):
        code = (q * by).astype(jnp.int32)
        ref[(*at, slice(k * mid, (k + 1) * mid))] = (code[:mid] << 16) | (code[mid:] & 0xFFFF)
    ref[(*at, slice(2 * mid, 2 * mid + 1))] = scale


def get(ref, at):
    mid = (ref.shape[-2] - 1) // 2
    scale = ref[(*at, slice(2 * mid, 2 * mid + 1))].astype(F32) * (1.0 / (TOP * UNIT))
    out = []
    for k in range(2):
        pair = ref[(*at, slice(k * mid, (k + 1) * mid))]
        both = jnp.concatenate([pair >> 16, (pair << 16) >> 16], axis=0)
        out.append(both.astype(F32) * scale)
    return jnp.concatenate(out, axis=1)


def kernel(
    n,
    mb_hbm,
    bl_hbm,
    tok_hbm,
    w_hbm,
    ain_hbm,
    aout_hbm,
    cot_hbm,
    hidden,
    igrad,
    dgrad,
    ugrad,
    mb,
    bl,
    cot,
    g,
    w,
    p,
    rb,
    r2,
    masked,
    acc,
    adt,
    ain,
    aout,
    cin,
    cout,
    part,
    xbuf,
    ybuf,
    low,
    usend,
    dsend,
    urecv,
    drecv,
    ag_s,
    rs_s,
    flow_r,
    turn_r,
    held_r,
    own_sem,
    w_sem,
    wx_s,
    wx_r,
    ad_sem,
    adx_s,
    adx_r,
    low_s,
    xz_r,
    y_r,
    gx_s,
    gx_r,
    in_sem,
    here,
):
    half = n // 2
    ticks = n - 1 + half
    cycle, shift = (5, 3) if n >= 8 else (2 * n, n)
    early, middle = n // 4, n // 2
    low_from = early
    low_to = low_from + 3 * half
    y, x, d = lax.axis_index(ROW), lax.axis_index(COL), lax.axis_index(CORE)
    mate = {CORE: 1 - d}
    me = y * n + x
    chunks = n * n
    group = 4
    members = ain.shape[0]
    owned = members // 2
    width = g.shape[3]
    own_depth = w_hbm.shape[1]
    own_chunks = own_depth // width
    rank = ain.shape[1]
    minor_axis, major_axis = (COL, ROW), (ROW, COL)
    minor_at, major_at = (x, y), (y, x)

    def chunk(c, major, minor):
        return major * n + minor if c == 0 else minor * n + major

    def wrap(v):
        return lax.rem(v + 2 * n, n)

    def remote(src, dst, ss, rs, to):
        return pltpu.make_async_remote_copy(
            src_ref=src, dst_ref=dst, send_sem=ss, recv_sem=rs, device_id=to, device_id_type=MESH
        )

    def landed(dst, sem):
        pltpu.make_async_copy(dst, dst, sem).wait()

    barrier = pltpu.get_barrier_semaphore()
    for step in (1, n - 1):
        pl.semaphore_signal(barrier, inc=1, device_id={COL: wrap(x + step)}, device_id_type=MESH)
        pl.semaphore_signal(barrier, inc=1, device_id={ROW: wrap(y + step)}, device_id_type=MESH)

    @pl.when(d == 1)
    def _():
        pl.semaphore_signal(barrier, inc=1, device_id=mate, device_id_type=MESH)

    own = pltpu.make_async_copy(tok_hbm, g.at[:, me], own_sem)
    own.start()
    taken = ((mb_hbm, mb), (bl_hbm, bl), (cot_hbm, cot))

    def take(k):
        return pltpu.make_async_copy(*taken[k], in_sem.at[k])

    for k in range(3):
        take(k).start()

    def ad_local(k):
        hbm, vm = ((ain_hbm, ain), (aout_hbm, aout))[k]
        return pltpu.make_async_copy(hbm, vm.at[pl.ds(d * owned, owned)], ad_sem.at[k])

    def ad_remote(k):
        hbm, vm = ((ain_hbm, ain), (aout_hbm, aout))[k]
        return remote(hbm, vm.at[pl.ds(d * owned, owned)], adx_s.at[k], adx_r.at[k], mate)

    def w_half(core):
        return w.at[:, pl.ds(pl.multiple_of(core * own_depth, LANES), own_depth)]

    w_local = pltpu.make_async_copy(w_hbm, w_half(d), w_sem)
    w_remote = remote(w_hbm, w_half(d), wx_s, wx_r, mate)

    def w_chunk(t):
        return w[:, pl.ds(pl.multiple_of(t * width, LANES), width)]

    for k in range(2):
        ad_local(k).start()
    w_local.start()
    own.wait()
    pl.semaphore_wait(barrier, 4 + 1 - d)

    @pl.when(d == 0)
    def _():
        pl.semaphore_signal(here, inc=1, device_id=mate, device_id_type=MESH)


    def minor_offset(j):
        back = lax.div(j + 1, 2)
        return jnp.where(lax.rem(j, 2) == 1, -back, lax.div(j, 2))

    def ag1_copy(c, j, right):
        src = chunk(c, major_at[c], wrap(minor_at[c] + minor_offset(j)))
        lands = jnp.where(j == 0, 1 if right else 2, j + 2)
        to = {minor_axis[c]: wrap(minor_at[c] + (1 if right else -1))}
        return remote(g.at[c, src], g.at[c, src], ag_s.at[c], turn_r.at[c, lands], to)

    def ag1_step(j):
        for c in range(2):
            src = chunk(c, major_at[c], wrap(minor_at[c] + minor_offset(j)))

            @pl.when(j >= 1)
            def _(c=c, src=src):
                landed(g.at[c, src], turn_r.at[c, j])

            @pl.when(jnp.logical_or(j == 0, jnp.logical_and(lax.rem(j, 2) == 1, j + 2 < n)))
            def _(c=c):
                ag1_copy(c, j, True).start()

            @pl.when(jnp.logical_and(lax.rem(j, 2) == 0, j + 2 < n))
            def _(c=c):
                ag1_copy(c, j, False).start()

    def ag2_copy(c, e, j, s):
        way = 1 - 2 * e
        t = chunk(c, wrap(major_at[c] - way * s), wrap(minor_at[c] + minor_offset(j)))
        to = {major_axis[c]: wrap(major_at[c] + way)}
        return remote(g.at[c, t], g.at[c, t], ag_s.at[c], flow_r.at[c, e, lax.rem(j, cycle), s], to)

    def ag2_landed(c, e, j, s):
        t = chunk(c, wrap(major_at[c] - (1 - 2 * e) * s), wrap(minor_at[c] + minor_offset(j)))
        landed(g.at[c, t], flow_r.at[c, e, lax.rem(j, cycle), s - 1])

    held = min(6, n)

    def held_chunk(c, j, s):
        return chunk(c, wrap(major_at[c] - (1 - 2 * (j % 2)) * s), wrap(minor_at[c] + minor_offset(j)))

    def held_copy(c, j):
        t = held_chunk(c, j, half - 1)
        to = {major_axis[c]: wrap(major_at[c] + 1 - 2 * (j % 2))}
        return remote(g.at[c, t], g.at[c, t], ag_s.at[c], held_r.at[c, j], to)

    def held_send(first, stop):
        for j in range(first, stop):
            for c in range(2):
                held_copy(c, j).start()

    def held_landed():
        for j in range(held):
            for c in range(2):
                landed(g.at[c, held_chunk(c, j, half)], held_r.at[c, j])

    def is_long(e, j):
        return lax.rem(j, 2) == e

    def streams(at, first, body):
        j = at + jnp.where(at > first, 1, 0)

        @pl.when(jnp.logical_and(at >= 0, at < n - 1))
        def _():
            lax.fori_loop(j, j + 1 + jnp.where(at == first, 1, 0), lambda k, z: (body(k), z)[1], 0)

    def ag_tick(tick, steps):
        if 0 in steps:
            streams(tick, 1, ag1_step)
        for s in steps:

            def hop(j, s=s):
                for c in range(2):
                    for e in range(2):
                        if s < half:
                            if s > 0:
                                ag2_landed(c, e, j, s)
                            if s < half - 1:
                                ag2_copy(c, e, j, s).start()
                            else:

                                @pl.when(jnp.logical_and(is_long(e, j), j >= held))
                                def _(c=c, e=e):
                                    ag2_copy(c, e, j, s).start()
                        else:

                            @pl.when(jnp.logical_and(is_long(e, j), j >= held))
                            def _(c=c, e=e):
                                ag2_landed(c, e, j, s)

            streams(tick - s, 1, hop)

    def dest_offset(i):
        ahead = lax.div(n - i, 2)
        back = lax.div(n - 1 - i, 2)
        return jnp.where(lax.rem(i, 2) == 0, ahead, -back)

    def hops(e, i):
        return jnp.where(is_long(e, i), half, half - 1)

    def rs1_chunk(c, e, i, s):
        far = (1 - 2 * e) * (hops(e, i) - s)
        return chunk(c, wrap(major_at[c] + far), wrap(minor_at[c] + dest_offset(i)))

    def rs1_sem(c, e, i, s):
        return flow_r.at[c, e, lax.rem(i + shift, cycle), s]

    def rs1_landed(c, e, i, s):
        landed(rb.at[c, e, i, s], rs1_sem(c, e, i, s))

    def rs1_copy(c, e, i, s):
        t = rs1_chunk(c, e, i, s)
        to = {major_axis[c]: wrap(major_at[c] + 1 - 2 * e)}
        return remote(p.at[c, t], rb.at[c, e, i, s], rs_s.at[c], rs1_sem(c, e, i, s), to)

    def rs1_add_send(c, e, i, s):
        t = rs1_chunk(c, e, i, s)
        put(p, (c, t), get(p, (c, t)) + get(rb, (c, e, i, s - 1)))
        rs1_copy(c, e, i, s).start()

    def rs2_copy(c, i, right):
        t = chunk(c, major_at[c], wrap(minor_at[c] + dest_offset(i)))
        to = {minor_axis[c]: wrap(minor_at[c] + (1 if right else -1))}
        return remote(p.at[c, t], r2.at[c, i], rs_s.at[c], turn_r.at[c, i], to)

    def rs1_done(c, i):
        t = chunk(c, major_at[c], wrap(minor_at[c] + dest_offset(i)))
        total = get(p, (c, t))
        for e in range(2):
            total = total + get(rb, (c, e, i, hops(e, i) - 1))
        return t, total

    def rs2_step(i):
        for c in range(2):

            @pl.when(i < 2)
            def _(c=c):
                t, total = rs1_done(c, i)
                put(p, (c, t), total)

            @pl.when(jnp.logical_and(i >= 2, i < n - 1))
            def _(c=c):
                landed(r2.at[c, i - 2], turn_r.at[c, i - 2])
                t, total = rs1_done(c, i)
                put(p, (c, t), total + get(r2, (c, i - 2)))

            @pl.when(jnp.logical_and(i < n - 1, lax.rem(i, 2) == 0))
            def _(c=c):
                rs2_copy(c, i, True).start()

            @pl.when(jnp.logical_and(i < n - 1, lax.rem(i, 2) == 1))
            def _(c=c):
                rs2_copy(c, i, False).start()

            @pl.when(i == n - 1)
            def _(c=c):
                t, total = rs1_done(c, i)
                total = total + adt[c]
                for k in (n - 3, n - 2):
                    landed(r2.at[c, k], turn_r.at[c, k])
                    total = total + get(r2, (c, k))
                igrad[c] = total.astype(BF16)

    def rs_tick(tick, steps):
        for s in steps:

            def hop(i, s=s):
                for c in range(2):
                    for e in range(2):
                        if s == 0:
                            rs1_copy(c, e, i, s).start()
                        elif s < half - 1:
                            rs1_landed(c, e, i, s - 1)
                            rs1_add_send(c, e, i, s)
                        elif s == half - 1:
                            rs1_landed(c, e, i, s - 1)

                            @pl.when(is_long(e, i))
                            def _(c=c, e=e):
                                rs1_add_send(c, e, i, s)
                        else:

                            @pl.when(is_long(e, i))
                            def _(c=c, e=e):
                                rs1_landed(c, e, i, s - 1)

                if s == half:
                    rs2_step(i)

            streams(tick - s, n - 3, hop)

    def some(body, first, last):
        lax.fori_loop(first, last, lambda k, z: (body(k), z)[1], 0)

    def member_of(b):
        end, count = jnp.int32(0), jnp.int32(0)
        for m in range(members):
            end = end + mb[m]
            count = count + jnp.where(end <= d * 2 + b, 1, 0)
        return count

    def weight_of(b, m):
        return jnp.where(member_of(b) == m, F32(1.0), F32(0.0))

    def live(b, shape, dim):
        at = lax.broadcasted_iota(jnp.int32, shape, dim)
        return jnp.where(at < bl[b], F32(1.0), F32(0.0))

    def rows(b):
        return pl.ds(b * BLOCK, BLOCK)

    def mask_step():
        for b in range(2):
            across = jnp.transpose(cot[:, b * BLOCK : (b + 1) * BLOCK].astype(F32))
            masked[rows(b)] = (across * live(b, across.shape, 0)).astype(BF16)

    def low_rank_start():
        for k in range(2):
            ad_local(k).wait()
            ad_remote(k).wait_recv()
        for b in range(2):
            a, o = weight_of(b, 0) * ain[0].astype(F32), weight_of(b, 0) * aout[0].astype(F32)
            for m in range(1, members):
                a = a + weight_of(b, m) * ain[m].astype(F32)
                o = o + weight_of(b, m) * aout[m].astype(F32)
            cin[b], cout[b] = a.astype(BF16), o.astype(BF16)
        tall = part.shape[1]
        for b in range(2):
            into = dot(g[b, me], cin[b], NT)
            back = dot(masked[rows(b)], cout[b], NT)
            both = jnp.concatenate([into, back], axis=1)
            each = BLOCK // tall
            part[pl.ds(b * each, each)] = both.reshape(each, tall, 2 * rank)

    def x_copy(e, s):
        way = 1 - 2 * e
        piece = wrap(x + way * (half - e - s))
        to = {COL: wrap(x + way)}
        return remote(part.at[piece], xbuf.at[e, s], low_s.at[0], xz_r.at[e, s], to)

    def x_step(s):
        for e in range(2):
            if 1 <= s <= half - e:
                piece = wrap(x + (1 - 2 * e) * (half - e - s))
                landed(xbuf.at[e, s - 1], xz_r.at[e, s - 1])
                part[piece] = part[piece] + xbuf[e, s - 1]
            if s < half - e:
                x_copy(e, s).start()

    def round_copy(buf, at, axis, ss, rs, e, s):
        src = wrap(at - (1 - 2 * e) * s)
        to = {axis: wrap(at + 1 - 2 * e)}
        return remote(buf.at[src], buf.at[src], ss, rs.at[e, s], to)

    def round_step(ring, s):
        buf, at, axis, ss, rs = ring
        for e in range(2):
            if 1 <= s <= half - e:
                landed(buf.at[wrap(at - (1 - 2 * e) * s)], rs.at[e, s - 1])
            if s < half - e:
                round_copy(*ring, e, s).start()

    y_ring, z_ring = (ybuf, y, ROW, low_s.at[1], y_r), (low, x, COL, low_s.at[2], xz_r)

    def total_of(ref):
        total = ref[0]
        for k in range(1, n):
            total = total + ref[k]
        return total

    def low_step(k):
        if k <= half:
            x_step(k)
        if k == half:
            ybuf[y] = part[x]
        if half <= k <= 2 * half:
            round_step(y_ring, k - half)
        if k == 2 * half:
            low[x] = total_of(ybuf).astype(BF16)
        if 2 * half <= k:
            round_step(z_ring, k - 2 * half)

    def low_of(b):
        each = n // 2
        both = low[pl.ds(b * each, each)].reshape(BLOCK, 2 * rank)
        return both[:, :rank], both[:, rank:]

    def g_copy(k):
        src, dst = ((usend, urecv), (dsend, drecv))[k]
        return remote(src, dst, gx_s.at[k], gx_r.at[k], mate)

    def grads_start():
        ups, downs = [], []
        for b in range(2):
            into, back = low_of(b)
            ups.append(SCALE * dot(into, masked[rows(b)], TN))
            downs.append(SCALE * dot(back, g[b, me], TN))
        for q in range(owned):
            theirs, mine = (1 - d) * owned + q, d * owned + q
            usend[q] = weight_of(0, theirs) * ups[0] + weight_of(1, theirs) * ups[1]
            dsend[q] = weight_of(0, theirs) * downs[0] + weight_of(1, theirs) * downs[1]
            ugrad[q] = weight_of(0, mine) * ups[0] + weight_of(1, mine) * ups[1]
            dgrad[q] = weight_of(0, mine) * downs[0] + weight_of(1, mine) * downs[1]

    def terms_step():
        for b in range(2):
            into, back = low_of(b)
            turned = jnp.transpose(into.astype(F32)).astype(BF16)
            acc[:, b * BLOCK : (b + 1) * BLOCK] += SCALE * dot(cout[b], turned, TN)
            adt[b] = SCALE * dot(back, cin[b], NN)

    def grads_done():
        for k in range(2):
            g_copy(k).wait_recv()
        for q in range(owned):
            ugrad[q] = ugrad[q] + urecv[q]
            dgrad[q] = dgrad[q] + drecv[q]

    def back_chunk(k):
        t = lax.rem(d * own_chunks + k, chunks)
        out = dot(masked[...], w_chunk(t), NN)
        for b in range(2):
            put(p, (b, t), out[b * BLOCK : (b + 1) * BLOCK])

    far_row, far_col = wrap(y + half), wrap(x + half)

    def front_group(row, q, hole):
        first = row * n + q * group
        there = [first + i for i in range(group)]
        if hole:
            there = [jnp.where(q * group + i == far_col, chunks, t) for i, t in enumerate(there)]
        rows_in = jnp.concatenate(
            [jnp.concatenate([g[0, first + i], g[1, t]], axis=0) for i, t in enumerate(there)], axis=1
        )
        at = pl.multiple_of(first * width, LANES)
        acc[...] += dot(w[:, pl.ds(at, group * width)], rows_in, NT)

    def front_early(k):
        front_group(wrap(far_row + 1 + lax.div(k, n // group)), lax.rem(k, n // group), True)

    def front_late():
        for q in range(n // group):
            front_group(far_row, q, False)

        def column(k):
            t = wrap(far_row + k) * n + far_col
            acc[:, BLOCK:] += dot(w_chunk(t), g[1, t], NT)

        some(column, 1, n)

    def hidden_step():
        for b in range(2):
            cols = acc[:, b * BLOCK : (b + 1) * BLOCK]
            hidden[:, b * BLOCK : (b + 1) * BLOCK] = (cols * live(b, cols.shape, 1)).astype(BF16)

    rs_from = n - 1 if n >= 8 else n + 1
    last = max(rs_from + ticks - 1, low_to + 2, rs_from + n + 1)
    back_from, back_ticks = early, rs_from - early
    back_each = -(-chunks // back_ticks)
    front_from, front_ticks = ticks, 3
    fronts = (n - 1) * (n // group)
    front_each = -(-fronts // front_ticks)
    tail = rs_from + n - 1

    def messages(tick, steps):
        @pl.when(tick < ticks)
        def _():
            ag_tick(tick, steps)

        @pl.when(tick >= rs_from)
        def _():
            rs_tick(tick - rs_from, steps)

    def every_tick(tick, carry):
        messages(tick, range(half - 1))

        @pl.when(tick == early - 1)
        def _():
            @pl.when(d == 1)
            def _():
                pl.semaphore_wait(here, 1)

            for k in range(2):
                ad_remote(k).start()
            w_remote.start()
            for k in range(3):
                take(k).wait()
            mask_step()
            acc[...] = jnp.zeros_like(acc)
            g[1, chunks] = jnp.zeros(g.shape[2:], BF16)

        @pl.when(tick == low_from)
        def _():
            low_rank_start()
            w_local.wait()

        @pl.when(tick == middle)
        def _():
            landed(w_half(1 - d), wx_r)

        @pl.when(jnp.logical_and(tick >= back_from, tick < back_from + back_ticks))
        def _():
            first = (tick - back_from) * back_each
            some(back_chunk, first, jnp.minimum(first + back_each, chunks))

        @pl.when(jnp.logical_and(tick >= front_from, tick < front_from + front_ticks))
        def _():
            first = (tick - front_from) * front_each
            some(front_early, first, jnp.minimum(first + front_each, fronts))

        messages(tick, range(half - 1, half + 1))

        for k in range(3 * half + 1):

            @pl.when(tick == low_from + k)
            def _(k=k):
                low_step(k)

        @pl.when(tick == low_to)
        def _():
            grads_start()
            for k in range(2):
                g_copy(k).start()
            terms_step()

        @pl.when(tick == low_to + 2)
        def _():
            grads_done()

        @pl.when(tick == tail)
        def _():
            held_send(0, 2)

        @pl.when(tick == tail + 1)
        def _():
            held_send(2, held)

        @pl.when(tick == tail + 2)
        def _():
            held_landed()
            front_late()
            hidden_step()

        return carry

    lax.fori_loop(0, last + 1, every_tick, 0)


    for k in range(2):
        ad_remote(k).wait_send()
        g_copy(k).wait_send()
    w_remote.wait_send()

    def sent(src, sem):
        pltpu.make_async_copy(src, src, sem).wait()

    for k, buf in enumerate((part, ybuf, low)):
        sent(buf.at[pl.ds(0, n - 1)], low_s.at[k])
    for c in range(2):
        sent(g.at[c, pl.ds(0, chunks - 1)], ag_s.at[c])
        sent(p.at[c, pl.ds(0, chunks - 1)], rs_s.at[c])


def hand_over(*refs):
    copies = [pltpu.make_async_copy(refs[k], refs[4 + k], refs[8].at[k]) for k in range(4)]
    for copy in copies:
        copy.start()
    for copy in copies:
        copy.wait()


def local(n, tokens, weight, adapter_in, adapter_out, cotangent, member_blocks, block_live):
    token_rows, width = tokens.shape
    hidden_width = weight.shape[1]
    blocks = token_rows // BLOCK
    owned, _, rank = adapter_in.shape
    members = 2 * owned
    half = n // 2
    tall = token_rows // n
    chunks = n * n
    vmem, hbm = (pl.BlockSpec(memory_space=s) for s in (pltpu.VMEM, pltpu.HBM))
    coded = BLOCK * width // (2 * LANES) + 1
    dma = lambda *shape: pltpu.SemaphoreType.DMA(shape)
    both_ways = (2, 2, n, half)
    out = pl.pallas_call(
        functools.partial(kernel, n),
        out_shape=(
            jax.ShapeDtypeStruct((hidden_width, token_rows), BF16),
            jax.ShapeDtypeStruct((blocks, BLOCK, width), BF16),
            jax.ShapeDtypeStruct((owned, rank, width), F32),
            jax.ShapeDtypeStruct((owned, rank, hidden_width), F32),
        ),
        in_specs=[hbm] * 7,
        out_specs=(vmem,) * 4,
        scratch_shapes=[
            pltpu.SMEM(member_blocks.shape, jnp.int32),
            pltpu.SMEM(block_live.shape, jnp.int32),
            pltpu.VMEM((hidden_width, token_rows), BF16),
            pltpu.VMEM((blocks, chunks + 1, BLOCK, width), BF16),
            pltpu.VMEM((hidden_width, chunks * width), BF16),
            pltpu.VMEM((blocks, chunks, coded, LANES), jnp.int32),
            pltpu.VMEM((*both_ways, coded, LANES), jnp.int32),
            pltpu.VMEM((2, n - 1, coded, LANES), jnp.int32),
            pltpu.VMEM((token_rows, hidden_width), BF16),
            pltpu.VMEM((hidden_width, token_rows), F32),
            pltpu.VMEM((blocks, BLOCK, width), F32),
            pltpu.VMEM((members, rank, width), BF16),
            pltpu.VMEM((members, rank, hidden_width), BF16),
            pltpu.VMEM((blocks, rank, width), BF16),
            pltpu.VMEM((blocks, rank, hidden_width), BF16),
            pltpu.VMEM((n, tall, 2 * rank), F32),
            pltpu.VMEM((2, half, tall, 2 * rank), F32),
            pltpu.VMEM((n, tall, 2 * rank), F32),
            pltpu.VMEM((n, tall, 2 * rank), BF16),
            pltpu.VMEM((owned, rank, hidden_width), F32),
            pltpu.VMEM((owned, rank, width), F32),
            pltpu.VMEM((owned, rank, hidden_width), F32),
            pltpu.VMEM((owned, rank, width), F32),
            dma(2),
            dma(2),
            dma(2, 2, 5 if n >= 8 else 2 * n, half),
            dma(2, n),
            dma(2, min(6, n)),
            pltpu.SemaphoreType.DMA,
            pltpu.SemaphoreType.DMA,
            pltpu.SemaphoreType.DMA,
            pltpu.SemaphoreType.DMA,
            dma(2),
            dma(2),
            dma(2),
            dma(3),
            dma(2, half),
            dma(2, half),
            dma(2),
            dma(2),
            dma(3),
            pltpu.SemaphoreType.REGULAR,
        ],
        compiler_params=pltpu.CompilerParams(
            collective_id=0, has_side_effects=True, vmem_limit_bytes=47 * 2**20
        ),
        name="step",
    )(
        *(
            pltpu.with_memory_space_constraint(v, pltpu.HBM)
            for v in (
                member_blocks,
                block_live,
                tokens.reshape(blocks, BLOCK, width),
                weight.T,
                jnp.swapaxes(adapter_in, 1, 2),
                adapter_out,
                cotangent.T,
            )
        )
    )
    out = pl.pallas_call(
        hand_over,
        out_shape=tuple(jax.ShapeDtypeStruct(o.shape, o.dtype) for o in out),
        in_specs=[vmem] * 4,
        out_specs=(hbm,) * 4,
        scratch_shapes=[dma(4)],
        compiler_params=pltpu.CompilerParams(vmem_limit_bytes=4 * 2**20),
        name="hand_over",
    )(*out)
    return (
        out[0].T,
        out[1].reshape(token_rows, width),
        jnp.swapaxes(out[2], 1, 2),
        out[3],
    )


def solution(mesh):
    n = math.isqrt(mesh.shape["tensor"])
    tensor = (ROW, COL)
    finer = Mesh(
        mesh.devices.reshape(mesh.shape["pop"], mesh.shape["dp"], n, n), ("pop", CORE, ROW, COL)
    )
    return jax.shard_map(
        functools.partial(local, n),
        mesh=finer,
        in_specs=(
            P(("pop", "dp"), tensor),
            P("dp", tensor),
            P(("pop", "dp"), tensor, None),
            P(("pop", "dp"), None, tensor),
            P(("pop", "dp"), tensor),
            P("pop"),
            P(("pop", "dp")),
        ),
        out_specs=(
            P(("pop", "dp"), tensor),
            P(("pop", "dp"), tensor),
            P(("pop", "dp"), tensor, None),
            P(("pop", "dp"), None, tensor),
        ),
        check_vma=False,
    )
```

```python
import functools
import math

import jax
import jax.numpy as jnp
from jax import lax
from jax.experimental import pallas as pl
from jax.experimental.pallas import tpu as pltpu
from jax.sharding import Mesh
from jax.sharding import PartitionSpec as P

BLOCK = 128
SCALE = 0.5
MESH = pl.DeviceIdType.MESH
ROW, COL, CORE = "tensor_0", "tensor_1", "dp"
F32, BF16 = jnp.float32, jnp.bfloat16

NN = (((1,), (0,)), ((), ()))
NT = (((1,), (1,)), ((), ()))
TN = (((0,), (0,)), ((), ()))


def dot(a, b, dims):
    return lax.dot_general(a, b, dims, preferred_element_type=F32)


LANES = 128
UNIT = 2.0**21
TOP = 32760.0


def halves(v):
    return [v[:, k : k + LANES] for k in range(0, v.shape[1], LANES)]


def put(ref, at, v):
    parts = halves(v)
    largest = jnp.max(functools.reduce(jnp.maximum, [jnp.abs(q) for q in parts]), axis=0, keepdims=True)
    scale = (largest * UNIT).astype(jnp.int32) + 1
    by = (TOP * UNIT) / scale.astype(F32)
    mid = v.shape[0] // 2
    for k, q in enumerate(parts):
        code = (q * by).astype(jnp.int32)
        ref[(*at, slice(k * mid, (k + 1) * mid))] = (code[:mid] << 16) | (code[mid:] & 0xFFFF)
    ref[(*at, slice(2 * mid, 2 * mid + 1))] = scale


def get(ref, at):
    mid = (ref.shape[-2] - 1) // 2
    scale = ref[(*at, slice(2 * mid, 2 * mid + 1))].astype(F32) * (1.0 / (TOP * UNIT))
    out = []
    for k in range(2):
        pair = ref[(*at, slice(k * mid, (k + 1) * mid))]
        both = jnp.concatenate([pair >> 16, (pair << 16) >> 16], axis=0)
        out.append(both.astype(F32) * scale)
    return jnp.concatenate(out, axis=1)


def kernel(
    n,
    mb_hbm,
    bl_hbm,
    tok_hbm,
    w_hbm,
    ain_hbm,
    aout_hbm,
    cot_hbm,
    hidden,
    igrad,
    dgrad,
    ugrad,
    mb,
    bl,
    cot,
    g,
    w,
    p,
    rb,
    r2,
    masked,
    acc,
    adt,
    ain,
    aout,
    cin,
    cout,
    part,
    xbuf,
    ybuf,
    low,
    usend,
    dsend,
    urecv,
    drecv,
    ag_s,
    rs_s,
    flow_r,
    turn_r,
    held_r,
    own_sem,
    w_sem,
    wx_s,
    wx_r,
    ad_sem,
    adx_s,
    adx_r,
    low_s,
    xz_r,
    y_r,
    gx_s,
    gx_r,
    in_sem,
    here,
):
    half = n // 2
    ticks = n - 1 + half
    cycle, shift = (5, 3) if n >= 8 else (2 * n, n)
    early, middle = n // 4, n // 2
    low_from = early
    low_to = low_from + 3 * half
    y, x, d = lax.axis_index(ROW), lax.axis_index(COL), lax.axis_index(CORE)
    mate = {CORE: 1 - d}
    me = y * n + x
    chunks = n * n
    group = 4
    members = ain.shape[0]
    owned = members // 2
    width = g.shape[3]
    own_depth = w_hbm.shape[1]
    own_chunks = own_depth // width
    rank = ain.shape[1]
    minor_axis, major_axis = (COL, ROW), (ROW, COL)
    minor_at, major_at = (x, y), (y, x)

    def chunk(c, major, minor):
        return major * n + minor if c == 0 else minor * n + major

    def wrap(v):
        return lax.rem(v + 2 * n, n)

    def remote(src, dst, ss, rs, to):
        return pltpu.make_async_remote_copy(
            src_ref=src, dst_ref=dst, send_sem=ss, recv_sem=rs, device_id=to, device_id_type=MESH
        )

    def landed(dst, sem):
        pltpu.make_async_copy(dst, dst, sem).wait()

    barrier = pltpu.get_barrier_semaphore()
    for step in (1, n - 1):
        pl.semaphore_signal(barrier, inc=1, device_id={COL: wrap(x + step)}, device_id_type=MESH)
        pl.semaphore_signal(barrier, inc=1, device_id={ROW: wrap(y + step)}, device_id_type=MESH)

    @pl.when(d == 1)
    def _():
        pl.semaphore_signal(barrier, inc=1, device_id=mate, device_id_type=MESH)

    own = pltpu.make_async_copy(tok_hbm, g.at[:, me], own_sem)
    own.start()
    taken = ((mb_hbm, mb), (bl_hbm, bl), (cot_hbm, cot))

    def take(k):
        return pltpu.make_async_copy(*taken[k], in_sem.at[k])

    for k in range(3):
        take(k).start()

    def ad_local(k):
        hbm, vm = ((ain_hbm, ain), (aout_hbm, aout))[k]
        return pltpu.make_async_copy(hbm, vm.at[pl.ds(d * owned, owned)], ad_sem.at[k])

    def ad_remote(k):
        hbm, vm = ((ain_hbm, ain), (aout_hbm, aout))[k]
        return remote(hbm, vm.at[pl.ds(d * owned, owned)], adx_s.at[k], adx_r.at[k], mate)

    def w_half(core):
        return w.at[:, pl.ds(pl.multiple_of(core * own_depth, LANES), own_depth)]

    w_local = pltpu.make_async_copy(w_hbm, w_half(d), w_sem)
    w_remote = remote(w_hbm, w_half(d), wx_s, wx_r, mate)

    def w_chunk(t):
        return w[:, pl.ds(pl.multiple_of(t * width, LANES), width)]

    for k in range(2):
        ad_local(k).start()
    w_local.start()
    own.wait()
    pl.semaphore_wait(barrier, 4 + 1 - d)

    @pl.when(d == 0)
    def _():
        pl.semaphore_signal(here, inc=1, device_id=mate, device_id_type=MESH)


    def minor_offset(j):
        back = lax.div(j + 1, 2)
        return jnp.where(lax.rem(j, 2) == 1, -back, lax.div(j, 2))

    def ag1_copy(c, j, right):
        src = chunk(c, major_at[c], wrap(minor_at[c] + minor_offset(j)))
        lands = jnp.where(j == 0, 1 if right else 2, j + 2)
        to = {minor_axis[c]: wrap(minor_at[c] + (1 if right else -1))}
        return remote(g.at[c, src], g.at[c, src], ag_s.at[c], turn_r.at[c, lands], to)

    def ag1_step(j):
        for c in range(2):
            src = chunk(c, major_at[c], wrap(minor_at[c] + minor_offset(j)))

            @pl.when(j >= 1)
            def _(c=c, src=src):
                landed(g.at[c, src], turn_r.at[c, j])

            @pl.when(jnp.logical_or(j == 0, jnp.logical_and(lax.rem(j, 2) == 1, j + 2 < n)))
            def _(c=c):
                ag1_copy(c, j, True).start()

            @pl.when(jnp.logical_and(lax.rem(j, 2) == 0, j + 2 < n))
            def _(c=c):
                ag1_copy(c, j, False).start()

    def ag2_copy(c, e, j, s):
        way = 1 - 2 * e
        t = chunk(c, wrap(major_at[c] - way * s), wrap(minor_at[c] + minor_offset(j)))
        to = {major_axis[c]: wrap(major_at[c] + way)}
        return remote(g.at[c, t], g.at[c, t], ag_s.at[c], flow_r.at[c, e, lax.rem(j, cycle), s], to)

    def ag2_landed(c, e, j, s):
        t = chunk(c, wrap(major_at[c] - (1 - 2 * e) * s), wrap(minor_at[c] + minor_offset(j)))
        landed(g.at[c, t], flow_r.at[c, e, lax.rem(j, cycle), s - 1])

    held = min(6, n)

    def held_chunk(c, j, s):
        return chunk(c, wrap(major_at[c] - (1 - 2 * (j % 2)) * s), wrap(minor_at[c] + minor_offset(j)))

    def held_copy(c, j):
        t = held_chunk(c, j, half - 1)
        to = {major_axis[c]: wrap(major_at[c] + 1 - 2 * (j % 2))}
        return remote(g.at[c, t], g.at[c, t], ag_s.at[c], held_r.at[c, j], to)

    def held_send(first, stop):
        for j in range(first, stop):
            for c in range(2):
                held_copy(c, j).start()

    def held_landed():
        for j in range(held):
            for c in range(2):
                landed(g.at[c, held_chunk(c, j, half)], held_r.at[c, j])

    def is_long(e, j):
        return lax.rem(j, 2) == e

    def streams(at, first, body):
        j = at + jnp.where(at > first, 1, 0)

        @pl.when(jnp.logical_and(at >= 0, at < n - 1))
        def _():
            lax.fori_loop(j, j + 1 + jnp.where(at == first, 1, 0), lambda k, z: (body(k), z)[1], 0)

    def ag_tick(tick, steps):
        if 0 in steps:
            streams(tick, 1, ag1_step)
        for s in steps:

            def hop(j, s=s):
                for c in range(2):
                    for e in range(2):
                        if s < half:
                            if s > 0:
                                ag2_landed(c, e, j, s)
                            if s < half - 1:
                                ag2_copy(c, e, j, s).start()
                            else:

                                @pl.when(jnp.logical_and(is_long(e, j), j >= held))
                                def _(c=c, e=e):
                                    ag2_copy(c, e, j, s).start()
                        else:

                            @pl.when(jnp.logical_and(is_long(e, j), j >= held))
                            def _(c=c, e=e):
                                ag2_landed(c, e, j, s)

            streams(tick - s, 1, hop)

    def dest_offset(i):
        ahead = lax.div(n - i, 2)
        back = lax.div(n - 1 - i, 2)
        return jnp.where(lax.rem(i, 2) == 0, -ahead, back)

    def hops(e, i):
        return jnp.where(is_long(e, i), half, half - 1)

    def rs1_chunk(c, e, i, s):
        far = (1 - 2 * e) * (hops(e, i) - s)
        return chunk(c, wrap(major_at[c] + far), wrap(minor_at[c] + dest_offset(i)))

    def rs1_sem(c, e, i, s):
        return flow_r.at[c, e, lax.rem(i + shift, cycle), s]

    def rs1_landed(c, e, i, s):
        landed(rb.at[c, e, i, s], rs1_sem(c, e, i, s))

    def rs1_copy(c, e, i, s):
        t = rs1_chunk(c, e, i, s)
        to = {major_axis[c]: wrap(major_at[c] + 1 - 2 * e)}
        return remote(p.at[c, t], rb.at[c, e, i, s], rs_s.at[c], rs1_sem(c, e, i, s), to)

    def rs1_add_send(c, e, i, s):
        t = rs1_chunk(c, e, i, s)
        put(p, (c, t), get(p, (c, t)) + get(rb, (c, e, i, s - 1)))
        rs1_copy(c, e, i, s).start()

    def rs2_copy(c, i, right):
        t = chunk(c, major_at[c], wrap(minor_at[c] + dest_offset(i)))
        to = {minor_axis[c]: wrap(minor_at[c] + (1 if right else -1))}
        return remote(p.at[c, t], r2.at[c, i], rs_s.at[c], turn_r.at[c, i], to)

    def rs1_done(c, i):
        t = chunk(c, major_at[c], wrap(minor_at[c] + dest_offset(i)))
        total = get(p, (c, t))
        for e in range(2):
            total = total + get(rb, (c, e, i, hops(e, i) - 1))
        return t, total

    def rs2_step(i):
        for c in range(2):

            @pl.when(i < 2)
            def _(c=c):
                t, total = rs1_done(c, i)
                put(p, (c, t), total)

            @pl.when(jnp.logical_and(i >= 2, i < n - 1))
            def _(c=c):
                landed(r2.at[c, i - 2], turn_r.at[c, i - 2])
                t, total = rs1_done(c, i)
                put(p, (c, t), total + get(r2, (c, i - 2)))

            @pl.when(jnp.logical_and(i < n - 1, lax.rem(i, 2) == 0))
            def _(c=c):
                rs2_copy(c, i, False).start()

            @pl.when(jnp.logical_and(i < n - 1, lax.rem(i, 2) == 1))
            def _(c=c):
                rs2_copy(c, i, True).start()

            @pl.when(i == n - 1)
            def _(c=c):
                t, total = rs1_done(c, i)
                total = total + adt[c]
                for k in (n - 3, n - 2):
                    landed(r2.at[c, k], turn_r.at[c, k])
                    total = total + get(r2, (c, k))
                igrad[c] = total.astype(BF16)

    def rs_tick(tick, steps):
        for s in steps:

            def hop(i, s=s):
                for c in range(2):
                    for e in range(2):
                        if s == 0:
                            rs1_copy(c, e, i, s).start()
                        elif s < half - 1:
                            rs1_landed(c, e, i, s - 1)
                            rs1_add_send(c, e, i, s)
                        elif s == half - 1:
                            rs1_landed(c, e, i, s - 1)

                            @pl.when(is_long(e, i))
                            def _(c=c, e=e):
                                rs1_add_send(c, e, i, s)
                        else:

                            @pl.when(is_long(e, i))
                            def _(c=c, e=e):
                                rs1_landed(c, e, i, s - 1)

                if s == half:
                    rs2_step(i)

            streams(tick - s, n - 3, hop)

    def some(body, first, last):
        lax.fori_loop(first, last, lambda k, z: (body(k), z)[1], 0)

    def member_of(b):
        end, count = jnp.int32(0), jnp.int32(0)
        for m in range(members):
            end = end + mb[m]
            count = count + jnp.where(end <= d * 2 + b, 1, 0)
        return count

    def weight_of(b, m):
        return jnp.where(member_of(b) == m, F32(1.0), F32(0.0))

    def live(b, shape, dim):
        at = lax.broadcasted_iota(jnp.int32, shape, dim)
        return jnp.where(at < bl[b], F32(1.0), F32(0.0))

    def rows(b):
        return pl.ds(b * BLOCK, BLOCK)

    def mask_step():
        for b in range(2):
            across = jnp.transpose(cot[:, b * BLOCK : (b + 1) * BLOCK].astype(F32))
            masked[rows(b)] = (across * live(b, across.shape, 0)).astype(BF16)

    def low_rank_start():
        for k in range(2):
            ad_local(k).wait()
            ad_remote(k).wait_recv()
        for b in range(2):
            a, o = weight_of(b, 0) * ain[0].astype(F32), weight_of(b, 0) * aout[0].astype(F32)
            for m in range(1, members):
                a = a + weight_of(b, m) * ain[m].astype(F32)
                o = o + weight_of(b, m) * aout[m].astype(F32)
            cin[b], cout[b] = a.astype(BF16), o.astype(BF16)
        tall = part.shape[1]
        for b in range(2):
            into = dot(g[b, me], cin[b], NT)
            back = dot(masked[rows(b)], cout[b], NT)
            both = jnp.concatenate([into, back], axis=1)
            each = BLOCK // tall
            part[pl.ds(b * each, each)] = both.reshape(each, tall, 2 * rank)

    def x_copy(e, s):
        way = 1 - 2 * e
        piece = wrap(x + way * (half - e - s))
        to = {COL: wrap(x + way)}
        return remote(part.at[piece], xbuf.at[e, s], low_s.at[0], xz_r.at[e, s], to)

    def x_step(s):
        for e in range(2):
            if 1 <= s <= half - e:
                piece = wrap(x + (1 - 2 * e) * (half - e - s))
                landed(xbuf.at[e, s - 1], xz_r.at[e, s - 1])
                part[piece] = part[piece] + xbuf[e, s - 1]
            if s < half - e:
                x_copy(e, s).start()

    def round_copy(buf, at, axis, ss, rs, e, s):
        src = wrap(at - (1 - 2 * e) * s)
        to = {axis: wrap(at + 1 - 2 * e)}
        return remote(buf.at[src], buf.at[src], ss, rs.at[e, s], to)

    def round_step(ring, s):
        buf, at, axis, ss, rs = ring
        for e in range(2):
            if 1 <= s <= half - e:
                landed(buf.at[wrap(at - (1 - 2 * e) * s)], rs.at[e, s - 1])
            if s < half - e:
                round_copy(*ring, e, s).start()

    y_ring, z_ring = (ybuf, y, ROW, low_s.at[1], y_r), (low, x, COL, low_s.at[2], xz_r)

    def total_of(ref):
        total = ref[0]
        for k in range(1, n):
            total = total + ref[k]
        return total

    def low_step(k):
        if k <= half:
            x_step(k)
        if k == half:
            ybuf[y] = part[x]
        if half <= k <= 2 * half:
            round_step(y_ring, k - half)
        if k == 2 * half:
            low[x] = total_of(ybuf).astype(BF16)
        if 2 * half <= k:
            round_step(z_ring, k - 2 * half)

    def low_of(b):
        each = n // 2
        both = low[pl.ds(b * each, each)].reshape(BLOCK, 2 * rank)
        return both[:, :rank], both[:, rank:]

    def g_copy(k):
        src, dst = ((usend, urecv), (dsend, drecv))[k]
        return remote(src, dst, gx_s.at[k], gx_r.at[k], mate)

    def grads_start():
        ups, downs = [], []
        for b in range(2):
            into, back = low_of(b)
            ups.append(SCALE * dot(into, masked[rows(b)], TN))
            downs.append(SCALE * dot(back, g[b, me], TN))
        for q in range(owned):
            theirs, mine = (1 - d) * owned + q, d * owned + q
            usend[q] = weight_of(0, theirs) * ups[0] + weight_of(1, theirs) * ups[1]
            dsend[q] = weight_of(0, theirs) * downs[0] + weight_of(1, theirs) * downs[1]
            ugrad[q] = weight_of(0, mine) * ups[0] + weight_of(1, mine) * ups[1]
            dgrad[q] = weight_of(0, mine) * downs[0] + weight_of(1, mine) * downs[1]

    def terms_step():
        for b in range(2):
            into, back = low_of(b)
            turned = jnp.transpose(into.astype(F32)).astype(BF16)
            acc[:, b * BLOCK : (b + 1) * BLOCK] += SCALE * dot(cout[b], turned, TN)
            adt[b] = SCALE * dot(back, cin[b], NN)

    def grads_done():
        for k in range(2):
            g_copy(k).wait_recv()
        for q in range(owned):
            ugrad[q] = ugrad[q] + urecv[q]
            dgrad[q] = dgrad[q] + drecv[q]

    def back_chunk(k):
        t = lax.rem(d * own_chunks + k, chunks)
        out = dot(masked[...], w_chunk(t), NN)
        for b in range(2):
            put(p, (b, t), out[b * BLOCK : (b + 1) * BLOCK])

    far_row, far_col = wrap(y + half), wrap(x + half)

    def front_group(row, q, hole):
        first = row * n + q * group
        there = [first + i for i in range(group)]
        if hole:
            there = [jnp.where(q * group + i == far_col, chunks, t) for i, t in enumerate(there)]
        rows_in = jnp.concatenate(
            [jnp.concatenate([g[0, first + i], g[1, t]], axis=0) for i, t in enumerate(there)], axis=1
        )
        at = pl.multiple_of(first * width, LANES)
        acc[...] += dot(w[:, pl.ds(at, group * width)], rows_in, NT)

    def front_early(k):
        front_group(wrap(far_row + 1 + lax.div(k, n // group)), lax.rem(k, n // group), True)

    def front_late():
        for q in range(n // group):
            front_group(far_row, q, False)

        def column(k):
            t = wrap(far_row + k) * n + far_col
            acc[:, BLOCK:] += dot(w_chunk(t), g[1, t], NT)

        some(column, 1, n)

    def hidden_step():
        for b in range(2):
            cols = acc[:, b * BLOCK : (b + 1) * BLOCK]
            hidden[:, b * BLOCK : (b + 1) * BLOCK] = (cols * live(b, cols.shape, 1)).astype(BF16)

    rs_from = n - 1 if n >= 8 else n + 1
    last = max(rs_from + ticks - 1, low_to + 2, rs_from + n + 1)
    back_from, back_ticks = early, rs_from - early
    back_each = -(-chunks // back_ticks)
    front_from, front_ticks = ticks, 3
    fronts = (n - 1) * (n // group)
    front_each = -(-fronts // front_ticks)
    tail = rs_from + n - 1

    def messages(tick, steps):
        @pl.when(tick < ticks)
        def _():
            ag_tick(tick, steps)

        @pl.when(tick >= rs_from)
        def _():
            rs_tick(tick - rs_from, steps)

    def every_tick(tick, carry):
        messages(tick, range(half - 1))

        @pl.when(tick == early - 1)
        def _():
            @pl.when(d == 1)
            def _():
                pl.semaphore_wait(here, 1)

            for k in range(2):
                ad_remote(k).start()
            w_remote.start()
            for k in range(3):
                take(k).wait()
            mask_step()
            acc[...] = jnp.zeros_like(acc)
            g[1, chunks] = jnp.zeros(g.shape[2:], BF16)

        @pl.when(tick == low_from)
        def _():
            low_rank_start()
            w_local.wait()

        @pl.when(tick == middle)
        def _():
            landed(w_half(1 - d), wx_r)

        @pl.when(jnp.logical_and(tick >= back_from, tick < back_from + back_ticks))
        def _():
            first = (tick - back_from) * back_each
            some(back_chunk, first, jnp.minimum(first + back_each, chunks))

        @pl.when(jnp.logical_and(tick >= front_from, tick < front_from + front_ticks))
        def _():
            first = (tick - front_from) * front_each
            some(front_early, first, jnp.minimum(first + front_each, fronts))

        messages(tick, range(half - 1, half + 1))

        for k in range(3 * half + 1):

            @pl.when(tick == low_from + k)
            def _(k=k):
                low_step(k)

        @pl.when(tick == low_to)
        def _():
            grads_start()
            for k in range(2):
                g_copy(k).start()
            terms_step()

        @pl.when(tick == low_to + 2)
        def _():
            grads_done()

        @pl.when(tick == tail)
        def _():
            held_send(0, 2)

        @pl.when(tick == tail + 1)
        def _():
            held_send(2, held)

        @pl.when(tick == tail + 2)
        def _():
            held_landed()
            front_late()
            hidden_step()

        return carry

    lax.fori_loop(0, last + 1, every_tick, 0)


    for k in range(2):
        ad_remote(k).wait_send()
        g_copy(k).wait_send()
    w_remote.wait_send()

    def sent(src, sem):
        pltpu.make_async_copy(src, src, sem).wait()

    for k, buf in enumerate((part, ybuf, low)):
        sent(buf.at[pl.ds(0, n - 1)], low_s.at[k])
    for c in range(2):
        sent(g.at[c, pl.ds(0, chunks - 1)], ag_s.at[c])
        sent(p.at[c, pl.ds(0, chunks - 1)], rs_s.at[c])


def hand_over(*refs):
    copies = [pltpu.make_async_copy(refs[k], refs[4 + k], refs[8].at[k]) for k in range(4)]
    for copy in copies:
        copy.start()
    for copy in copies:
        copy.wait()


def local(n, tokens, weight, adapter_in, adapter_out, cotangent, member_blocks, block_live):
    token_rows, width = tokens.shape
    hidden_width = weight.shape[1]
    blocks = token_rows // BLOCK
    owned, _, rank = adapter_in.shape
    members = 2 * owned
    half = n // 2
    tall = token_rows // n
    chunks = n * n
    vmem, hbm = (pl.BlockSpec(memory_space=s) for s in (pltpu.VMEM, pltpu.HBM))
    coded = BLOCK * width // (2 * LANES) + 1
    dma = lambda *shape: pltpu.SemaphoreType.DMA(shape)
    both_ways = (2, 2, n, half)
    out = pl.pallas_call(
        functools.partial(kernel, n),
        out_shape=(
            jax.ShapeDtypeStruct((hidden_width, token_rows), BF16),
            jax.ShapeDtypeStruct((blocks, BLOCK, width), BF16),
            jax.ShapeDtypeStruct((owned, rank, width), F32),
            jax.ShapeDtypeStruct((owned, rank, hidden_width), F32),
        ),
        in_specs=[hbm] * 7,
        out_specs=(vmem,) * 4,
        scratch_shapes=[
            pltpu.SMEM(member_blocks.shape, jnp.int32),
            pltpu.SMEM(block_live.shape, jnp.int32),
            pltpu.VMEM((hidden_width, token_rows), BF16),
            pltpu.VMEM((blocks, chunks + 1, BLOCK, width), BF16),
            pltpu.VMEM((hidden_width, chunks * width), BF16),
            pltpu.VMEM((blocks, chunks, coded, LANES), jnp.int32),
            pltpu.VMEM((*both_ways, coded, LANES), jnp.int32),
            pltpu.VMEM((2, n - 1, coded, LANES), jnp.int32),
            pltpu.VMEM((token_rows, hidden_width), BF16),
            pltpu.VMEM((hidden_width, token_rows), F32),
            pltpu.VMEM((blocks, BLOCK, width), F32),
            pltpu.VMEM((members, rank, width), BF16),
            pltpu.VMEM((members, rank, hidden_width), BF16),
            pltpu.VMEM((blocks, rank, width), BF16),
            pltpu.VMEM((blocks, rank, hidden_width), BF16),
            pltpu.VMEM((n, tall, 2 * rank), F32),
            pltpu.VMEM((2, half, tall, 2 * rank), F32),
            pltpu.VMEM((n, tall, 2 * rank), F32),
            pltpu.VMEM((n, tall, 2 * rank), BF16),
            pltpu.VMEM((owned, rank, hidden_width), F32),
            pltpu.VMEM((owned, rank, width), F32),
            pltpu.VMEM((owned, rank, hidden_width), F32),
            pltpu.VMEM((owned, rank, width), F32),
            dma(2),
            dma(2),
            dma(2, 2, 5 if n >= 8 else 2 * n, half),
            dma(2, n),
            dma(2, min(6, n)),
            pltpu.SemaphoreType.DMA,
            pltpu.SemaphoreType.DMA,
            pltpu.SemaphoreType.DMA,
            pltpu.SemaphoreType.DMA,
            dma(2),
            dma(2),
            dma(2),
            dma(3),
            dma(2, half),
            dma(2, half),
            dma(2),
            dma(2),
            dma(3),
            pltpu.SemaphoreType.REGULAR,
        ],
        compiler_params=pltpu.CompilerParams(
            collective_id=0, has_side_effects=True, vmem_limit_bytes=47 * 2**20
        ),
        name="step",
    )(
        *(
            pltpu.with_memory_space_constraint(v, pltpu.HBM)
            for v in (
                member_blocks,
                block_live,
                tokens.reshape(blocks, BLOCK, width),
                weight.T,
                jnp.swapaxes(adapter_in, 1, 2),
                adapter_out,
                cotangent.T,
            )
        )
    )
    out = pl.pallas_call(
        hand_over,
        out_shape=tuple(jax.ShapeDtypeStruct(o.shape, o.dtype) for o in out),
        in_specs=[vmem] * 4,
        out_specs=(hbm,) * 4,
        scratch_shapes=[dma(4)],
        compiler_params=pltpu.CompilerParams(vmem_limit_bytes=4 * 2**20),
        name="hand_over",
    )(*out)
    return (
        out[0].T,
        out[1].reshape(token_rows, width),
        jnp.swapaxes(out[2], 1, 2),
        out[3],
    )


def solution(mesh):
    n = math.isqrt(mesh.shape["tensor"])
    tensor = (ROW, COL)
    finer = Mesh(
        mesh.devices.reshape(mesh.shape["pop"], mesh.shape["dp"], n, n), ("pop", CORE, ROW, COL)
    )
    return jax.shard_map(
        functools.partial(local, n),
        mesh=finer,
        in_specs=(
            P(("pop", "dp"), tensor),
            P("dp", tensor),
            P(("pop", "dp"), tensor, None),
            P(("pop", "dp"), None, tensor),
            P(("pop", "dp"), tensor),
            P("pop"),
            P(("pop", "dp")),
        ),
        out_specs=(
            P(("pop", "dp"), tensor),
            P(("pop", "dp"), tensor),
            P(("pop", "dp"), tensor, None),
            P(("pop", "dp"), None, tensor),
        ),
        check_vma=False,
    )
```

```python
import functools
import math

import jax
import jax.numpy as jnp
from jax import lax
from jax.experimental import pallas as pl
from jax.experimental.pallas import tpu as pltpu
from jax.sharding import Mesh
from jax.sharding import PartitionSpec as P

BLOCK = 128
SCALE = 0.5
MESH = pl.DeviceIdType.MESH
ROW, COL, CORE = "tensor_0", "tensor_1", "dp"
F32, BF16 = jnp.float32, jnp.bfloat16

NN = (((1,), (0,)), ((), ()))
NT = (((1,), (1,)), ((), ()))
TN = (((0,), (0,)), ((), ()))


def dot(a, b, dims):
    return lax.dot_general(a, b, dims, preferred_element_type=F32)


LANES = 128
UNIT = 2.0**21
TOP = 32760.0


def halves(v):
    return [v[:, k : k + LANES] for k in range(0, v.shape[1], LANES)]


def put(ref, at, v):
    parts = halves(v)
    largest = jnp.max(functools.reduce(jnp.maximum, [jnp.abs(q) for q in parts]), axis=0, keepdims=True)
    scale = (largest * UNIT).astype(jnp.int32) + 1
    by = (TOP * UNIT) / scale.astype(F32)
    mid = v.shape[0] // 2
    for k, q in enumerate(parts):
        code = (q * by).astype(jnp.int32)
        ref[(*at, slice(k * mid, (k + 1) * mid))] = (code[:mid] << 16) | (code[mid:] & 0xFFFF)
    ref[(*at, slice(2 * mid, 2 * mid + 1))] = scale


def get(ref, at):
    mid = (ref.shape[-2] - 1) // 2
    scale = ref[(*at, slice(2 * mid, 2 * mid + 1))].astype(F32) * (1.0 / (TOP * UNIT))
    out = []
    for k in range(2):
        pair = ref[(*at, slice(k * mid, (k + 1) * mid))]
        both = jnp.concatenate([pair >> 16, (pair << 16) >> 16], axis=0)
        out.append(both.astype(F32) * scale)
    return jnp.concatenate(out, axis=1)


def kernel(
    n,
    mb_hbm,
    bl_hbm,
    tok_hbm,
    w_hbm,
    ain_hbm,
    aout_hbm,
    cot_hbm,
    hidden,
    igrad,
    dgrad,
    ugrad,
    mb,
    bl,
    cot,
    g,
    w,
    p,
    rb,
    r2,
    masked,
    acc,
    adt,
    ain,
    aout,
    cin,
    cout,
    part,
    xbuf,
    ybuf,
    low,
    usend,
    dsend,
    urecv,
    drecv,
    ag_s,
    rs_s,
    flow_r,
    turn_r,
    held_r,
    own_sem,
    w_sem,
    wx_s,
    wx_r,
    ad_sem,
    adx_s,
    adx_r,
    low_s,
    xz_r,
    y_r,
    gx_s,
    gx_r,
    in_sem,
    here,
):
    half = n // 2
    ticks = n - 1 + half
    cycle, shift = (5, 3) if n >= 8 else (2 * n, n)
    early, middle = n // 4, n // 2
    low_from = early
    low_to = low_from + 3 * half
    y, x, d = lax.axis_index(ROW), lax.axis_index(COL), lax.axis_index(CORE)
    mate = {CORE: 1 - d}
    me = y * n + x
    chunks = n * n
    group = 4
    members = ain.shape[0]
    owned = members // 2
    width = g.shape[3]
    own_depth = w_hbm.shape[1]
    own_chunks = own_depth // width
    rank = ain.shape[1]
    minor_axis, major_axis = (COL, ROW), (ROW, COL)
    minor_at, major_at = (x, y), (y, x)

    def chunk(c, major, minor):
        return major * n + minor if c == 0 else minor * n + major

    def wrap(v):
        return lax.rem(v + 2 * n, n)

    def remote(src, dst, ss, rs, to):
        return pltpu.make_async_remote_copy(
            src_ref=src, dst_ref=dst, send_sem=ss, recv_sem=rs, device_id=to, device_id_type=MESH
        )

    def landed(dst, sem):
        pltpu.make_async_copy(dst, dst, sem).wait()

    barrier = pltpu.get_barrier_semaphore()
    for step in (1, n - 1):
        pl.semaphore_signal(barrier, inc=1, device_id={COL: wrap(x + step)}, device_id_type=MESH)
        pl.semaphore_signal(barrier, inc=1, device_id={ROW: wrap(y + step)}, device_id_type=MESH)

    @pl.when(d == 1)
    def _():
        pl.semaphore_signal(barrier, inc=1, device_id=mate, device_id_type=MESH)

    own = pltpu.make_async_copy(tok_hbm, g.at[:, me], own_sem)
    own.start()
    taken = ((mb_hbm, mb), (bl_hbm, bl), (cot_hbm, cot))

    def take(k):
        return pltpu.make_async_copy(*taken[k], in_sem.at[k])

    for k in range(3):
        take(k).start()

    def ad_local(k):
        hbm, vm = ((ain_hbm, ain), (aout_hbm, aout))[k]
        return pltpu.make_async_copy(hbm, vm.at[pl.ds(d * owned, owned)], ad_sem.at[k])

    def ad_remote(k):
        hbm, vm = ((ain_hbm, ain), (aout_hbm, aout))[k]
        return remote(hbm, vm.at[pl.ds(d * owned, owned)], adx_s.at[k], adx_r.at[k], mate)

    def w_half(core):
        return w.at[:, pl.ds(pl.multiple_of(core * own_depth, LANES), own_depth)]

    w_local = pltpu.make_async_copy(w_hbm, w_half(d), w_sem)
    w_remote = remote(w_hbm, w_half(d), wx_s, wx_r, mate)

    def w_chunk(t):
        return w[:, pl.ds(pl.multiple_of(t * width, LANES), width)]

    for k in range(2):
        ad_local(k).start()
    w_local.start()
    own.wait()
    pl.semaphore_wait(barrier, 4 + 1 - d)

    @pl.when(d == 0)
    def _():
        pl.semaphore_signal(here, inc=1, device_id=mate, device_id_type=MESH)


    def minor_offset(j):
        back = lax.div(j + 1, 2)
        return jnp.where(lax.rem(j, 2) == 1, -back, lax.div(j, 2))

    def ag1_copy(c, j, right):
        src = chunk(c, major_at[c], wrap(minor_at[c] + minor_offset(j)))
        lands = jnp.where(j == 0, 1 if right else 2, j + 2)
        to = {minor_axis[c]: wrap(minor_at[c] + (1 if right else -1))}
        return remote(g.at[c, src], g.at[c, src], ag_s.at[c], turn_r.at[c, lands], to)

    def ag1_step(j):
        for c in range(2):
            src = chunk(c, major_at[c], wrap(minor_at[c] + minor_offset(j)))

            @pl.when(j >= 1)
            def _(c=c, src=src):
                landed(g.at[c, src], turn_r.at[c, j])

            @pl.when(jnp.logical_or(j == 0, jnp.logical_and(lax.rem(j, 2) == 1, j + 2 < n)))
            def _(c=c):
                ag1_copy(c, j, True).start()

            @pl.when(jnp.logical_and(lax.rem(j, 2) == 0, j + 2 < n))
            def _(c=c):
                ag1_copy(c, j, False).start()

    def ag2_copy(c, e, j, s):
        way = 1 - 2 * e
        t = chunk(c, wrap(major_at[c] - way * s), wrap(minor_at[c] + minor_offset(j)))
        to = {major_axis[c]: wrap(major_at[c] + way)}
        return remote(g.at[c, t], g.at[c, t], ag_s.at[c], flow_r.at[c, e, lax.rem(j, cycle), s], to)

    def ag2_landed(c, e, j, s):
        t = chunk(c, wrap(major_at[c] - (1 - 2 * e) * s), wrap(minor_at[c] + minor_offset(j)))
        landed(g.at[c, t], flow_r.at[c, e, lax.rem(j, cycle), s - 1])

    held = min(6, n)

    def held_chunk(c, j, s):
        return chunk(c, wrap(major_at[c] - (1 - 2 * (j % 2)) * s), wrap(minor_at[c] + minor_offset(j)))

    def held_copy(c, j):
        t = held_chunk(c, j, half - 1)
        to = {major_axis[c]: wrap(major_at[c] + 1 - 2 * (j % 2))}
        return remote(g.at[c, t], g.at[c, t], ag_s.at[c], held_r.at[c, j], to)

    def held_send(first, stop):
        for j in range(first, stop):
            for c in range(2):
                held_copy(c, j).start()

    def held_landed():
        for j in range(held):
            for c in range(2):
                landed(g.at[c, held_chunk(c, j, half)], held_r.at[c, j])

    def is_long(e, j):
        return lax.rem(j, 2) == e

    def streams(at, first, body):
        j = at + jnp.where(at > first, 1, 0)

        @pl.when(jnp.logical_and(at >= 0, at < n - 1))
        def _():
            lax.fori_loop(j, j + 1 + jnp.where(at == first, 1, 0), lambda k, z: (body(k), z)[1], 0)

    def ag_tick(tick, steps):
        if 0 in steps:
            streams(tick, 1, ag1_step)
        for s in steps:

            def hop(j, s=s):
                for c in range(2):
                    for e in range(2):
                        if s < half:
                            if s > 0:
                                ag2_landed(c, e, j, s)
                            if s < half - 1:
                                ag2_copy(c, e, j, s).start()
                            else:

                                @pl.when(jnp.logical_and(is_long(e, j), j >= held))
                                def _(c=c, e=e):
                                    ag2_copy(c, e, j, s).start()
                        else:

                            @pl.when(jnp.logical_and(is_long(e, j), j >= held))
                            def _(c=c, e=e):
                                ag2_landed(c, e, j, s)

            streams(tick - s, 1, hop)

    def dest_offset(i):
        ahead = lax.div(n - i, 2)
        back = lax.div(n - 1 - i, 2)
        return jnp.where(lax.rem(i, 2) == 0, -ahead, back)

    def hops(e, i):
        return jnp.where(is_long(e, i), half, half - 1)

    def rs1_chunk(c, e, i, s):
        far = (1 - 2 * e) * (hops(e, i) - s)
        return chunk(c, wrap(major_at[c] + far), wrap(minor_at[c] + dest_offset(i)))

    def rs1_sem(c, e, i, s):
        return flow_r.at[c, e, lax.rem(i + shift, cycle), s]

    def rs1_landed(c, e, i, s):
        landed(rb.at[c, e, i, s], rs1_sem(c, e, i, s))

    def rs1_copy(c, e, i, s):
        t = rs1_chunk(c, e, i, s)
        to = {major_axis[c]: wrap(major_at[c] + 1 - 2 * e)}
        return remote(p.at[c, t], rb.at[c, e, i, s], rs_s.at[c], rs1_sem(c, e, i, s), to)

    def rs1_add_send(c, e, i, s):
        t = rs1_chunk(c, e, i, s)
        put(p, (c, t), get(p, (c, t)) + get(rb, (c, e, i, s - 1)))
        rs1_copy(c, e, i, s).start()

    def rs2_copy(c, i, right):
        t = chunk(c, major_at[c], wrap(minor_at[c] + dest_offset(i)))
        to = {minor_axis[c]: wrap(minor_at[c] + (1 if right else -1))}
        return remote(p.at[c, t], r2.at[c, i], rs_s.at[c], turn_r.at[c, i], to)

    def rs1_done(c, i):
        t = chunk(c, major_at[c], wrap(minor_at[c] + dest_offset(i)))
        total = get(p, (c, t))
        for e in range(2):
            total = total + get(rb, (c, e, i, hops(e, i) - 1))
        return t, total

    def rs2_step(i):
        for c in range(2):

            @pl.when(i < 2)
            def _(c=c):
                t, total = rs1_done(c, i)
                put(p, (c, t), total)

            @pl.when(jnp.logical_and(i >= 2, i < n - 1))
            def _(c=c):
                landed(r2.at[c, i - 2], turn_r.at[c, i - 2])
                t, total = rs1_done(c, i)
                put(p, (c, t), total + get(r2, (c, i - 2)))

            @pl.when(jnp.logical_and(i < n - 1, lax.rem(i, 2) == 0))
            def _(c=c):
                rs2_copy(c, i, False).start()

            @pl.when(jnp.logical_and(i < n - 1, lax.rem(i, 2) == 1))
            def _(c=c):
                rs2_copy(c, i, True).start()

            @pl.when(i == n - 1)
            def _(c=c):
                t, total = rs1_done(c, i)
                total = total + adt[c]
                for k in (n - 3, n - 2):
                    landed(r2.at[c, k], turn_r.at[c, k])
                    total = total + get(r2, (c, k))
                igrad[c] = total.astype(BF16)

    def rs_tick(tick, steps):
        for s in steps:

            def hop(i, s=s):
                for c in range(2):
                    for e in range(2):
                        if s == 0:
                            rs1_copy(c, e, i, s).start()
                        elif s < half - 1:
                            rs1_landed(c, e, i, s - 1)
                            rs1_add_send(c, e, i, s)
                        elif s == half - 1:
                            rs1_landed(c, e, i, s - 1)

                            @pl.when(is_long(e, i))
                            def _(c=c, e=e):
                                rs1_add_send(c, e, i, s)
                        else:

                            @pl.when(is_long(e, i))
                            def _(c=c, e=e):
                                rs1_landed(c, e, i, s - 1)

                if s == half:
                    rs2_step(i)

            streams(tick - s, n - 3, hop)

    def some(body, first, last):
        lax.fori_loop(first, last, lambda k, z: (body(k), z)[1], 0)

    def member_of(b):
        end, count = jnp.int32(0), jnp.int32(0)
        for m in range(members):
            end = end + mb[m]
            count = count + jnp.where(end <= d * 2 + b, 1, 0)
        return count

    def weight_of(b, m):
        return jnp.where(member_of(b) == m, F32(1.0), F32(0.0))

    def live(b, shape, dim):
        at = lax.broadcasted_iota(jnp.int32, shape, dim)
        return jnp.where(at < bl[b], F32(1.0), F32(0.0))

    def rows(b):
        return pl.ds(b * BLOCK, BLOCK)

    def mask_step():
        for b in range(2):
            across = jnp.transpose(cot[:, b * BLOCK : (b + 1) * BLOCK].astype(F32))
            masked[rows(b)] = (across * live(b, across.shape, 0)).astype(BF16)

    def low_rank_start():
        for k in range(2):
            ad_local(k).wait()
            ad_remote(k).wait_recv()
        for b in range(2):
            a, o = weight_of(b, 0) * ain[0].astype(F32), weight_of(b, 0) * aout[0].astype(F32)
            for m in range(1, members):
                a = a + weight_of(b, m) * ain[m].astype(F32)
                o = o + weight_of(b, m) * aout[m].astype(F32)
            cin[b], cout[b] = a.astype(BF16), o.astype(BF16)
        tall = part.shape[1]
        for b in range(2):
            into = dot(g[b, me], cin[b], NT)
            back = dot(masked[rows(b)], cout[b], NT)
            both = jnp.concatenate([into, back], axis=1)
            each = BLOCK // tall
            part[pl.ds(b * each, each)] = both.reshape(each, tall, 2 * rank)

    def x_copy(e, s):
        way = 1 - 2 * e
        piece = wrap(x + way * (half - e - s))
        to = {COL: wrap(x + way)}
        return remote(part.at[piece], xbuf.at[e, s], low_s.at[0], xz_r.at[e, s], to)

    def x_step(s):
        for e in range(2):
            if 1 <= s <= half - e:
                piece = wrap(x + (1 - 2 * e) * (half - e - s))
                landed(xbuf.at[e, s - 1], xz_r.at[e, s - 1])
                part[piece] = part[piece] + xbuf[e, s - 1]
            if s < half - e:
                x_copy(e, s).start()

    def round_copy(buf, at, axis, ss, rs, e, s):
        src = wrap(at - (1 - 2 * e) * s)
        to = {axis: wrap(at + 1 - 2 * e)}
        return remote(buf.at[src], buf.at[src], ss, rs.at[e, s], to)

    def round_step(ring, s):
        buf, at, axis, ss, rs = ring
        for e in range(2):
            if 1 <= s <= half - e:
                landed(buf.at[wrap(at - (1 - 2 * e) * s)], rs.at[e, s - 1])
            if s < half - e:
                round_copy(*ring, e, s).start()

    y_ring, z_ring = (ybuf, y, ROW, low_s.at[1], y_r), (low, x, COL, low_s.at[2], xz_r)

    def total_of(ref):
        total = ref[0]
        for k in range(1, n):
            total = total + ref[k]
        return total

    def low_step(k):
        if k <= half:
            x_step(k)
        if k == half:
            ybuf[y] = part[x]
        if half <= k <= 2 * half:
            round_step(y_ring, k - half)
        if k == 2 * half:
            low[x] = total_of(ybuf).astype(BF16)
        if 2 * half <= k:
            round_step(z_ring, k - 2 * half)

    def low_of(b):
        each = n // 2
        both = low[pl.ds(b * each, each)].reshape(BLOCK, 2 * rank)
        return both[:, :rank], both[:, rank:]

    def g_copy(k):
        src, dst = ((usend, urecv), (dsend, drecv))[k]
        return remote(src, dst, gx_s.at[k], gx_r.at[k], mate)

    def grads_start():
        ups, downs = [], []
        for b in range(2):
            into, back = low_of(b)
            ups.append(SCALE * dot(into, masked[rows(b)], TN))
            downs.append(SCALE * dot(back, g[b, me], TN))
        for q in range(owned):
            theirs, mine = (1 - d) * owned + q, d * owned + q
            usend[q] = weight_of(0, theirs) * ups[0] + weight_of(1, theirs) * ups[1]
            dsend[q] = weight_of(0, theirs) * downs[0] + weight_of(1, theirs) * downs[1]
            ugrad[q] = weight_of(0, mine) * ups[0] + weight_of(1, mine) * ups[1]
            dgrad[q] = weight_of(0, mine) * downs[0] + weight_of(1, mine) * downs[1]

    def terms_step():
        for b in range(2):
            into, back = low_of(b)
            turned = jnp.transpose(into.astype(F32)).astype(BF16)
            acc[:, b * BLOCK : (b + 1) * BLOCK] += SCALE * dot(cout[b], turned, TN)
            adt[b] = SCALE * dot(back, cin[b], NN)

    def grads_done():
        for k in range(2):
            g_copy(k).wait_recv()
        for q in range(owned):
            ugrad[q] = ugrad[q] + urecv[q]
            dgrad[q] = dgrad[q] + drecv[q]

    def back_pair(k):
        t = lax.rem(d * own_chunks + 2 * k, chunks)
        at = pl.multiple_of(t * width, LANES)
        out = dot(masked[...], w[:, pl.ds(at, 2 * width)], NN)
        for i in range(2):
            for b in range(2):
                put(p, (b, t + i), out[b * BLOCK : (b + 1) * BLOCK, i * width : (i + 1) * width])

    far_row, far_col = wrap(y + half), wrap(x + half)

    def front_group(row, q, hole):
        first = row * n + q * group
        there = [first + i for i in range(group)]
        if hole:
            there = [jnp.where(q * group + i == far_col, chunks, t) for i, t in enumerate(there)]
        rows_in = jnp.concatenate(
            [jnp.concatenate([g[0, first + i], g[1, t]], axis=0) for i, t in enumerate(there)], axis=1
        )
        at = pl.multiple_of(first * width, LANES)
        acc[...] += dot(w[:, pl.ds(at, group * width)], rows_in, NT)

    def front_early(k):
        front_group(wrap(far_row + 1 + lax.div(k, n // group)), lax.rem(k, n // group), True)

    def front_late():
        for q in range(n // group):
            front_group(far_row, q, False)

        def column(k):
            t = wrap(far_row + k) * n + far_col
            acc[:, BLOCK:] += dot(w_chunk(t), g[1, t], NT)

        some(column, 1, n)

    def hidden_step():
        for b in range(2):
            cols = acc[:, b * BLOCK : (b + 1) * BLOCK]
            hidden[:, b * BLOCK : (b + 1) * BLOCK] = (cols * live(b, cols.shape, 1)).astype(BF16)

    rs_from = n - 1 if n >= 8 else n + 1
    last = max(rs_from + ticks - 1, low_to + 2, rs_from + n + 1)
    back_from, back_ticks = early, rs_from - early
    back_each = -(-(chunks // 2) // back_ticks)
    front_from, front_ticks = ticks, 3
    fronts = (n - 1) * (n // group)
    front_each = -(-fronts // front_ticks)
    tail = rs_from + n - 1

    def messages(tick, steps):
        @pl.when(tick < ticks)
        def _():
            ag_tick(tick, steps)

        @pl.when(tick >= rs_from)
        def _():
            rs_tick(tick - rs_from, steps)

    def every_tick(tick, carry):
        messages(tick, range(half - 1))

        @pl.when(tick == early - 1)
        def _():
            @pl.when(d == 1)
            def _():
                pl.semaphore_wait(here, 1)

            for k in range(2):
                ad_remote(k).start()
            w_remote.start()
            for k in range(3):
                take(k).wait()
            mask_step()
            acc[...] = jnp.zeros_like(acc)
            g[1, chunks] = jnp.zeros(g.shape[2:], BF16)

        @pl.when(tick == low_from)
        def _():
            low_rank_start()
            w_local.wait()

        @pl.when(tick == middle)
        def _():
            landed(w_half(1 - d), wx_r)

        @pl.when(jnp.logical_and(tick >= back_from, tick < back_from + back_ticks))
        def _():
            first = (tick - back_from) * back_each
            some(back_pair, first, jnp.minimum(first + back_each, chunks // 2))

        @pl.when(jnp.logical_and(tick >= front_from, tick < front_from + front_ticks))
        def _():
            first = (tick - front_from) * front_each
            some(front_early, first, jnp.minimum(first + front_each, fronts))

        messages(tick, range(half - 1, half + 1))

        for k in range(3 * half + 1):

            @pl.when(tick == low_from + k)
            def _(k=k):
                low_step(k)

        @pl.when(tick == low_to)
        def _():
            grads_start()
            for k in range(2):
                g_copy(k).start()
            terms_step()

        @pl.when(tick == low_to + 2)
        def _():
            grads_done()

        @pl.when(tick == tail)
        def _():
            held_send(0, 2)

        @pl.when(tick == tail + 1)
        def _():
            held_send(2, held)

        @pl.when(tick == tail + 2)
        def _():
            held_landed()
            front_late()
            hidden_step()

        return carry

    lax.fori_loop(0, last + 1, every_tick, 0)


    for k in range(2):
        ad_remote(k).wait_send()
        g_copy(k).wait_send()
    w_remote.wait_send()

    def sent(src, sem):
        pltpu.make_async_copy(src, src, sem).wait()

    for k, buf in enumerate((part, ybuf, low)):
        sent(buf.at[pl.ds(0, n - 1)], low_s.at[k])
    for c in range(2):
        sent(g.at[c, pl.ds(0, chunks - 1)], ag_s.at[c])
        sent(p.at[c, pl.ds(0, chunks - 1)], rs_s.at[c])


def hand_over(*refs):
    copies = [pltpu.make_async_copy(refs[k], refs[4 + k], refs[8].at[k]) for k in range(4)]
    for copy in copies:
        copy.start()
    for copy in copies:
        copy.wait()


def local(n, tokens, weight, adapter_in, adapter_out, cotangent, member_blocks, block_live):
    token_rows, width = tokens.shape
    hidden_width = weight.shape[1]
    blocks = token_rows // BLOCK
    owned, _, rank = adapter_in.shape
    members = 2 * owned
    half = n // 2
    tall = token_rows // n
    chunks = n * n
    vmem, hbm = (pl.BlockSpec(memory_space=s) for s in (pltpu.VMEM, pltpu.HBM))
    coded = BLOCK * width // (2 * LANES) + 1
    dma = lambda *shape: pltpu.SemaphoreType.DMA(shape)
    both_ways = (2, 2, n, half)
    out = pl.pallas_call(
        functools.partial(kernel, n),
        out_shape=(
            jax.ShapeDtypeStruct((hidden_width, token_rows), BF16),
            jax.ShapeDtypeStruct((blocks, BLOCK, width), BF16),
            jax.ShapeDtypeStruct((owned, rank, width), F32),
            jax.ShapeDtypeStruct((owned, rank, hidden_width), F32),
        ),
        in_specs=[hbm] * 7,
        out_specs=(vmem,) * 4,
        scratch_shapes=[
            pltpu.SMEM(member_blocks.shape, jnp.int32),
            pltpu.SMEM(block_live.shape, jnp.int32),
            pltpu.VMEM((hidden_width, token_rows), BF16),
            pltpu.VMEM((blocks, chunks + 1, BLOCK, width), BF16),
            pltpu.VMEM((hidden_width, chunks * width), BF16),
            pltpu.VMEM((blocks, chunks, coded, LANES), jnp.int32),
            pltpu.VMEM((*both_ways, coded, LANES), jnp.int32),
            pltpu.VMEM((2, n - 1, coded, LANES), jnp.int32),
            pltpu.VMEM((token_rows, hidden_width), BF16),
            pltpu.VMEM((hidden_width, token_rows), F32),
            pltpu.VMEM((blocks, BLOCK, width), F32),
            pltpu.VMEM((members, rank, width), BF16),
            pltpu.VMEM((members, rank, hidden_width), BF16),
            pltpu.VMEM((blocks, rank, width), BF16),
            pltpu.VMEM((blocks, rank, hidden_width), BF16),
            pltpu.VMEM((n, tall, 2 * rank), F32),
            pltpu.VMEM((2, half, tall, 2 * rank), F32),
            pltpu.VMEM((n, tall, 2 * rank), F32),
            pltpu.VMEM((n, tall, 2 * rank), BF16),
            pltpu.VMEM((owned, rank, hidden_width), F32),
            pltpu.VMEM((owned, rank, width), F32),
            pltpu.VMEM((owned, rank, hidden_width), F32),
            pltpu.VMEM((owned, rank, width), F32),
            dma(2),
            dma(2),
            dma(2, 2, 5 if n >= 8 else 2 * n, half),
            dma(2, n),
            dma(2, min(6, n)),
            pltpu.SemaphoreType.DMA,
            pltpu.SemaphoreType.DMA,
            pltpu.SemaphoreType.DMA,
            pltpu.SemaphoreType.DMA,
            dma(2),
            dma(2),
            dma(2),
            dma(3),
            dma(2, half),
            dma(2, half),
            dma(2),
            dma(2),
            dma(3),
            pltpu.SemaphoreType.REGULAR,
        ],
        compiler_params=pltpu.CompilerParams(
            collective_id=0, has_side_effects=True, vmem_limit_bytes=47 * 2**20
        ),
        name="step",
    )(
        *(
            pltpu.with_memory_space_constraint(v, pltpu.HBM)
            for v in (
                member_blocks,
                block_live,
                tokens.reshape(blocks, BLOCK, width),
                weight.T,
                jnp.swapaxes(adapter_in, 1, 2),
                adapter_out,
                cotangent.T,
            )
        )
    )
    out = pl.pallas_call(
        hand_over,
        out_shape=tuple(jax.ShapeDtypeStruct(o.shape, o.dtype) for o in out),
        in_specs=[vmem] * 4,
        out_specs=(hbm,) * 4,
        scratch_shapes=[dma(4)],
        compiler_params=pltpu.CompilerParams(vmem_limit_bytes=4 * 2**20),
        name="hand_over",
    )(*out)
    return (
        out[0].T,
        out[1].reshape(token_rows, width),
        jnp.swapaxes(out[2], 1, 2),
        out[3],
    )


def solution(mesh):
    n = math.isqrt(mesh.shape["tensor"])
    tensor = (ROW, COL)
    finer = Mesh(
        mesh.devices.reshape(mesh.shape["pop"], mesh.shape["dp"], n, n), ("pop", CORE, ROW, COL)
    )
    return jax.shard_map(
        functools.partial(local, n),
        mesh=finer,
        in_specs=(
            P(("pop", "dp"), tensor),
            P("dp", tensor),
            P(("pop", "dp"), tensor, None),
            P(("pop", "dp"), None, tensor),
            P(("pop", "dp"), tensor),
            P("pop"),
            P(("pop", "dp")),
        ),
        out_specs=(
            P(("pop", "dp"), tensor),
            P(("pop", "dp"), tensor),
            P(("pop", "dp"), tensor, None),
            P(("pop", "dp"), None, tensor),
        ),
        check_vma=False,
    )
```
